32 devices in a mesh: tr: 4 (over z), tc: 8 (over y, x, core).
Axes of the slice: x: 2, y: 2, z: 4, core: 2. Of those that a mesh axis runs over, the one named last changes fastest.
Arguments:
- cov_tiles: float32 [16384, 16384], P('tr', 'tc'), may hold values from -3 to 9, as said below
- block_order: int32 [32], replicated, may hold values from 0 to 31, as said below
- stations: int32 [1, 256], P(None, 'tc'), may hold values from 0 to 31
- obs_values: float32 [1, 256, 512], P(None, 'tc'), may hold values from -0.25 to 0.25
- obs_error: float32 [1, 256], P(None, 'tc'), may hold values from 0.5 to 4
Outputs:
- cov_updated: float32 [16384, 16384], P('tr', 'tc')
The draws below stay inside these ranges and needn't reach their ends.
Inputs may be any that keep to these rules, and one draw needn't show every extreme that they name: `block_order`: a permutation of 0 to 31. `cov_tiles`: the matrix that the live tiles describe, completed by symmetry, is positive definite with diagonal tiles symmetric; tiles that are not live are zero.
All inputs are finite; a program needn't handle non-finite values.
Results may differ from the reference program's by a relative error of at most 0.0001.
Values sent between devices are 32-bit elements; how exact they have to be, the bound alone decides.
A program may use at most 192 MiB of HBM per device.

```python
import math
import jax
import jax.numpy as jnp
from jax import lax

ORDER = 16384
TILE = 512
NOBS = 256
BATCHES = 1
BLOCKS = 32


def order_from(key):
    return jax.random.permutation(jax.random.fold_in(key, 17), ORDER // TILE).astype(jnp.int32)


def draw_block_order(key, part):
    return order_from(key)


def draw_cov_tiles(key, part):
    count_blocks = ORDER // TILE
    permuted = order_from(key)
    first_key, second_key, third_key = jax.random.split(jax.random.fold_in(key, 29), 3)
    noise = jax.random.normal(first_key, (ORDER, ORDER), jnp.float32)
    loading = jax.random.normal(second_key, (ORDER, 32), jnp.float32)
    spread = jnp.exp(jax.random.uniform(third_key, (ORDER,), jnp.float32, math.log(2.0), math.log(6.0)))
    loading = loading * 0.125
    matrix = (noise + noise.T) * (0.55 / math.sqrt(ORDER)) + jnp.diag(spread)
    matrix = matrix + jnp.dot(loading, loading.T, precision=lax.Precision.HIGHEST, preferred_element_type=jnp.float32)
    positions = jnp.arange(count_blocks, dtype=jnp.int32)
    live = (permuted[:, None] > permuted[None, :]).astype(jnp.float32) + (positions[:, None] == positions[None, :]).astype(jnp.float32)
    spread_mask = jnp.broadcast_to(live[:, None, :, None], (count_blocks, TILE, count_blocks, TILE)).reshape(ORDER, ORDER)
    return matrix * spread_mask


def touch_ends(array, rng, least, high):
    index_at = [jax.random.randint(jax.random.fold_in(rng, axis), (), 0, length) for axis, length in enumerate(array.shape)]
    widest = array.shape.index(max(array.shape))
    beside = index_at[:widest] + [(index_at[widest] + 1) % array.shape[widest]] + index_at[widest + 1:]
    return array.at[tuple(index_at)].set(least).at[tuple(beside)].set(high)


def steps_of(rng, extent, shards, least, top_value):
    def one(axis_at, blocks):
        steps = jax.random.uniform(jax.random.fold_in(jax.random.fold_in(rng, 6), axis_at), (blocks,), jnp.float32, least / len(shards), top_value / len(shards))
        return jnp.repeat(jnp.exp(steps), extent[axis_at] // blocks).reshape((-1,) + (1,) * (len(extent) - axis_at - 1))

    level = one(*shards[0])
    for cut in shards[1:]:
        level = level * one(*cut)
    return level


def scatter_about(stream_key, extent, width, limit, shards=(), kind=jnp.bfloat16):
    factor_of = steps_of(stream_key, extent, shards, -0.22, 0.18) if shards else 1.0
    array = jax.random.normal(stream_key, extent, jnp.float32) * width * factor_of
    return jnp.minimum(jnp.maximum(array, -limit), limit).astype(kind)


def setup_inputs(seed: int = 0) -> dict:
    key_list = jax.random.split(jax.random.key(seed), 6)
    cov_tiles = draw_cov_tiles(jax.random.fold_in(key_list[5], 71), 0)
    block_order = draw_block_order(jax.random.fold_in(key_list[5], 71), 0)
    stations = touch_ends(jax.random.randint(key_list[2], (BATCHES, NOBS), 0, BLOCKS), jax.random.fold_in(key_list[2], 1), 0, BLOCKS - 1).astype(jnp.int32)
    obs_values = scatter_about(key_list[3], (BATCHES, NOBS, TILE), TILE ** -0.5, 0.25, ((1, 8),), jnp.float32)
    obs_error = jnp.clip(jnp.exp(math.log(4.0) - 2.0794415 * jax.random.uniform(key_list[4], (BATCHES, NOBS), jnp.float32) ** steps_of(key_list[4], (BATCHES, NOBS), ((1, 8),), -0.2, 0.2)), 0.5, 4.0)
    return dict(cov_tiles=cov_tiles, block_order=block_order, stations=stations, obs_values=obs_values, obs_error=obs_error)


precise = lax.Precision.HIGHEST

def tile_spread(blockwise):
    return jnp.broadcast_to(blockwise[:, None, :, None], (BLOCKS, TILE, BLOCKS, TILE)).reshape(ORDER, ORDER)

def reference(cov_tiles, block_order, stations, obs_values, obs_error):
    positions = jnp.arange(BLOCKS, dtype=jnp.int32)
    below_mask = (block_order[:, None] > block_order[None, :]).astype(jnp.float32)
    on_diagonal = (positions[:, None] == positions[None, :]).astype(jnp.float32)
    strict = cov_tiles * tile_spread(below_mask)
    covariance = strict + strict.T + cov_tiles * tile_spread(on_diagonal)
    for batch_index in range(BATCHES):
        select = (stations[batch_index][None, :] == block_order[:, None]).astype(jnp.float32)
        design = (select[:, None, :] * obs_values[batch_index].T[None, :, :]).reshape(ORDER, NOBS)
        cross_cov = jnp.dot(covariance.astype(jnp.float32), design.astype(jnp.float32), precision=precise, preferred_element_type=jnp.float32)
        innovation = jnp.dot(design.T.astype(jnp.float32), cross_cov.astype(jnp.float32), precision=precise, preferred_element_type=jnp.float32)
        innovation = innovation + jnp.diag(obs_error[batch_index])
        factor = jnp.linalg.cholesky(innovation)
        scaled = lax.linalg.triangular_solve(factor, cross_cov, left_side=False, lower=True, transpose_a=True)
        covariance = covariance - jnp.dot(scaled.astype(jnp.float32), scaled.T.astype(jnp.float32), precision=precise, preferred_element_type=jnp.float32)
    return covariance * tile_spread(below_mask + on_diagonal)
```

```python
import functools

import jax
import jax.numpy as jnp
from jax import lax
from jax.experimental import pallas as pl
from jax.experimental.pallas import tpu as pltpu
from jax.sharding import PartitionSpec as P

exact = lax.Precision.HIGHEST
bf16, f32, i32 = jnp.bfloat16, jnp.float32, jnp.int32
DEPTH = 4
ANY = pl.BlockSpec(memory_space=pl.ANY)
VMEM = pl.BlockSpec(memory_space=pltpu.VMEM)
SMEM = pl.BlockSpec(memory_space=pltpu.SMEM)


def product(former, latter, over, precision=exact):
    return lax.dot_general(
        former,
        latter,
        (((over[0],), (over[1],)), ((), ())),
        precision=precision,
        preferred_element_type=jnp.float32,
    )


def halves(array):
    high = array.astype(bf16)
    return high, (array - high.astype(f32)).astype(bf16)


def dot(former, latter):
    return jnp.dot(former, latter, preferred_element_type=f32)


def dot3(former, latter):
    return dot(former[0], latter[0]) + dot(former[0], latter[1]) + dot(former[1], latter[0])


def list_tiles(order_ref, live_ref, row_blocks, col_blocks, when_dead=None):
    row_first = lax.axis_index("tr") * row_blocks
    col_first = lax.axis_index("tc") * col_blocks

    def step(tile, count):
        row, col = tile // col_blocks, tile % col_blocks
        p, q = row_first + row, col_first + col
        live = (order_ref[p] > order_ref[q]) | (p == q)

        @pl.when(live)
        def _():
            live_ref[count] = tile

        if when_dead is not None:

            @pl.when(jnp.logical_not(live))
            def _():
                when_dead(tile)

        return count + live.astype(i32)

    return lax.fori_loop(0, row_blocks * col_blocks, step, jnp.int32(0))


def tile_at(ref, tile, col_blocks, size):
    row, col = tile // col_blocks, tile % col_blocks
    return ref.at[
        pl.ds(pl.multiple_of(row * size, size), size), pl.ds(pl.multiple_of(col * size, size), size)
    ]


def forward_kernel(
    order_ref, packed_ref, cov_ref, rows_ref, cols_ref, gram_ref,
    live_ref, held, sem, for_rows, for_cols,
):
    row_blocks, size, count_obs = rows_ref.shape
    col_blocks = cols_ref.shape[0]
    row_first = lax.axis_index("tr") * row_blocks
    col_first = lax.axis_index("tc") * col_blocks
    count = list_tiles(order_ref, live_ref, row_blocks, col_blocks)

    def fetch(at):
        slot = at % DEPTH
        return pltpu.make_async_copy(
            tile_at(cov_ref, live_ref[at], col_blocks, size), held.at[slot], sem.at[slot]
        )

    for at in range(DEPTH - 1):

        @pl.when(at < count)
        def _():
            fetch(at).start()

    values = packed_ref[:, :size]
    extras = packed_ref[:, size:]
    codes_down = extras[:, 0:1].astype(i32)
    flipped = extras.T
    codes_across = flipped[0:1, :].astype(i32)
    errors_across = flipped[1:2, :]
    values_t = values.T
    for block in range(row_blocks):
        chosen = jnp.where(codes_down == order_ref[row_first + block], values, 0.0)
        for_rows[block, 0], for_rows[block, 1] = halves(chosen)
    for block in range(col_blocks):
        chosen = jnp.where(codes_across == order_ref[col_first + block], values_t, 0.0)
        for_cols[block, 0], for_cols[block, 1] = halves(chosen)
    rows_ref[...] = jnp.zeros_like(rows_ref)
    cols_ref[...] = jnp.zeros_like(cols_ref)

    def step(at, carry):
        tile = live_ref[at]
        row, col = tile // col_blocks, tile % col_blocks
        slot = at % DEPTH

        @pl.when(at + DEPTH - 1 < count)
        def _():
            fetch(at + DEPTH - 1).start()

        fetch(at).wait()
        parts = halves(held[slot])
        rows_ref[row] += dot3(parts, (for_cols[col, 0], for_cols[col, 1]))

        @pl.when(row_first + row != col_first + col)
        def _():
            cols_ref[col] += dot3((for_rows[row, 0], for_rows[row, 1]), parts)

        return carry

    lax.fori_loop(0, count, step, 0)
    first = (lax.axis_index("tr") == 0) & (lax.axis_index("tc") == 0)
    across = lax.broadcasted_iota(i32, (count_obs, count_obs), 1)
    down = lax.broadcasted_iota(i32, (count_obs, count_obs), 0)
    gram_ref[...] = jnp.zeros_like(gram_ref)

    def add_col(block, carry):
        gram_ref[...] += dot3(halves(cols_ref[block]), (for_cols[block, 0], for_cols[block, 1]))
        return carry

    lax.fori_loop(0, col_blocks, add_col, 0)
    gram_ref[...] = gram_ref[...].T + jnp.where((across == down) & first, errors_across, 0.0)

    def add_row(block, carry):
        gram_ref[...] += dot3((for_rows[block, 0], for_rows[block, 1]), halves(rows_ref[block]))
        return carry

    lax.fori_loop(0, row_blocks, add_row, 0)


def forward(block_order, packed, cov_tiles, size):
    count_obs = packed.shape[0]
    row_blocks, col_blocks = cov_tiles.shape[0] // size, cov_tiles.shape[1] // size
    tiles = row_blocks * col_blocks
    return pl.pallas_call(
        forward_kernel,
        out_shape=(
            jax.ShapeDtypeStruct((row_blocks, size, count_obs), f32),
            jax.ShapeDtypeStruct((col_blocks, count_obs, size), f32),
            jax.ShapeDtypeStruct((count_obs, count_obs), f32),
        ),
        in_specs=[SMEM, VMEM, ANY],
        out_specs=(VMEM, VMEM, VMEM),
        scratch_shapes=[
            pltpu.SMEM((tiles,), i32),
            pltpu.VMEM((DEPTH, size, size), f32),
            pltpu.SemaphoreType.DMA((DEPTH,)),
            pltpu.VMEM((row_blocks, 2, count_obs, size), bf16),
            pltpu.VMEM((col_blocks, 2, size, count_obs), bf16),
        ],
        cost_estimate=pl.CostEstimate(
            flops=6 * tiles * size * size * count_obs, bytes_accessed=2 * tiles * size * size, transcendentals=0
        ),
        name="forward",
    )(block_order, packed, cov_tiles)


def update_kernel(
    order_ref, rows_ref, cols_ref, inverse_ref, cov_ref, out_ref,
    live_ref, held, made, zeros, weighted, in_sem, out_sem, zero_sem,
):
    row_blocks, size, _ = rows_ref.shape
    col_blocks = cols_ref.shape[0]
    tiles = row_blocks * col_blocks
    zeros[...] = jnp.zeros_like(zeros)

    def blank(tile):
        return pltpu.make_async_copy(zeros, tile_at(out_ref, tile, col_blocks, size), zero_sem.at[tile])

    count = list_tiles(order_ref, live_ref, row_blocks, col_blocks)

    def fetch(at):
        slot = at % DEPTH
        return pltpu.make_async_copy(
            tile_at(cov_ref, live_ref[at], col_blocks, size), held.at[slot], in_sem.at[slot]
        )

    def put(at):
        slot = at % DEPTH
        return pltpu.make_async_copy(
            made.at[slot], tile_at(out_ref, live_ref[at], col_blocks, size), out_sem.at[slot]
        )

    for at in range(DEPTH - 1):

        @pl.when(at < count)
        def _():
            fetch(at).start()

    list_tiles(order_ref, live_ref, row_blocks, col_blocks, lambda tile: blank(tile).start())
    for block in range(col_blocks):
        weighted[block, 0], weighted[block, 1] = halves(product(inverse_ref[...], cols_ref[block], (1, 0)))

    def step(at, carry):
        tile = live_ref[at]
        row, col = tile // col_blocks, tile % col_blocks
        slot = at % DEPTH

        @pl.when(at + DEPTH - 1 < count)
        def _():
            fetch(at + DEPTH - 1).start()

        @pl.when(at >= DEPTH)
        def _():
            put(at - DEPTH).wait()

        fetch(at).wait()
        made[slot] = held[slot] - dot3(halves(rows_ref[row]), (weighted[col, 0], weighted[col, 1]))
        put(at).start()
        return carry

    lax.fori_loop(0, count, step, 0)
    lax.fori_loop(jnp.maximum(count - DEPTH, 0), count, lambda at, carry: (put(at).wait(), carry)[1], 0)
    list_tiles(order_ref, live_ref, row_blocks, col_blocks, lambda tile: blank(tile).wait())


def update(block_order, cross_rows, cross_cols, inverted, cov_tiles):
    row_blocks, size, count_obs = cross_rows.shape
    col_blocks = cross_cols.shape[0]
    tiles = row_blocks * col_blocks
    return pl.pallas_call(
        update_kernel,
        out_shape=jax.ShapeDtypeStruct(cov_tiles.shape, f32),
        in_specs=[SMEM, VMEM, VMEM, VMEM, ANY],
        out_specs=ANY,
        scratch_shapes=[
            pltpu.SMEM((tiles,), i32),
            pltpu.VMEM((DEPTH, size, size), f32),
            pltpu.VMEM((DEPTH, size, size), f32),
            pltpu.VMEM((size, size), f32),
            pltpu.VMEM((col_blocks, 2, count_obs, size), bf16),
            pltpu.SemaphoreType.DMA((DEPTH,)),
            pltpu.SemaphoreType.DMA((DEPTH,)),
            pltpu.SemaphoreType.DMA((tiles,)),
        ],
        cost_estimate=pl.CostEstimate(
            flops=3 * tiles * size * size * count_obs, bytes_accessed=6 * tiles * size * size, transcendentals=0
        ),
        name="update",
    )(block_order, cross_rows, cross_cols, inverted, cov_tiles)


def swept(matrix, work):
    size = matrix.shape[0]
    work[...] = matrix
    lanes = lax.broadcasted_iota(jnp.int32, (1, size), 1)
    rows = lax.broadcasted_iota(jnp.int32, (size, 1), 0)

    def step(pivot, carry):
        held = work[...]
        row = work[pl.ds(pivot, 1), :]
        at_lane = lanes == pivot
        at_row = rows == pivot
        column = jnp.sum(jnp.where(at_lane, held, 0.0), axis=1, keepdims=True)
        share = 1.0 / jnp.sum(jnp.where(at_lane, row, 0.0), axis=1, keepdims=True)
        kept = jnp.where(at_lane | at_row, 0.0, held)
        left = jnp.where(at_row, -1.0, column)
        right = jnp.where(at_lane, -1.0, row)
        work[...] = kept - left * (right * share)
        return carry

    lax.fori_loop(0, size, step, 0)
    return -work[...]


def inverse_of(matrix, work):
    size = matrix.shape[0]
    if size <= 128:
        return swept(matrix, work)
    half = size // 2
    upper, corner, lower = matrix[:half, :half], matrix[half:, :half], matrix[half:, half:]
    upper_inverse = inverse_of(upper, work)
    weight = product(corner, upper_inverse, (1, 0))
    lower_inverse = inverse_of(lower - product(weight, corner, (1, 1)), work)
    below = -product(lower_inverse, weight, (1, 0))
    above = upper_inverse - product(weight, below, (0, 0))
    return jnp.concatenate(
        (jnp.concatenate((above, below.T), axis=1), jnp.concatenate((below, lower_inverse), axis=1)), axis=0
    )


def inverse_kernel(matrix_ref, inverse_ref, work):
    inverse_ref[...] = inverse_of(matrix_ref[...], work)


def inverse(matrix):
    size = matrix.shape[0]
    part = size
    while part > 128:
        part //= 2
    return pl.pallas_call(
        inverse_kernel,
        out_shape=jax.ShapeDtypeStruct(matrix.shape, jnp.float32),
        in_specs=[pl.BlockSpec(memory_space=pltpu.VMEM)],
        out_specs=pl.BlockSpec(memory_space=pltpu.VMEM),
        scratch_shapes=[pltpu.VMEM((part, part), jnp.float32)],
        cost_estimate=pl.CostEstimate(flops=400_000_000, bytes_accessed=8 * size * size, transcendentals=0),
        name="inverse",
    )(matrix)


def pack(stations, obs_values, obs_error):
    values = obs_values[0]
    count, size = values.shape
    return jnp.concatenate(
        (
            values,
            stations[0].astype(f32)[:, None],
            obs_error[0][:, None],
            jnp.zeros((count, 126), f32),
        ),
        axis=1,
    )


def exchange_plain(row_part, col_part, gram_part):
    tr_size, tc_size = lax.axis_size("tr"), lax.axis_size("tc")
    row_blocks, size, count_obs = row_part.shape
    col_blocks = col_part.shape[0]
    row_part = row_part.reshape(row_blocks * size, count_obs)
    col_part = col_part.transpose(0, 2, 1).reshape(col_blocks * size, count_obs)
    innovation = lax.psum(gram_part, ("tr", "tc"))
    count = tr_size * tc_size
    to_rows = [((q % tr_size) * tc_size + q // tr_size, q) for q in range(count)]
    to_cols = [(there, here) for here, there in to_rows]
    col_chunk = lax.psum_scatter(col_part, "tr", scatter_dimension=0, tiled=True)
    row_chunk = lax.psum_scatter(row_part, "tc", scatter_dimension=0, tiled=True)
    chunk = row_chunk + lax.ppermute(col_chunk, ("tr", "tc"), to_rows)
    cross_rows = lax.all_gather(chunk, "tc", axis=0, tiled=True)
    cross_cols = lax.all_gather(lax.ppermute(chunk, ("tr", "tc"), to_cols), "tr", axis=0, tiled=True)
    return (
        cross_rows.reshape(row_blocks, size, count_obs),
        cross_cols.reshape(col_blocks, size, count_obs).transpose(0, 2, 1),
        innovation,
    )


class Sems:
    def __init__(self):
        self.count = 0

    def take(self, number=1):
        self.count += number
        return self.count - number


def share_kernel(mine_ref, all_ref, send, recv):
    row, col = lax.axis_index("tr"), lax.axis_index("tc")
    many = all_ref.shape[0]
    copies = [
        pltpu.make_async_remote_copy(
            mine_ref, all_ref.at[col], send.at[step], recv.at[step],
            device_id=(row, lax.rem(col + step, many)), device_id_type=pl.DeviceIdType.MESH,
        )
        for step in range(1, many)
    ]
    for copy in copies:
        copy.start()
    all_ref[col] = mine_ref[...]
    for copy in copies:
        copy.wait_send()
    for step in range(1, many):
        pltpu.make_async_remote_copy(
            mine_ref, all_ref.at[lax.rem(col + many - step, many)], send.at[step], recv.at[step],
            device_id=(row, lax.rem(col + step, many)), device_id_type=pl.DeviceIdType.MESH,
        ).wait_recv()


def share(packed):
    many = lax.axis_size("tc")
    full = pl.pallas_call(
        share_kernel,
        out_shape=jax.ShapeDtypeStruct((many, *packed.shape), f32),
        in_specs=[VMEM],
        out_specs=VMEM,
        scratch_shapes=[pltpu.SemaphoreType.DMA((many,)), pltpu.SemaphoreType.DMA((many,))],
        compiler_params=pltpu.CompilerParams(has_side_effects=True),
        name="share",
    )(packed)
    return full.reshape(many * packed.shape[0], packed.shape[1])


def exchange_kernel(
    count_bits, row_ref, col_ref, gram_ref, rows_out, cols_out, gram_out,
    send, recv, from_core, sums, landed, upward, downward, rows_here, cols_here, total,
    gram_work, gram_core, gram_bits, gram_line,
):
    sems = Sems()
    line = lax.axis_size("tr")
    z, j = lax.axis_index("tr"), lax.axis_index("tc")
    chip, core = j // 2, j % 2
    parts = count_bits
    width = rows_here.shape[1]
    pending = []
    beside = (z, 2 * chip + 1 - core)

    def copy(source, target, sem, device=beside):
        return pltpu.make_async_remote_copy(
            source, target, send.at[sem], recv.at[sem], device_id=device, device_id_type=pl.DeviceIdType.MESH
        )

    def begin(source, target, device):
        made = copy(source, target, sems.take(), device)
        made.start()
        pending.append(made)
        return made

    def bit(number):
        return chip // 2**number % 2

    def across(number):
        return z, 2 * (chip + (1 - 2 * bit(number)) * 2**number) + core

    up, down = sems.take(line), sems.take(line)

    def line_begin(step):
        chunk, other = line - step, step - 1

        @pl.when(z == 0)
        def _():
            copy(col_ref.at[chunk], upward.at[chunk], up + chunk, (z + 1, j)).start()

        @pl.when(z == line - 1)
        def _():
            copy(col_ref.at[other], downward.at[other], down + other, (z - 1, j)).start()

    def line_pass(step):
        chunk, other = line - step, step - 1

        @pl.when((z > 0) & (z < chunk))
        def _():
            copy(upward.at[chunk], upward.at[chunk], up + chunk).wait_recv()
            upward[chunk] += col_ref[chunk]
            copy(upward.at[chunk], upward.at[chunk], up + chunk, (z + 1, j)).start()

        @pl.when((z < line - 1) & (z > other))
        def _():
            copy(downward.at[other], downward.at[other], down + other).wait_recv()
            downward[other] += col_ref[other]
            copy(downward.at[other], downward.at[other], down + other, (z - 1, j)).start()

    def line_end():
        total[...] = col_ref[z]

        @pl.when(z > 0)
        def _():
            copy(upward.at[z], upward.at[z], up + z).wait_recv()
            total[...] += upward[z]

        @pl.when(z < line - 1)
        def _():
            copy(downward.at[z], downward.at[z], down + z).wait_recv()
            total[...] += downward[z]

    def line_sent():
        for step in range(1, line):
            chunk, other = line - step, step - 1

            @pl.when(z < chunk)
            def _():
                copy(upward.at[chunk], upward.at[chunk], up + chunk).wait_send()

            @pl.when(z > other)
            def _():
                copy(downward.at[other], downward.at[other], down + other).wait_send()

    def chosen(part, step, flip):
        order = [(part + turn) % count_bits for turn in range(count_bits)]
        free = order[step + 1:]
        picks = []
        for pick in range(2 ** len(free)):
            where = 0
            for turn, number in enumerate(order):
                if number in free:
                    value = pick // 2 ** free.index(number) % 2
                elif turn == step and flip:
                    value = 1 - bit(number)
                else:
                    value = bit(number)
                where = where + value * 2**number
            picks.append(where)
        return order[step], picks

    step_base = [0]
    for step in range(count_bits):
        step_base.append(step_base[-1] + parts * 2 ** (count_bits - 1 - step))

    def plane_send(step):
        made = []
        for part in range(parts):
            number, picks = chosen(part, step, True)
            for slot, pick in enumerate(picks):
                at = step_base[step] + part * len(picks) + slot
                made.append(begin(sums.at[pick, part], landed.at[at], across(number)))
        return made

    def plane_add(step, made):
        for one in made:
            one.wait_recv()
        for part in range(parts):
            _, picks = chosen(part, step, False)
            for slot, pick in enumerate(picks):
                sums[pick, part] += landed[step_base[step] + part * len(picks) + slot]

    line_begin(1)
    held = 2**count_bits
    half = begin(gram_ref.at[pl.ds((1 - core) * held, held)], gram_core, beside)
    core_sum = begin(row_ref.at[1 - core], from_core, beside)
    half.wait_recv()
    gram_work[pl.ds(core * held, held)] = gram_ref[pl.ds(core * held, held)] + gram_core[...]
    for number in reversed(range(count_bits)):
        size = 2**number
        start = core * held + chip // (2 * size) * (2 * size)
        keep, give = start + bit(number) * size, start + (1 - bit(number)) * size
        begin(gram_work.at[pl.ds(give, size)], gram_bits.at[pl.ds(size, size)], across(number)).wait_recv()
        gram_work[pl.ds(keep, size)] += gram_bits[pl.ds(size, size)]
    mine = core * held + chip
    gram_line[z] = gram_work[mine]
    base = sems.take(line)
    for step in range(1, line):
        copy(gram_work.at[mine], gram_line.at[z], base + step, (lax.rem(z + step, line), j)).start()
    for step in range(2, line):
        line_begin(step)

    core_sum.wait_recv()
    sums[...] = row_ref[core] + from_core[...]
    made = plane_send(0)
    for step in range(1, line):
        copy(gram_work.at[mine], gram_line.at[lax.rem(z + line - step, line)], base + step).wait()
    gram_out[mine] = sum(gram_line[step] for step in range(line))
    line_pass(1)
    for number in range(count_bits):
        size = 2**number
        start = core * held + chip // size * size
        begin(gram_out.at[pl.ds(start, size)], gram_out.at[pl.ds(start, size)], across(number)).wait_recv()
    begin(gram_out.at[pl.ds(core * held, held)], gram_out.at[pl.ds(core * held, held)], beside).wait_recv()
    for step in range(1, max(line - 1, count_bits)):
        if step < count_bits:
            plane_add(step - 1, made)
            made = plane_send(step)
        if step + 1 < line - 1:
            line_pass(step + 1)
    plane_add(count_bits - 1, made)

    to_rows, to_cols = sems.take(), sems.take()
    partner = (chip, 2 * z + core)
    apart = z != chip

    @pl.when(apart)
    def _():
        copy(sums.at[chip], rows_here, to_rows, partner).start()

    if line > 2:
        line_pass(line - 1)
    line_end()

    @pl.when(apart)
    def _():
        copy(total, cols_here, to_cols, partner).start()
        copy(sums.at[chip], rows_here, to_rows, partner).wait()

    @pl.when(jnp.logical_not(apart))
    def _():
        rows_here[...] = sums[chip]
        cols_here[...] = total[...]

    for part in range(parts):
        lanes = slice(part * width, (part + 1) * width)
        cols_out[z, :, lanes] = total[:, lanes] + rows_here[part].T
    around, back = sems.take(line), sems.take(line)

    def line_spread(step):
        chunk, other = z - (step - 1), z + (step - 1)

        @pl.when(chunk >= 0)
        def _():
            if step > 1:
                copy(cols_out.at[chunk], cols_out.at[chunk], around + chunk).wait_recv()

            @pl.when(z < line - 1)
            def _():
                copy(cols_out.at[chunk], cols_out.at[chunk], around + chunk, (z + 1, j)).start()

        @pl.when(other < line)
        def _():
            if step > 1:
                copy(cols_out.at[other], cols_out.at[other], back + other).wait_recv()

            @pl.when(z > 0)
            def _():
                copy(cols_out.at[other], cols_out.at[other], back + other, (z - 1, j)).start()

    def line_spread_sent():
        for step in range(1, line + 1):
            chunk, other = z - (step - 1), z + (step - 1)

            @pl.when((chunk >= 0) & (z < line - 1))
            def _():
                copy(cols_out.at[chunk], cols_out.at[chunk], around + chunk).wait_send()

            @pl.when((other < line) & (z > 0))
            def _():
                copy(cols_out.at[other], cols_out.at[other], back + other).wait_send()

    line_spread(1)

    @pl.when(apart)
    def _():
        copy(total, cols_here, to_cols, partner).wait()

    for part in range(parts):
        lanes = slice(part * width, (part + 1) * width)
        rows_out[core, chip, part] = sums[chip, part] + cols_here[:, lanes].T

    made = []
    for turn in range(max(line, count_bits + 1)):
        for one in made:
            one.wait_recv()
        made = []
        if turn < count_bits:
            for part in range(parts):
                number, picks = chosen(part, count_bits - 1 - turn, False)
                for pick in picks:
                    spot = rows_out.at[core, pick, part]
                    made.append(begin(spot, spot, across(number)))
        elif turn == count_bits:
            made = [begin(rows_out.at[core], rows_out.at[core], beside)]
        if 1 <= turn < line:
            line_spread(turn + 1)
    for one in made:
        one.wait_recv()
    line_spread_sent()
    line_sent()
    for one in pending:
        one.wait_send()


def exchange(row_part, col_part, gram_part):
    line, many = lax.axis_size("tr"), lax.axis_size("tc")
    count_bits = line.bit_length() - 1
    row_blocks, size, count_obs = row_part.shape
    parts, width = count_bits, size // count_bits
    seg = count_obs // many
    rows = (2, line, parts, width, count_obs)
    cols = col_part.shape
    gram = (many, seg, count_obs)
    landings = sum(parts * 2 ** (count_bits - 1 - step) for step in range(count_bits))
    cross_rows, cross_cols, innovation = pl.pallas_call(
        functools.partial(exchange_kernel, count_bits),
        out_shape=tuple(jax.ShapeDtypeStruct(shape, f32) for shape in (rows, cols, gram)),
        in_specs=[VMEM] * 3,
        out_specs=(VMEM,) * 3,
        scratch_shapes=[
            pltpu.SemaphoreType.DMA((96,)),
            pltpu.SemaphoreType.DMA((96,)),
            pltpu.VMEM(rows[1:], f32),
            pltpu.VMEM(rows[1:], f32),
            pltpu.VMEM((landings, width, count_obs), f32),
            pltpu.VMEM(cols, f32),
            pltpu.VMEM(cols, f32),
            pltpu.VMEM(rows[2:], f32),
            pltpu.VMEM(cols[1:], f32),
            pltpu.VMEM(cols[1:], f32),
            pltpu.VMEM(gram, f32),
            pltpu.VMEM((many // 2, seg, count_obs), f32),
            pltpu.VMEM((many // 2, seg, count_obs), f32),
            pltpu.VMEM((line, seg, count_obs), f32),
        ],
        compiler_params=pltpu.CompilerParams(has_side_effects=True),
        name="exchange",
    )(row_part.reshape(rows), col_part, gram_part.reshape(gram))
    return cross_rows.reshape(row_part.shape), cross_cols, innovation.reshape(gram_part.shape)


def body(cov_tiles, block_order, stations, obs_values, obs_error):
    size = obs_values.shape[2]
    line, many = lax.axis_size("tr"), lax.axis_size("tc")
    packed = share(pack(stations, obs_values, obs_error))
    row_part, col_part, gram_part = forward(block_order, packed, cov_tiles, size)
    square = many == 2 * line and line & (line - 1) == 0 and line > 1
    whole_tiles = row_part.shape[0] == many and col_part.shape[0] == line
    spread = exchange if square and whole_tiles else exchange_plain
    cross_rows, cross_cols, innovation = spread(row_part, col_part, gram_part)
    return update(block_order, cross_rows, cross_cols, inverse(innovation), cov_tiles)


def solution(mesh):
    in_specs = (P("tr", "tc"), P(), P(None, "tc"), P(None, "tc", None), P(None, "tc"))
    out_specs = P("tr", "tc")
    return jax.shard_map(body, mesh=mesh, in_specs=in_specs, out_specs=out_specs, check_vma=False)
```

```python
import functools

import jax
import jax.numpy as jnp
from jax import lax
from jax.experimental import pallas as pl
from jax.experimental.pallas import tpu as pltpu
from jax.sharding import PartitionSpec as P

exact = lax.Precision.HIGHEST
bf16, f32, i32 = jnp.bfloat16, jnp.float32, jnp.int32
DEPTH = 4
ANY = pl.BlockSpec(memory_space=pl.ANY)
VMEM = pl.BlockSpec(memory_space=pltpu.VMEM)
SMEM = pl.BlockSpec(memory_space=pltpu.SMEM)


def product(former, latter, over, precision=exact):
    return lax.dot_general(
        former,
        latter,
        (((over[0],), (over[1],)), ((), ())),
        precision=precision,
        preferred_element_type=jnp.float32,
    )


def halves(array):
    high = array.astype(bf16)
    return high, (array - high.astype(f32)).astype(bf16)


def dot(former, latter):
    return jnp.dot(former, latter, preferred_element_type=f32)


def dot3(former, latter):
    return dot(former[0], latter[0]) + dot(former[0], latter[1]) + dot(former[1], latter[0])


def list_tiles(order_ref, live_ref, row_blocks, col_blocks, when_dead=None):
    row_first = lax.axis_index("tr") * row_blocks
    col_first = lax.axis_index("tc") * col_blocks

    def step(tile, count):
        row, col = tile // col_blocks, tile % col_blocks
        p, q = row_first + row, col_first + col
        live = (order_ref[p] > order_ref[q]) | (p == q)

        @pl.when(live)
        def _():
            live_ref[count] = tile

        if when_dead is not None:

            @pl.when(jnp.logical_not(live))
            def _():
                when_dead(tile)

        return count + live.astype(i32)

    return lax.fori_loop(0, row_blocks * col_blocks, step, jnp.int32(0))


def tile_at(ref, tile, col_blocks, size):
    row, col = tile // col_blocks, tile % col_blocks
    return ref.at[
        pl.ds(pl.multiple_of(row * size, size), size), pl.ds(pl.multiple_of(col * size, size), size)
    ]


def forward_kernel(
    order_ref, packed_ref, cov_ref, rows_ref, cols_ref, gram_ref,
    live_ref, held, sem, for_rows, for_cols,
):
    row_blocks, size, count_obs = rows_ref.shape
    col_blocks = cols_ref.shape[0]
    row_first = lax.axis_index("tr") * row_blocks
    col_first = lax.axis_index("tc") * col_blocks
    count = list_tiles(order_ref, live_ref, row_blocks, col_blocks)

    def fetch(at):
        slot = at % DEPTH
        return pltpu.make_async_copy(
            tile_at(cov_ref, live_ref[at], col_blocks, size), held.at[slot], sem.at[slot]
        )

    for at in range(DEPTH - 1):

        @pl.when(at < count)
        def _():
            fetch(at).start()

    values = packed_ref[:, :size]
    extras = packed_ref[:, size:]
    codes_down = extras[:, 0:1].astype(i32)
    flipped = extras.T
    codes_across = flipped[0:1, :].astype(i32)
    errors_across = flipped[1:2, :]
    values_t = values.T
    for block in range(row_blocks):
        chosen = jnp.where(codes_down == order_ref[row_first + block], values, 0.0)
        for_rows[block, 0], for_rows[block, 1] = halves(chosen)
    for block in range(col_blocks):
        chosen = jnp.where(codes_across == order_ref[col_first + block], values_t, 0.0)
        for_cols[block, 0], for_cols[block, 1] = halves(chosen)
    rows_ref[...] = jnp.zeros_like(rows_ref)
    cols_ref[...] = jnp.zeros_like(cols_ref)

    def step(at, carry):
        tile = live_ref[at]
        row, col = tile // col_blocks, tile % col_blocks
        slot = at % DEPTH

        @pl.when(at + DEPTH - 1 < count)
        def _():
            fetch(at + DEPTH - 1).start()

        fetch(at).wait()
        parts = halves(held[slot])
        rows_ref[row] += dot3(parts, (for_cols[col, 0], for_cols[col, 1]))

        @pl.when(row_first + row != col_first + col)
        def _():
            cols_ref[col] += dot3((for_rows[row, 0], for_rows[row, 1]), parts)

        return carry

    lax.fori_loop(0, count, step, 0)
    first = (lax.axis_index("tr") == 0) & (lax.axis_index("tc") == 0)
    across = lax.broadcasted_iota(i32, (count_obs, count_obs), 1)
    down = lax.broadcasted_iota(i32, (count_obs, count_obs), 0)
    gram_ref[...] = jnp.zeros_like(gram_ref)

    def add_col(block, carry):
        gram_ref[...] += dot3(halves(cols_ref[block]), (for_cols[block, 0], for_cols[block, 1]))
        return carry

    lax.fori_loop(0, col_blocks, add_col, 0)
    gram_ref[...] = gram_ref[...].T + jnp.where((across == down) & first, errors_across, 0.0)

    def add_row(block, carry):
        gram_ref[...] += dot3((for_rows[block, 0], for_rows[block, 1]), halves(rows_ref[block]))
        return carry

    lax.fori_loop(0, row_blocks, add_row, 0)


def forward(block_order, packed, cov_tiles, size):
    count_obs = packed.shape[0]
    row_blocks, col_blocks = cov_tiles.shape[0] // size, cov_tiles.shape[1] // size
    tiles = row_blocks * col_blocks
    return pl.pallas_call(
        forward_kernel,
        out_shape=(
            jax.ShapeDtypeStruct((row_blocks, size, count_obs), f32),
            jax.ShapeDtypeStruct((col_blocks, count_obs, size), f32),
            jax.ShapeDtypeStruct((count_obs, count_obs), f32),
        ),
        in_specs=[SMEM, VMEM, ANY],
        out_specs=(VMEM, VMEM, VMEM),
        scratch_shapes=[
            pltpu.SMEM((tiles,), i32),
            pltpu.VMEM((DEPTH, size, size), f32),
            pltpu.SemaphoreType.DMA((DEPTH,)),
            pltpu.VMEM((row_blocks, 2, count_obs, size), bf16),
            pltpu.VMEM((col_blocks, 2, size, count_obs), bf16),
        ],
        cost_estimate=pl.CostEstimate(
            flops=6 * tiles * size * size * count_obs, bytes_accessed=2 * tiles * size * size, transcendentals=0
        ),
        name="forward",
    )(block_order, packed, cov_tiles)


def update_kernel(
    order_ref, rows_ref, cols_ref, inverse_ref, cov_ref, out_ref,
    live_ref, held, made, zeros, weighted, in_sem, out_sem, zero_sem,
):
    row_blocks, size, _ = rows_ref.shape
    col_blocks = cols_ref.shape[0]
    tiles = row_blocks * col_blocks
    zeros[...] = jnp.zeros_like(zeros)

    def blank(tile):
        return pltpu.make_async_copy(zeros, tile_at(out_ref, tile, col_blocks, size), zero_sem.at[tile])

    count = list_tiles(order_ref, live_ref, row_blocks, col_blocks)

    def fetch(at):
        slot = at % DEPTH
        return pltpu.make_async_copy(
            tile_at(cov_ref, live_ref[at], col_blocks, size), held.at[slot], in_sem.at[slot]
        )

    def put(at):
        slot = at % DEPTH
        return pltpu.make_async_copy(
            made.at[slot], tile_at(out_ref, live_ref[at], col_blocks, size), out_sem.at[slot]
        )

    for at in range(DEPTH - 1):

        @pl.when(at < count)
        def _():
            fetch(at).start()

    list_tiles(order_ref, live_ref, row_blocks, col_blocks, lambda tile: blank(tile).start())
    for block in range(col_blocks):
        weighted[block, 0], weighted[block, 1] = halves(product(inverse_ref[...], cols_ref[block], (1, 0)))

    def step(at, carry):
        tile = live_ref[at]
        row, col = tile // col_blocks, tile % col_blocks
        slot = at % DEPTH

        @pl.when(at + DEPTH - 1 < count)
        def _():
            fetch(at + DEPTH - 1).start()

        @pl.when(at >= DEPTH)
        def _():
            put(at - DEPTH).wait()

        fetch(at).wait()
        made[slot] = held[slot] - dot3(halves(rows_ref[row]), (weighted[col, 0], weighted[col, 1]))
        put(at).start()
        return carry

    lax.fori_loop(0, count, step, 0)
    lax.fori_loop(jnp.maximum(count - DEPTH, 0), count, lambda at, carry: (put(at).wait(), carry)[1], 0)
    list_tiles(order_ref, live_ref, row_blocks, col_blocks, lambda tile: blank(tile).wait())


def update(block_order, cross_rows, cross_cols, inverted, cov_tiles):
    row_blocks, size, count_obs = cross_rows.shape
    col_blocks = cross_cols.shape[0]
    tiles = row_blocks * col_blocks
    return pl.pallas_call(
        update_kernel,
        out_shape=jax.ShapeDtypeStruct(cov_tiles.shape, f32),
        in_specs=[SMEM, VMEM, VMEM, VMEM, ANY],
        out_specs=ANY,
        scratch_shapes=[
            pltpu.SMEM((tiles,), i32),
            pltpu.VMEM((DEPTH, size, size), f32),
            pltpu.VMEM((DEPTH, size, size), f32),
            pltpu.VMEM((size, size), f32),
            pltpu.VMEM((col_blocks, 2, count_obs, size), bf16),
            pltpu.SemaphoreType.DMA((DEPTH,)),
            pltpu.SemaphoreType.DMA((DEPTH,)),
            pltpu.SemaphoreType.DMA((tiles,)),
        ],
        cost_estimate=pl.CostEstimate(
            flops=3 * tiles * size * size * count_obs, bytes_accessed=6 * tiles * size * size, transcendentals=0
        ),
        name="update",
    )(block_order, cross_rows, cross_cols, inverted, cov_tiles)


def swept(matrix, work):
    size = matrix.shape[0]
    work[...] = matrix
    lanes = lax.broadcasted_iota(jnp.int32, (1, size), 1)
    rows = lax.broadcasted_iota(jnp.int32, (size, 1), 0)

    def step(pivot, carry):
        held = work[...]
        row = work[pl.ds(pivot, 1), :]
        at_lane = lanes == pivot
        at_row = rows == pivot
        column = jnp.sum(jnp.where(at_lane, held, 0.0), axis=1, keepdims=True)
        share = 1.0 / jnp.sum(jnp.where(at_lane, row, 0.0), axis=1, keepdims=True)
        kept = jnp.where(at_lane | at_row, 0.0, held)
        left = jnp.where(at_row, -1.0, column)
        right = jnp.where(at_lane, -1.0, row)
        work[...] = kept - left * (right * share)
        return carry

    quarter = size // 4
    for turn in range(4):
        lax.fori_loop(turn * quarter, (turn + 1) * quarter, step, 0)
        yield
    return -work[...]


def inverse_of(matrix, work):
    size = matrix.shape[0]
    if size <= 128:
        return (yield from swept(matrix, work))
    half = size // 2
    upper, corner, lower = matrix[:half, :half], matrix[half:, :half], matrix[half:, half:]
    upper_inverse = yield from inverse_of(upper, work)
    weight = product(corner, upper_inverse, (1, 0))
    lower_inverse = yield from inverse_of(lower - product(weight, corner, (1, 1)), work)
    below = -product(lower_inverse, weight, (1, 0))
    above = upper_inverse - product(weight, below, (0, 0))
    return jnp.concatenate(
        (jnp.concatenate((above, below.T), axis=1), jnp.concatenate((below, lower_inverse), axis=1)), axis=0
    )


def inverse_steps(matrix_ref, inverse_ref, work):
    size = matrix_ref.shape[-1]
    inverse_ref[...] = yield from inverse_of(matrix_ref[...].reshape(size, size), work)


def inverse_kernel(matrix_ref, inverse_ref, work):
    for _ in inverse_steps(matrix_ref, inverse_ref, work):
        pass


def pivot_size(size):
    return size if size <= 128 else pivot_size(size // 2)


def inverse(matrix):
    size = matrix.shape[0]
    part = pivot_size(size)
    return pl.pallas_call(
        inverse_kernel,
        out_shape=jax.ShapeDtypeStruct(matrix.shape, jnp.float32),
        in_specs=[VMEM],
        out_specs=VMEM,
        scratch_shapes=[pltpu.VMEM((part, part), jnp.float32)],
        cost_estimate=pl.CostEstimate(flops=400_000_000, bytes_accessed=8 * size * size, transcendentals=0),
        name="inverse",
    )(matrix)


def pack(stations, obs_values, obs_error):
    values = obs_values[0]
    count, size = values.shape
    return jnp.concatenate(
        (
            values,
            stations[0].astype(f32)[:, None],
            obs_error[0][:, None],
            jnp.zeros((count, 126), f32),
        ),
        axis=1,
    )


def exchange_plain(row_part, col_part, gram_part):
    tr_size, tc_size = lax.axis_size("tr"), lax.axis_size("tc")
    row_blocks, size, count_obs = row_part.shape
    col_blocks = col_part.shape[0]
    row_part = row_part.reshape(row_blocks * size, count_obs)
    col_part = col_part.transpose(0, 2, 1).reshape(col_blocks * size, count_obs)
    innovation = lax.psum(gram_part, ("tr", "tc"))
    count = tr_size * tc_size
    to_rows = [((q % tr_size) * tc_size + q // tr_size, q) for q in range(count)]
    to_cols = [(there, here) for here, there in to_rows]
    col_chunk = lax.psum_scatter(col_part, "tr", scatter_dimension=0, tiled=True)
    row_chunk = lax.psum_scatter(row_part, "tc", scatter_dimension=0, tiled=True)
    chunk = row_chunk + lax.ppermute(col_chunk, ("tr", "tc"), to_rows)
    cross_rows = lax.all_gather(chunk, "tc", axis=0, tiled=True)
    cross_cols = lax.all_gather(lax.ppermute(chunk, ("tr", "tc"), to_cols), "tr", axis=0, tiled=True)
    return (
        cross_rows.reshape(row_blocks, size, count_obs),
        cross_cols.reshape(col_blocks, size, count_obs).transpose(0, 2, 1),
        inverse(innovation),
    )


class Sems:
    def __init__(self):
        self.count = 0

    def take(self, number=1):
        self.count += number
        return self.count - number


def share_kernel(mine_ref, all_ref, send, recv, core_send, core_recv):
    row, col = lax.axis_index("tr"), lax.axis_index("tc")
    chips = all_ref.shape[0] // 2
    chip, core = col // 2, col % 2

    def copy(source, block, step):
        return pltpu.make_async_remote_copy(
            source, all_ref.at[block], send.at[step], recv.at[step],
            device_id=(row, 2 * lax.rem(chip + step, chips) + core), device_id_type=pl.DeviceIdType.MESH,
        )

    def beside(source, block, step):
        return pltpu.make_async_remote_copy(
            source, all_ref.at[block], core_send.at[step], core_recv.at[step],
            device_id=(row, 2 * chip + 1 - core), device_id_type=pl.DeviceIdType.MESH,
        )

    sent = [copy(mine_ref, col, step) for step in range(1, chips)]
    sent.append(beside(mine_ref, col, 0))
    for one in sent:
        one.start()
    all_ref[col] = mine_ref[...]
    for step in range(1, chips):
        block = 2 * lax.rem(chip + chips - step, chips) + core
        copy(mine_ref, block, step).wait_recv()
        sent.append(beside(all_ref.at[block], block, step))
        sent[-1].start()
    for step in range(chips):
        beside(mine_ref, 2 * lax.rem(chip + chips - step, chips) + 1 - core, step).wait_recv()
    for one in sent:
        one.wait_send()


def share(packed):
    many = lax.axis_size("tc")
    full = pl.pallas_call(
        share_kernel,
        out_shape=jax.ShapeDtypeStruct((many, *packed.shape), f32),
        in_specs=[VMEM],
        out_specs=VMEM,
        scratch_shapes=[pltpu.SemaphoreType.DMA((many // 2,))] * 4,
        compiler_params=pltpu.CompilerParams(has_side_effects=True),
        name="share",
    )(packed)
    return full.reshape(many * packed.shape[0], packed.shape[1])


def exchange_kernel(
    count_bits, row_ref, col_ref, gram_ref, rows_out, cols_out, inverse_out,
    gram_out, work, send, recv, from_core, sums, landed, upward, downward, rows_here, cols_here, total,
    gram_work, gram_core, gram_bits, gram_line,
):
    sems = Sems()
    line = lax.axis_size("tr")
    z, j = lax.axis_index("tr"), lax.axis_index("tc")
    chip, core = j // 2, j % 2
    parts = count_bits
    width = rows_here.shape[1]
    pending = []
    beside = (z, 2 * chip + 1 - core)

    def copy(source, target, sem, device=beside):
        return pltpu.make_async_remote_copy(
            source, target, send.at[sem], recv.at[sem], device_id=device, device_id_type=pl.DeviceIdType.MESH
        )

    def begin(source, target, device):
        made = copy(source, target, sems.take(), device)
        made.start()
        pending.append(made)
        return made

    def bit(number):
        return chip // 2**number % 2

    def across(number):
        return z, 2 * (chip + (1 - 2 * bit(number)) * 2**number) + core

    up, down = sems.take(line), sems.take(line)

    def line_begin(step):
        chunk, other = line - step, step - 1

        @pl.when(z == 0)
        def _():
            copy(col_ref.at[chunk], upward.at[chunk], up + chunk, (z + 1, j)).start()

        @pl.when(z == line - 1)
        def _():
            copy(col_ref.at[other], downward.at[other], down + other, (z - 1, j)).start()

    def line_round(step):
        chunk, other = z + line - 1 - step, z - line + 1 + step

        @pl.when((z > 0) & (chunk < line))
        def _():
            copy(upward.at[chunk], upward.at[chunk], up + chunk).wait_recv()
            upward[chunk] += col_ref[chunk]
            copy(upward.at[chunk], upward.at[chunk], up + chunk, (z + 1, j)).start()

        @pl.when((z < line - 1) & (other >= 0))
        def _():
            copy(downward.at[other], downward.at[other], down + other).wait_recv()
            downward[other] += col_ref[other]
            copy(downward.at[other], downward.at[other], down + other, (z - 1, j)).start()

    def line_end():
        total[...] = col_ref[z]

        @pl.when(z > 0)
        def _():
            copy(upward.at[z], upward.at[z], up + z).wait_recv()
            total[...] += upward[z]

        @pl.when(z < line - 1)
        def _():
            copy(downward.at[z], downward.at[z], down + z).wait_recv()
            total[...] += downward[z]

    def line_sent():
        for step in range(1, line):
            chunk, other = line - step, step - 1

            @pl.when(z < chunk)
            def _():
                copy(upward.at[chunk], upward.at[chunk], up + chunk).wait_send()

            @pl.when(z > other)
            def _():
                copy(downward.at[other], downward.at[other], down + other).wait_send()

    def chosen(part, step, flip):
        order = [(part + turn) % count_bits for turn in range(count_bits)]
        free = order[step + 1:]
        picks = []
        for pick in range(2 ** len(free)):
            where = 0
            for turn, number in enumerate(order):
                if number in free:
                    value = pick // 2 ** free.index(number) % 2
                elif turn == step and flip:
                    value = 1 - bit(number)
                else:
                    value = bit(number)
                where = where + value * 2**number
            picks.append(where)
        return order[step], picks

    step_base = [0]
    for step in range(count_bits):
        step_base.append(step_base[-1] + parts * 2 ** (count_bits - 1 - step))

    def plane_send(step):
        made = []
        for part in range(parts):
            number, picks = chosen(part, step, True)
            for slot, pick in enumerate(picks):
                at = step_base[step] + part * len(picks) + slot
                made.append(begin(sums.at[pick, part], landed.at[at], across(number)))
        return made

    def plane_add(step, made):
        for one in made:
            one.wait_recv()
        for part in range(parts):
            _, picks = chosen(part, step, False)
            for slot, pick in enumerate(picks):
                sums[pick, part] += landed[step_base[step] + part * len(picks) + slot]

    line_begin(1)
    held = 2**count_bits
    half = begin(gram_ref.at[pl.ds((1 - core) * held, held)], gram_core, beside)
    core_sum = begin(row_ref.at[1 - core], from_core, beside)
    half.wait_recv()
    gram_work[pl.ds(core * held, held)] = gram_ref[pl.ds(core * held, held)] + gram_core[...]
    for number in reversed(range(count_bits)):
        size = 2**number
        start = core * held + chip // (2 * size) * (2 * size)
        keep, give = start + bit(number) * size, start + (1 - bit(number)) * size
        begin(gram_work.at[pl.ds(give, size)], gram_bits.at[pl.ds(size, size)], across(number)).wait_recv()
        gram_work[pl.ds(keep, size)] += gram_bits[pl.ds(size, size)]
    mine = core * held + chip
    gram_line[z] = gram_work[mine]
    base = sems.take(line)
    for step in range(1, line):
        copy(gram_work.at[mine], gram_line.at[z], base + step, (lax.rem(z + step, line), j)).start()
    for step in range(2, line):
        line_begin(step)

    core_sum.wait_recv()
    sums[...] = row_ref[core] + from_core[...]
    made = plane_send(0)

    def gram_back():
        for step in range(1, line):
            copy(gram_work.at[mine], gram_line.at[lax.rem(z + line - step, line)], base + step).wait()
        gram_out[mine] = sum(gram_line[step] for step in range(line))
        for number in range(count_bits):
            size = 2**number
            spot = gram_out.at[pl.ds(core * held + chip // size * size, size)]
            sent = begin(spot, spot, across(number))
            yield
            sent.wait_recv()
        spot = gram_out.at[pl.ds(core * held, held)]
        sent = begin(spot, spot, beside)
        yield
        sent.wait_recv()

    gram_turns = gram_back()
    for step in range(1, line - 1):
        line_round(step)
        next(gram_turns, None)
        if step < count_bits:
            plane_add(step - 1, made)
            made = plane_send(step)
            next(gram_turns, None)
    for _ in gram_turns:
        pass
    for step in range(max(line - 1, 1), count_bits):
        plane_add(step - 1, made)
        made = plane_send(step)
    plane_add(count_bits - 1, made)
    inverse_turns = inverse_steps(gram_out, inverse_out, work)

    def fill(number):
        for _ in range(number):
            next(inverse_turns, None)

    to_rows, to_cols = sems.take(), sems.take()
    partner = (chip, 2 * z + core)
    apart = z != chip

    @pl.when(apart)
    def _():
        copy(sums.at[chip], rows_here, to_rows, partner).start()

    fill(1)
    line_end()

    @pl.when(apart)
    def _():
        copy(total, cols_here, to_cols, partner).start()
        copy(sums.at[chip], rows_here, to_rows, partner).wait()

    @pl.when(jnp.logical_not(apart))
    def _():
        rows_here[...] = sums[chip]
        cols_here[...] = total[...]

    for part in range(parts):
        lanes = slice(part * width, (part + 1) * width)
        cols_out[z, :, lanes] = total[:, lanes] + rows_here[part].T
    around, back = sems.take(line), sems.take(line)

    def line_spread(step):
        chunk, other = z - (step - 1), z + (step - 1)

        @pl.when(chunk >= 0)
        def _():
            if step > 1:
                copy(cols_out.at[chunk], cols_out.at[chunk], around + chunk).wait_recv()

            @pl.when(z < line - 1)
            def _():
                copy(cols_out.at[chunk], cols_out.at[chunk], around + chunk, (z + 1, j)).start()

        @pl.when(other < line)
        def _():
            if step > 1:
                copy(cols_out.at[other], cols_out.at[other], back + other).wait_recv()

            @pl.when(z > 0)
            def _():
                copy(cols_out.at[other], cols_out.at[other], back + other, (z - 1, j)).start()

    def line_spread_sent():
        for step in range(1, line + 1):
            chunk, other = z - (step - 1), z + (step - 1)

            @pl.when((chunk >= 0) & (z < line - 1))
            def _():
                copy(cols_out.at[chunk], cols_out.at[chunk], around + chunk).wait_send()

            @pl.when((other < line) & (z > 0))
            def _():
                copy(cols_out.at[other], cols_out.at[other], back + other).wait_send()

    line_spread(1)
    fill(2)

    @pl.when(apart)
    def _():
        copy(total, cols_here, to_cols, partner).wait()

    for part in range(parts):
        lanes = slice(part * width, (part + 1) * width)
        rows_out[core, chip, part] = sums[chip, part] + cols_here[:, lanes].T

    def plane_spread(turn):
        if turn == count_bits:
            return [begin(rows_out.at[core], rows_out.at[core], beside)]
        made = []
        for part in range(parts):
            number, picks = chosen(part, count_bits - 1 - turn, False)
            for pick in picks:
                spot = rows_out.at[core, pick, part]
                made.append(begin(spot, spot, across(number)))
        return made

    made = []
    for turn in range(max(line, count_bits + 1)):
        for one in made:
            one.wait_recv()
        made = plane_spread(turn) if turn <= count_bits else []
        if turn == count_bits:
            fill(64)
        if turn + 2 <= line:
            line_spread(turn + 2)
        if turn < count_bits:
            fill(2)
    for one in made:
        one.wait_recv()
    line_spread_sent()
    line_sent()
    for one in pending:
        one.wait_send()


def exchange(row_part, col_part, gram_part):
    line, many = lax.axis_size("tr"), lax.axis_size("tc")
    count_bits = line.bit_length() - 1
    row_blocks, size, count_obs = row_part.shape
    parts, width = count_bits, size // count_bits
    seg = count_obs // many
    rows = (2, line, parts, width, count_obs)
    cols = col_part.shape
    gram = (many, seg, count_obs)
    landings = sum(parts * 2 ** (count_bits - 1 - step) for step in range(count_bits))
    part = pivot_size(count_obs)
    cross_rows, cross_cols, inverted = pl.pallas_call(
        functools.partial(exchange_kernel, count_bits),
        out_shape=tuple(jax.ShapeDtypeStruct(shape, f32) for shape in (rows, cols, gram_part.shape)),
        in_specs=[VMEM] * 3,
        out_specs=(VMEM,) * 3,
        scratch_shapes=[
            pltpu.VMEM(gram, f32),
            pltpu.VMEM((part, part), f32),
            pltpu.SemaphoreType.DMA((96,)),
            pltpu.SemaphoreType.DMA((96,)),
            pltpu.VMEM(rows[1:], f32),
            pltpu.VMEM(rows[1:], f32),
            pltpu.VMEM((landings, width, count_obs), f32),
            pltpu.VMEM(cols, f32),
            pltpu.VMEM(cols, f32),
            pltpu.VMEM(rows[2:], f32),
            pltpu.VMEM(cols[1:], f32),
            pltpu.VMEM(cols[1:], f32),
            pltpu.VMEM(gram, f32),
            pltpu.VMEM((many // 2, seg, count_obs), f32),
            pltpu.VMEM((many // 2, seg, count_obs), f32),
            pltpu.VMEM((line, seg, count_obs), f32),
        ],
        compiler_params=pltpu.CompilerParams(has_side_effects=True),
        name="exchange",
    )(row_part.reshape(rows), col_part, gram_part.reshape(gram))
    return cross_rows.reshape(row_part.shape), cross_cols, inverted


def body(cov_tiles, block_order, stations, obs_values, obs_error):
    size = obs_values.shape[2]
    line, many = lax.axis_size("tr"), lax.axis_size("tc")
    packed = share(pack(stations, obs_values, obs_error))
    row_part, col_part, gram_part = forward(block_order, packed, cov_tiles, size)
    square = many == 2 * line and line & (line - 1) == 0 and line > 1
    whole_tiles = row_part.shape[0] == many and col_part.shape[0] == line
    spread = exchange if square and whole_tiles else exchange_plain
    cross_rows, cross_cols, inverted = spread(row_part, col_part, gram_part)
    return update(block_order, cross_rows, cross_cols, inverted, cov_tiles)


def solution(mesh):
    in_specs = (P("tr", "tc"), P(), P(None, "tc"), P(None, "tc", None), P(None, "tc"))
    out_specs = P("tr", "tc")
    return jax.shard_map(body, mesh=mesh, in_specs=in_specs, out_specs=out_specs, check_vma=False)
```

```python
import functools

import jax
import jax.numpy as jnp
from jax import lax
from jax.experimental import pallas as pl
from jax.experimental.pallas import tpu as pltpu
from jax.sharding import PartitionSpec as P

exact = lax.Precision.HIGHEST
bf16, f32, i32 = jnp.bfloat16, jnp.float32, jnp.int32
DEPTH = 4
ANY = pl.BlockSpec(memory_space=pl.ANY)
VMEM = pl.BlockSpec(memory_space=pltpu.VMEM)
SMEM = pl.BlockSpec(memory_space=pltpu.SMEM)


def product(former, latter, over, precision=exact):
    return lax.dot_general(
        former,
        latter,
        (((over[0],), (over[1],)), ((), ())),
        precision=precision,
        preferred_element_type=jnp.float32,
    )


def halves(array):
    high = array.astype(bf16)
    return high, (array - high.astype(f32)).astype(bf16)


def dot(former, latter):
    return jnp.dot(former, latter, preferred_element_type=f32)


def dot3(former, latter):
    return dot(former[0], latter[0]) + dot(former[0], latter[1]) + dot(former[1], latter[0])


def list_tiles(order_ref, live_ref, row_blocks, col_blocks, when_dead=None):
    row_first = lax.axis_index("tr") * row_blocks
    col_first = lax.axis_index("tc") * col_blocks

    def step(tile, count):
        row, col = tile // col_blocks, tile % col_blocks
        p, q = row_first + row, col_first + col
        live = (order_ref[p] > order_ref[q]) | (p == q)

        @pl.when(live)
        def _():
            live_ref[count] = tile

        if when_dead is not None:

            @pl.when(jnp.logical_not(live))
            def _():
                when_dead(tile)

        return count + live.astype(i32)

    return lax.fori_loop(0, row_blocks * col_blocks, step, jnp.int32(0))


def tile_at(ref, tile, col_blocks, size):
    row, col = tile // col_blocks, tile % col_blocks
    return ref.at[
        pl.ds(pl.multiple_of(row * size, size), size), pl.ds(pl.multiple_of(col * size, size), size)
    ]


def forward_kernel(
    order_ref, packed_ref, cov_ref, rows_ref, cols_ref, gram_ref,
    live_ref, held, sem, for_rows, for_cols,
):
    row_blocks, size, count_obs = rows_ref.shape
    col_blocks = cols_ref.shape[0]
    row_first = lax.axis_index("tr") * row_blocks
    col_first = lax.axis_index("tc") * col_blocks
    count = list_tiles(order_ref, live_ref, row_blocks, col_blocks)

    def fetch(at):
        slot = at % DEPTH
        return pltpu.make_async_copy(
            tile_at(cov_ref, live_ref[at], col_blocks, size), held.at[slot], sem.at[slot]
        )

    for at in range(DEPTH - 1):

        @pl.when(at < count)
        def _():
            fetch(at).start()

    values = packed_ref[:, :size]
    extras = packed_ref[:, size:]
    codes_down = extras[:, 0:1].astype(i32)
    flipped = extras.T
    codes_across = flipped[0:1, :].astype(i32)
    errors_across = flipped[1:2, :]
    values_t = values.T
    for block in range(row_blocks):
        chosen = jnp.where(codes_down == order_ref[row_first + block], values, 0.0)
        for_rows[block, 0], for_rows[block, 1] = halves(chosen)
    for block in range(col_blocks):
        chosen = jnp.where(codes_across == order_ref[col_first + block], values_t, 0.0)
        for_cols[block, 0], for_cols[block, 1] = halves(chosen)
    rows_ref[...] = jnp.zeros_like(rows_ref)
    cols_ref[...] = jnp.zeros_like(cols_ref)

    def step(at, carry):
        tile = live_ref[at]
        row, col = tile // col_blocks, tile % col_blocks
        slot = at % DEPTH

        @pl.when(at + DEPTH - 1 < count)
        def _():
            fetch(at + DEPTH - 1).start()

        fetch(at).wait()
        parts = halves(held[slot])
        rows_ref[row] += dot3(parts, (for_cols[col, 0], for_cols[col, 1]))

        @pl.when(row_first + row != col_first + col)
        def _():
            cols_ref[col] += dot3((for_rows[row, 0], for_rows[row, 1]), parts)

        return carry

    lax.fori_loop(0, count, step, 0)
    first = (lax.axis_index("tr") == 0) & (lax.axis_index("tc") == 0)
    across = lax.broadcasted_iota(i32, (count_obs, count_obs), 1)
    down = lax.broadcasted_iota(i32, (count_obs, count_obs), 0)
    gram_ref[...] = jnp.zeros_like(gram_ref)

    def add_col(block, carry):
        gram_ref[...] += dot3(halves(cols_ref[block]), (for_cols[block, 0], for_cols[block, 1]))
        return carry

    lax.fori_loop(0, col_blocks, add_col, 0)
    gram_ref[...] = gram_ref[...].T + jnp.where((across == down) & first, errors_across, 0.0)

    def add_row(block, carry):
        gram_ref[...] += dot3((for_rows[block, 0], for_rows[block, 1]), halves(rows_ref[block]))
        return carry

    lax.fori_loop(0, row_blocks, add_row, 0)


def forward(block_order, packed, cov_tiles, size):
    count_obs = packed.shape[0]
    row_blocks, col_blocks = cov_tiles.shape[0] // size, cov_tiles.shape[1] // size
    tiles = row_blocks * col_blocks
    return pl.pallas_call(
        forward_kernel,
        out_shape=(
            jax.ShapeDtypeStruct((row_blocks, size, count_obs), f32),
            jax.ShapeDtypeStruct((col_blocks, count_obs, size), f32),
            jax.ShapeDtypeStruct((count_obs, count_obs), f32),
        ),
        in_specs=[SMEM, VMEM, ANY],
        out_specs=(VMEM, VMEM, VMEM),
        scratch_shapes=[
            pltpu.SMEM((tiles,), i32),
            pltpu.VMEM((DEPTH, size, size), f32),
            pltpu.SemaphoreType.DMA((DEPTH,)),
            pltpu.VMEM((row_blocks, 2, count_obs, size), bf16),
            pltpu.VMEM((col_blocks, 2, size, count_obs), bf16),
        ],
        cost_estimate=pl.CostEstimate(
            flops=6 * tiles * size * size * count_obs, bytes_accessed=2 * tiles * size * size, transcendentals=0
        ),
        name="forward",
    )(block_order, packed, cov_tiles)


def update_kernel(
    order_ref, rows_ref, cols_ref, inverse_ref, cov_ref, out_ref,
    live_ref, held, made, zeros, weighted, in_sem, out_sem, zero_sem,
):
    row_blocks, size, _ = rows_ref.shape
    col_blocks = cols_ref.shape[0]
    tiles = row_blocks * col_blocks
    zeros[...] = jnp.zeros_like(zeros)

    def blank(tile):
        return pltpu.make_async_copy(zeros, tile_at(out_ref, tile, col_blocks, size), zero_sem.at[tile])

    count = list_tiles(order_ref, live_ref, row_blocks, col_blocks)

    def fetch(at):
        slot = at % DEPTH
        return pltpu.make_async_copy(
            tile_at(cov_ref, live_ref[at], col_blocks, size), held.at[slot], in_sem.at[slot]
        )

    def put(at):
        slot = at % DEPTH
        return pltpu.make_async_copy(
            made.at[slot], tile_at(out_ref, live_ref[at], col_blocks, size), out_sem.at[slot]
        )

    for at in range(DEPTH - 1):

        @pl.when(at < count)
        def _():
            fetch(at).start()

    list_tiles(order_ref, live_ref, row_blocks, col_blocks, lambda tile: blank(tile).start())
    for block in range(col_blocks):
        weighted[block, 0], weighted[block, 1] = halves(product(inverse_ref[...], cols_ref[block], (1, 0)))

    def step(at, carry):
        tile = live_ref[at]
        row, col = tile // col_blocks, tile % col_blocks
        slot = at % DEPTH

        @pl.when(at + DEPTH - 1 < count)
        def _():
            fetch(at + DEPTH - 1).start()

        @pl.when(at >= DEPTH)
        def _():
            put(at - DEPTH).wait()

        fetch(at).wait()
        made[slot] = held[slot] - dot3(halves(rows_ref[row]), (weighted[col, 0], weighted[col, 1]))
        put(at).start()
        return carry

    lax.fori_loop(0, count, step, 0)
    lax.fori_loop(jnp.maximum(count - DEPTH, 0), count, lambda at, carry: (put(at).wait(), carry)[1], 0)
    list_tiles(order_ref, live_ref, row_blocks, col_blocks, lambda tile: blank(tile).wait())


def update(block_order, cross_rows, cross_cols, inverted, cov_tiles):
    row_blocks, size, count_obs = cross_rows.shape
    col_blocks = cross_cols.shape[0]
    tiles = row_blocks * col_blocks
    return pl.pallas_call(
        update_kernel,
        out_shape=jax.ShapeDtypeStruct(cov_tiles.shape, f32),
        in_specs=[SMEM, VMEM, VMEM, VMEM, ANY],
        out_specs=ANY,
        scratch_shapes=[
            pltpu.SMEM((tiles,), i32),
            pltpu.VMEM((DEPTH, size, size), f32),
            pltpu.VMEM((DEPTH, size, size), f32),
            pltpu.VMEM((size, size), f32),
            pltpu.VMEM((col_blocks, 2, count_obs, size), bf16),
            pltpu.SemaphoreType.DMA((DEPTH,)),
            pltpu.SemaphoreType.DMA((DEPTH,)),
            pltpu.SemaphoreType.DMA((tiles,)),
        ],
        cost_estimate=pl.CostEstimate(
            flops=3 * tiles * size * size * count_obs, bytes_accessed=6 * tiles * size * size, transcendentals=0
        ),
        name="update",
    )(block_order, cross_rows, cross_cols, inverted, cov_tiles)


def swept(matrix, work):
    size = matrix.shape[0]
    work[...] = matrix
    lanes = lax.broadcasted_iota(jnp.int32, (1, size), 1)
    rows = lax.broadcasted_iota(jnp.int32, (size, 1), 0)

    def step(pivot, carry):
        held = work[...]
        row = work[pl.ds(pivot, 1), :]
        at_lane = lanes == pivot
        at_row = rows == pivot
        column = jnp.sum(jnp.where(at_lane, held, 0.0), axis=1, keepdims=True)
        share = 1.0 / jnp.sum(jnp.where(at_lane, row, 0.0), axis=1, keepdims=True)
        kept = jnp.where(at_lane | at_row, 0.0, held)
        left = jnp.where(at_row, -1.0, column)
        right = jnp.where(at_lane, -1.0, row)
        work[...] = kept - left * (right * share)
        return carry

    quarter = size // 4
    for turn in range(4):
        lax.fori_loop(turn * quarter, (turn + 1) * quarter, step, 0)
        yield
    return -work[...]


def inverse_of(matrix, work):
    size = matrix.shape[0]
    if size <= 128:
        return (yield from swept(matrix, work))
    half = size // 2
    upper, corner, lower = matrix[:half, :half], matrix[half:, :half], matrix[half:, half:]
    upper_inverse = yield from inverse_of(upper, work)
    weight = product(corner, upper_inverse, (1, 0))
    lower_inverse = yield from inverse_of(lower - product(weight, corner, (1, 1)), work)
    below = -product(lower_inverse, weight, (1, 0))
    above = upper_inverse - product(weight, below, (0, 0))
    return jnp.concatenate(
        (jnp.concatenate((above, below.T), axis=1), jnp.concatenate((below, lower_inverse), axis=1)), axis=0
    )


def inverse_steps(matrix_ref, inverse_ref, work):
    size = matrix_ref.shape[-1]
    inverse_ref[...] = yield from inverse_of(matrix_ref[...].reshape(size, size), work)


def inverse_kernel(matrix_ref, inverse_ref, work):
    for _ in inverse_steps(matrix_ref, inverse_ref, work):
        pass


def pivot_size(size):
    return size if size <= 128 else pivot_size(size // 2)


def inverse(matrix):
    size = matrix.shape[0]
    part = pivot_size(size)
    return pl.pallas_call(
        inverse_kernel,
        out_shape=jax.ShapeDtypeStruct(matrix.shape, jnp.float32),
        in_specs=[VMEM],
        out_specs=VMEM,
        scratch_shapes=[pltpu.VMEM((part, part), jnp.float32)],
        cost_estimate=pl.CostEstimate(flops=400_000_000, bytes_accessed=8 * size * size, transcendentals=0),
        name="inverse",
    )(matrix)


def pack(stations, obs_values, obs_error):
    values = obs_values[0]
    count, size = values.shape
    return jnp.concatenate(
        (
            values,
            stations[0].astype(f32)[:, None],
            obs_error[0][:, None],
            jnp.zeros((count, 126), f32),
        ),
        axis=1,
    )


def exchange_plain(row_part, col_part, gram_part):
    tr_size, tc_size = lax.axis_size("tr"), lax.axis_size("tc")
    row_blocks, size, count_obs = row_part.shape
    col_blocks = col_part.shape[0]
    row_part = row_part.reshape(row_blocks * size, count_obs)
    col_part = col_part.transpose(0, 2, 1).reshape(col_blocks * size, count_obs)
    innovation = lax.psum(gram_part, ("tr", "tc"))
    count = tr_size * tc_size
    to_rows = [((q % tr_size) * tc_size + q // tr_size, q) for q in range(count)]
    to_cols = [(there, here) for here, there in to_rows]
    col_chunk = lax.psum_scatter(col_part, "tr", scatter_dimension=0, tiled=True)
    row_chunk = lax.psum_scatter(row_part, "tc", scatter_dimension=0, tiled=True)
    chunk = row_chunk + lax.ppermute(col_chunk, ("tr", "tc"), to_rows)
    cross_rows = lax.all_gather(chunk, "tc", axis=0, tiled=True)
    cross_cols = lax.all_gather(lax.ppermute(chunk, ("tr", "tc"), to_cols), "tr", axis=0, tiled=True)
    return (
        cross_rows.reshape(row_blocks, size, count_obs),
        cross_cols.reshape(col_blocks, size, count_obs).transpose(0, 2, 1),
        inverse(innovation),
    )


class Sems:
    def __init__(self):
        self.count = 0

    def take(self, number=1):
        self.count += number
        return self.count - number


def share_kernel(mine_ref, all_ref, send, recv, core_send, core_recv):
    row, col = lax.axis_index("tr"), lax.axis_index("tc")
    chips = all_ref.shape[0] // 2
    chip, core = col // 2, col % 2

    def copy(source, block, step):
        return pltpu.make_async_remote_copy(
            source, all_ref.at[block], send.at[step], recv.at[step],
            device_id=(row, 2 * lax.rem(chip + step, chips) + core), device_id_type=pl.DeviceIdType.MESH,
        )

    def beside(source, block, step):
        return pltpu.make_async_remote_copy(
            source, all_ref.at[block], core_send.at[step], core_recv.at[step],
            device_id=(row, 2 * chip + 1 - core), device_id_type=pl.DeviceIdType.MESH,
        )

    sent = [copy(mine_ref, col, step) for step in range(1, chips)]
    sent.append(beside(mine_ref, col, 0))
    for one in sent:
        one.start()
    all_ref[col] = mine_ref[...]
    for step in range(1, chips):
        block = 2 * lax.rem(chip + chips - step, chips) + core
        copy(mine_ref, block, step).wait_recv()
        sent.append(beside(all_ref.at[block], block, step))
        sent[-1].start()
    for step in range(chips):
        beside(mine_ref, 2 * lax.rem(chip + chips - step, chips) + 1 - core, step).wait_recv()
    for one in sent:
        one.wait_send()


def share(packed):
    many = lax.axis_size("tc")
    full = pl.pallas_call(
        share_kernel,
        out_shape=jax.ShapeDtypeStruct((many, *packed.shape), f32),
        in_specs=[VMEM],
        out_specs=VMEM,
        scratch_shapes=[pltpu.SemaphoreType.DMA((many // 2,))] * 4,
        compiler_params=pltpu.CompilerParams(has_side_effects=True),
        name="share",
    )(packed)
    return full.reshape(many * packed.shape[0], packed.shape[1])


def exchange_kernel(
    count_bits, row_ref, col_ref, gram_ref, rows_out, cols_out, inverse_out,
    gram_out, work, send, recv, from_core, sums, landed, upward, downward, rows_here, cols_here, total, relay,
    gram_work, gram_core, gram_bits, gram_line,
):
    sems = Sems()
    line = lax.axis_size("tr")
    z, j = lax.axis_index("tr"), lax.axis_index("tc")
    chip, core = j // 2, j % 2
    parts = count_bits
    width = rows_here.shape[1]
    pending = []
    beside = (z, 2 * chip + 1 - core)

    def copy(source, target, sem, device=beside):
        return pltpu.make_async_remote_copy(
            source, target, send.at[sem], recv.at[sem], device_id=device, device_id_type=pl.DeviceIdType.MESH
        )

    def begin(source, target, device):
        made = copy(source, target, sems.take(), device)
        made.start()
        pending.append(made)
        return made

    def bit(number):
        return chip // 2**number % 2

    def across(number):
        return z, 2 * (chip + (1 - 2 * bit(number)) * 2**number) + core

    def mixed(value, plane):
        return sum(
            (value // 2**number + plane // 2 ** (count_bits - 1 - number)) % 2 * 2**number
            for number in range(count_bits)
        )

    def plane_of(value, chunk):
        return sum(
            (value // 2**number + chunk // 2**number) % 2 * 2 ** (count_bits - 1 - number)
            for number in range(count_bits)
        )

    up, down = sems.take(line), sems.take(line)

    def line_begin(step):
        chunk, other = line - step, step - 1

        @pl.when(z == 0)
        def _():
            copy(col_ref.at[chunk], upward.at[chunk], up + chunk, (z + 1, j)).start()

        @pl.when(z == line - 1)
        def _():
            copy(col_ref.at[other], downward.at[other], down + other, (z - 1, j)).start()

    def line_round(step):
        chunk, other = z + line - 1 - step, z - line + 1 + step

        @pl.when((z > 0) & (chunk < line))
        def _():
            copy(upward.at[chunk], upward.at[chunk], up + chunk).wait_recv()
            upward[chunk] += col_ref[chunk]
            copy(upward.at[chunk], upward.at[chunk], up + chunk, (z + 1, j)).start()

        @pl.when((z < line - 1) & (other >= 0))
        def _():
            copy(downward.at[other], downward.at[other], down + other).wait_recv()
            downward[other] += col_ref[other]
            copy(downward.at[other], downward.at[other], down + other, (z - 1, j)).start()

    def line_end():
        total[...] = col_ref[z]

        @pl.when(z > 0)
        def _():
            copy(upward.at[z], upward.at[z], up + z).wait_recv()
            total[...] += upward[z]

        @pl.when(z < line - 1)
        def _():
            copy(downward.at[z], downward.at[z], down + z).wait_recv()
            total[...] += downward[z]

    def line_sent():
        for step in range(1, line):
            chunk, other = line - step, step - 1

            @pl.when(z < chunk)
            def _():
                copy(upward.at[chunk], upward.at[chunk], up + chunk).wait_send()

            @pl.when(z > other)
            def _():
                copy(downward.at[other], downward.at[other], down + other).wait_send()

    def chosen(part, step, flip):
        order = [(part + turn) % count_bits for turn in range(count_bits)]
        free = order[step + 1:]
        picks = []
        for pick in range(2 ** len(free)):
            where = 0
            for turn, number in enumerate(order):
                if number in free:
                    value = pick // 2 ** free.index(number) % 2
                elif turn == step and flip:
                    value = 1 - bit(number)
                else:
                    value = bit(number)
                where = where + value * 2**number
            picks.append(where)
        return order[step], picks

    step_base = [0]
    for step in range(count_bits):
        step_base.append(step_base[-1] + parts * 2 ** (count_bits - 1 - step))

    def plane_send(step):
        made = []
        for part in range(parts):
            number, picks = chosen(part, step, True)
            for slot, pick in enumerate(picks):
                at = step_base[step] + part * len(picks) + slot
                made.append(begin(sums.at[pick, part], landed.at[at], across(number)))
        return made

    def plane_add(step, made):
        for one in made:
            one.wait_recv()
        for part in range(parts):
            _, picks = chosen(part, step, False)
            for slot, pick in enumerate(picks):
                sums[pick, part] += landed[step_base[step] + part * len(picks) + slot]

    line_begin(1)
    held = 2**count_bits
    half = begin(gram_ref.at[pl.ds((1 - core) * held, held)], gram_core, beside)
    core_sum = begin(row_ref.at[1 - core], from_core, beside)
    half.wait_recv()
    gram_work[pl.ds(core * held, held)] = gram_ref[pl.ds(core * held, held)] + gram_core[...]
    for number in reversed(range(count_bits)):
        size = 2**number
        start = core * held + chip // (2 * size) * (2 * size)
        keep, give = start + bit(number) * size, start + (1 - bit(number)) * size
        begin(gram_work.at[pl.ds(give, size)], gram_bits.at[pl.ds(size, size)], across(number)).wait_recv()
        gram_work[pl.ds(keep, size)] += gram_bits[pl.ds(size, size)]
    mine = core * held + chip
    gram_line[z] = gram_work[mine]
    base = sems.take(line)
    for step in range(1, line):
        copy(gram_work.at[mine], gram_line.at[z], base + step, (lax.rem(z + step, line), j)).start()
    for step in range(2, line):
        line_begin(step)

    core_sum.wait_recv()
    for owner in range(line):
        chunk = mixed(owner, z)
        sums[owner] = row_ref[core, chunk] + from_core[chunk]
    made = plane_send(0)

    def gram_back():
        for step in range(1, line):
            copy(gram_work.at[mine], gram_line.at[lax.rem(z + line - step, line)], base + step).wait()
        gram_out[mine] = sum(gram_line[step] for step in range(line))
        for number in range(count_bits):
            size = 2**number
            spot = gram_out.at[pl.ds(core * held + chip // size * size, size)]
            sent = begin(spot, spot, across(number))
            yield
            sent.wait_recv()
        spot = gram_out.at[pl.ds(core * held, held)]
        sent = begin(spot, spot, beside)
        yield
        sent.wait_recv()

    gram_turns = gram_back()
    for step in range(1, line - 1):
        line_round(step)
        next(gram_turns, None)
        if step < count_bits:
            plane_add(step - 1, made)
            made = plane_send(step)
            next(gram_turns, None)
    for _ in gram_turns:
        pass
    for step in range(max(line - 1, 1), count_bits):
        plane_add(step - 1, made)
        made = plane_send(step)
    plane_add(count_bits - 1, made)
    inverse_turns = inverse_steps(gram_out, inverse_out, work)

    def fill(number):
        for _ in range(number):
            next(inverse_turns, None)

    to_cols, first_leg, second_leg = sems.take(), sems.take(2), sems.take(2)
    owned = mixed(chip, z)
    apart = (owned != z) | (z != chip)
    column = (owned, 2 * z + core)
    via = mixed(z, chip)
    beyond = plane_of(chip, z)

    @pl.when(apart)
    def _():
        copy(sums.at[chip], rows_here, to_cols, column).start()

    @pl.when(jnp.logical_not(apart))
    def _():
        rows_here[...] = sums[chip]

    fill(1)
    line_end()

    def piece(ref, number):
        size = total.shape[0] // 2
        return ref.at[pl.ds(number * size, size)]

    def leg_one(number):
        return copy(piece(total, number), piece(relay, number), first_leg + number, (z, 2 * via + core))

    def leg_two(number):
        return copy(piece(relay, number), piece(cols_here, number), second_leg + number, (beyond, j))

    @pl.when(via != chip)
    def _():
        leg_one(0).start()
        leg_one(1).start()

    @pl.when(via == chip)
    def _():
        relay[...] = total[...]

    @pl.when(apart)
    def _():
        copy(sums.at[chip], rows_here, to_cols, column).wait()

    for part in range(parts):
        lanes = slice(part * width, (part + 1) * width)
        cols_out[z, :, lanes] = total[:, lanes] + rows_here[part].T
    around, back = sems.take(line), sems.take(line)

    def line_spread(step):
        chunk, other = z - (step - 1), z + (step - 1)

        @pl.when(chunk >= 0)
        def _():
            if step > 1:
                copy(cols_out.at[chunk], cols_out.at[chunk], around + chunk).wait_recv()

            @pl.when(z < line - 1)
            def _():
                copy(cols_out.at[chunk], cols_out.at[chunk], around + chunk, (z + 1, j)).start()

        @pl.when(other < line)
        def _():
            if step > 1:
                copy(cols_out.at[other], cols_out.at[other], back + other).wait_recv()

            @pl.when(z > 0)
            def _():
                copy(cols_out.at[other], cols_out.at[other], back + other, (z - 1, j)).start()

    def line_spread_sent():
        for step in range(1, line + 1):
            chunk, other = z - (step - 1), z + (step - 1)

            @pl.when((chunk >= 0) & (z < line - 1))
            def _():
                copy(cols_out.at[chunk], cols_out.at[chunk], around + chunk).wait_send()

            @pl.when((other < line) & (z > 0))
            def _():
                copy(cols_out.at[other], cols_out.at[other], back + other).wait_send()

    line_spread(1)
    for number in range(2):

        @pl.when(via != chip)
        def _():
            leg_one(number).wait()

        @pl.when(beyond != z)
        def _():
            leg_two(number).start()

    @pl.when(beyond == z)
    def _():
        cols_here[...] = relay[...]

    fill(3)

    @pl.when(beyond != z)
    def _():
        leg_two(0).wait()
        leg_two(1).wait()

    for part in range(parts):
        lanes = slice(part * width, (part + 1) * width)
        rows_out[core, owned, part] = sums[chip, part] + cols_here[:, lanes].T

    def spots(turn, flip):
        for part in range(parts):
            number, picks = chosen(part, count_bits - 1 - turn, flip)
            for pick in picks:
                yield number, rows_out.at[core, mixed(pick, z), part]

    beside_copies = [begin(rows_out.at[core, owned], rows_out.at[core, owned], beside)]
    for turn in range(max(line - 1, count_bits)):
        if turn < count_bits:
            made = [begin(spot, spot, across(number)) for number, spot in spots(turn, False)]
        if turn == count_bits:
            fill(64)
        if turn + 2 <= line:
            line_spread(turn + 2)
        if turn < count_bits:
            fill(2)
            for one in made:
                one.wait_recv()
            beside_copies += [begin(spot, spot, beside) for _, spot in spots(turn, True)]
    fill(64)
    for one in beside_copies:
        one.wait_recv()
    line_spread_sent()
    line_sent()
    for one in pending:
        one.wait_send()


def exchange(row_part, col_part, gram_part):
    line, many = lax.axis_size("tr"), lax.axis_size("tc")
    count_bits = line.bit_length() - 1
    row_blocks, size, count_obs = row_part.shape
    parts, width = count_bits, size // count_bits
    seg = count_obs // many
    rows = (2, line, parts, width, count_obs)
    cols = col_part.shape
    gram = (many, seg, count_obs)
    landings = sum(parts * 2 ** (count_bits - 1 - step) for step in range(count_bits))
    part = pivot_size(count_obs)
    cross_rows, cross_cols, inverted = pl.pallas_call(
        functools.partial(exchange_kernel, count_bits),
        out_shape=tuple(jax.ShapeDtypeStruct(shape, f32) for shape in (rows, cols, gram_part.shape)),
        in_specs=[VMEM] * 3,
        out_specs=(VMEM,) * 3,
        scratch_shapes=[
            pltpu.VMEM(gram, f32),
            pltpu.VMEM((part, part), f32),
            pltpu.SemaphoreType.DMA((96,)),
            pltpu.SemaphoreType.DMA((96,)),
            pltpu.VMEM(rows[1:], f32),
            pltpu.VMEM(rows[1:], f32),
            pltpu.VMEM((landings, width, count_obs), f32),
            pltpu.VMEM(cols, f32),
            pltpu.VMEM(cols, f32),
            pltpu.VMEM(rows[2:], f32),
            pltpu.VMEM(cols[1:], f32),
            pltpu.VMEM(cols[1:], f32),
            pltpu.VMEM(cols[1:], f32),
            pltpu.VMEM(gram, f32),
            pltpu.VMEM((many // 2, seg, count_obs), f32),
            pltpu.VMEM((many // 2, seg, count_obs), f32),
            pltpu.VMEM((line, seg, count_obs), f32),
        ],
        compiler_params=pltpu.CompilerParams(has_side_effects=True),
        name="exchange",
    )(row_part.reshape(rows), col_part, gram_part.reshape(gram))
    return cross_rows.reshape(row_part.shape), cross_cols, inverted


def body(cov_tiles, block_order, stations, obs_values, obs_error):
    size = obs_values.shape[2]
    line, many = lax.axis_size("tr"), lax.axis_size("tc")
    packed = share(pack(stations, obs_values, obs_error))
    row_part, col_part, gram_part = forward(block_order, packed, cov_tiles, size)
    square = many == 2 * line and line & (line - 1) == 0 and line > 1
    whole_tiles = row_part.shape[0] == many and col_part.shape[0] == line
    spread = exchange if square and whole_tiles else exchange_plain
    cross_rows, cross_cols, inverted = spread(row_part, col_part, gram_part)
    return update(block_order, cross_rows, cross_cols, inverted, cov_tiles)


def solution(mesh):
    in_specs = (P("tr", "tc"), P(), P(None, "tc"), P(None, "tc", None), P(None, "tc"))
    out_specs = P("tr", "tc")
    return jax.shard_map(body, mesh=mesh, in_specs=in_specs, out_specs=out_specs, check_vma=False)
```

```python
import functools

import jax
import jax.numpy as jnp
from jax import lax
from jax.experimental import pallas as pl
from jax.experimental.pallas import tpu as pltpu
from jax.sharding import PartitionSpec as P

exact = lax.Precision.HIGHEST
bf16, f32, i32 = jnp.bfloat16, jnp.float32, jnp.int32
DEPTH = 4
ANY = pl.BlockSpec(memory_space=pl.ANY)
VMEM = pl.BlockSpec(memory_space=pltpu.VMEM)
SMEM = pl.BlockSpec(memory_space=pltpu.SMEM)


def product(former, latter, over, precision=exact):
    return lax.dot_general(
        former,
        latter,
        (((over[0],), (over[1],)), ((), ())),
        precision=precision,
        preferred_element_type=jnp.float32,
    )


def halves(array):
    high = array.astype(bf16)
    return high, (array - high.astype(f32)).astype(bf16)


def dot(former, latter):
    return jnp.dot(former, latter, preferred_element_type=f32)


def dot3(former, latter):
    return dot(former[0], latter[0]) + dot(former[0], latter[1]) + dot(former[1], latter[0])


def list_tiles(order_ref, live_ref, row_blocks, col_blocks, when_dead=None):
    row_first = lax.axis_index("tr") * row_blocks
    col_first = lax.axis_index("tc") * col_blocks

    def step(tile, count):
        row, col = tile // col_blocks, tile % col_blocks
        p, q = row_first + row, col_first + col
        live = (order_ref[p] > order_ref[q]) | (p == q)

        @pl.when(live)
        def _():
            live_ref[count] = tile

        if when_dead is not None:

            @pl.when(jnp.logical_not(live))
            def _():
                when_dead(tile)

        return count + live.astype(i32)

    return lax.fori_loop(0, row_blocks * col_blocks, step, jnp.int32(0))


def tile_at(ref, tile, col_blocks, size):
    row, col = tile // col_blocks, tile % col_blocks
    return ref.at[
        pl.ds(pl.multiple_of(row * size, size), size), pl.ds(pl.multiple_of(col * size, size), size)
    ]


def sorted_by_station(packed, size):
    count = packed.shape[0]
    codes = packed[:, size:size + 1]
    codes_across = packed[:, size:].T[0:1, :]
    down = lax.broadcasted_iota(i32, (count, count), 0)
    across = lax.broadcasted_iota(i32, (count, count), 1)
    earlier = (codes < codes_across) | ((codes == codes_across) & (down < across))
    rank = jnp.sum(jnp.where(earlier, 1.0, 0.0), axis=0, keepdims=True).astype(i32)
    return product(jnp.where(down == rank, 1.0, 0.0), packed, (1, 0))


def forward_kernel(
    order_ref, packed_ref, cov_ref, rows_ref, cols_ref, gram_ref,
    live_ref, used_rows, used_cols, held, sem, for_rows, for_cols,
):
    row_blocks, size, count_obs = rows_ref.shape
    col_blocks = cols_ref.shape[0]
    windows, span = for_rows.shape[1], for_rows.shape[2] // 2
    row_first = lax.axis_index("tr") * row_blocks
    col_first = lax.axis_index("tc") * col_blocks
    count = list_tiles(order_ref, live_ref, row_blocks, col_blocks)

    def fetch(at):
        slot = at % DEPTH
        return pltpu.make_async_copy(
            tile_at(cov_ref, live_ref[at], col_blocks, size), held.at[slot], sem.at[slot]
        )

    for at in range(DEPTH - 1):

        @pl.when(at < count)
        def _():
            fetch(at).start()

    packed = sorted_by_station(packed_ref[...], size)
    values = packed[:, :size]
    extras = packed[:, size:]
    codes_down = extras[:, 0:1].astype(i32)
    flipped = extras.T
    codes_across = flipped[0:1, :].astype(i32)
    errors_across = flipped[1:2, :]
    values_t = values.T
    for window in range(windows):
        here = slice(window * span, (window + 1) * span)
        for block in range(row_blocks):
            match = codes_down[here] == order_ref[row_first + block]
            high, low = halves(jnp.where(match, values[here], 0.0))
            for_rows[block, window] = jnp.concatenate((high, low), axis=0)
            same = codes_across[:, here] == order_ref[row_first + block]
            used_rows[block * windows + window] = jnp.sum(jnp.where(same, 1, 0))
        for block in range(col_blocks):
            match = codes_across[:, here] == order_ref[col_first + block]
            high, low = halves(jnp.where(match, values_t[:, here], 0.0))
            for_cols[block, window] = jnp.concatenate((high, low), axis=1)
            used_cols[block * windows + window] = jnp.sum(jnp.where(match, 1, 0))
    rows_ref[...] = jnp.zeros_like(rows_ref)
    cols_ref[...] = jnp.zeros_like(cols_ref)
    gram_ref[...] = jnp.zeros_like(gram_ref)

    def times_cols(parts, block, window):
        both = dot(parts[0], for_cols[block, window]) + dot(parts[1], for_cols[block, window])
        return both[:, :span] + both[:, span:]

    def rows_times(parts, block, window):
        both = dot(for_rows[block, window], parts[0])
        return both[:span] + both[span:] + dot(for_rows[block, window, :span], parts[1])

    def step(at, carry):
        tile = live_ref[at]
        row, col = tile // col_blocks, tile % col_blocks
        slot = at % DEPTH

        @pl.when(at + DEPTH - 1 < count)
        def _():
            fetch(at + DEPTH - 1).start()

        fetch(at).wait()
        strict = row_first + row != col_first + col
        for window in range(windows):
            here = slice(window * span, (window + 1) * span)

            @pl.when(used_cols[col * windows + window] > 0)
            def _():
                rows_ref[row, :, here] += times_cols(halves(held[slot]), col, window)

            @pl.when(strict & (used_rows[row * windows + window] > 0))
            def _():
                cols_ref[col, here] += rows_times(halves(held[slot]), row, window)

        return carry

    lax.fori_loop(0, count, step, 0)

    def add_col(block, carry):
        for window in range(windows):
            here = slice(window * span, (window + 1) * span)

            @pl.when(used_cols[block * windows + window] > 0)
            def _():
                gram_ref[:, here] += times_cols(halves(cols_ref[block]), block, window)

        return carry

    lax.fori_loop(0, col_blocks, add_col, 0)
    first = (lax.axis_index("tr") == 0) & (lax.axis_index("tc") == 0)
    across = lax.broadcasted_iota(i32, (count_obs, count_obs), 1)
    down = lax.broadcasted_iota(i32, (count_obs, count_obs), 0)
    gram_ref[...] = gram_ref[...].T + jnp.where((across == down) & first, errors_across, 0.0)

    def add_row(block, carry):
        for window in range(windows):
            here = slice(window * span, (window + 1) * span)

            @pl.when(used_rows[block * windows + window] > 0)
            def _():
                gram_ref[here] += rows_times(halves(rows_ref[block]), block, window)

        return carry

    lax.fori_loop(0, row_blocks, add_row, 0)


def forward(block_order, packed, cov_tiles, size):
    count_obs = packed.shape[0]
    row_blocks, col_blocks = cov_tiles.shape[0] // size, cov_tiles.shape[1] // size
    tiles = row_blocks * col_blocks
    span = pivot_size(count_obs)
    windows = count_obs // span
    return pl.pallas_call(
        forward_kernel,
        out_shape=(
            jax.ShapeDtypeStruct((row_blocks, size, count_obs), f32),
            jax.ShapeDtypeStruct((col_blocks, count_obs, size), f32),
            jax.ShapeDtypeStruct((count_obs, count_obs), f32),
        ),
        in_specs=[SMEM, VMEM, ANY],
        out_specs=(VMEM, VMEM, VMEM),
        scratch_shapes=[
            pltpu.SMEM((tiles,), i32),
            pltpu.SMEM((row_blocks * windows,), i32),
            pltpu.SMEM((col_blocks * windows,), i32),
            pltpu.VMEM((DEPTH, size, size), f32),
            pltpu.SemaphoreType.DMA((DEPTH,)),
            pltpu.VMEM((row_blocks, windows, 2 * span, size), bf16),
            pltpu.VMEM((col_blocks, windows, size, 2 * span), bf16),
        ],
        cost_estimate=pl.CostEstimate(
            flops=6 * tiles * size * size * count_obs, bytes_accessed=2 * tiles * size * size, transcendentals=0
        ),
        name="forward",
    )(block_order, packed, cov_tiles)


def update_kernel(
    order_ref, rows_ref, cols_ref, inverse_ref, cov_ref, out_ref,
    live_ref, held, made, zeros, weighted, in_sem, out_sem, zero_sem,
):
    row_blocks, size, _ = rows_ref.shape
    col_blocks = cols_ref.shape[0]
    tiles = row_blocks * col_blocks
    zeros[...] = jnp.zeros_like(zeros)

    def blank(tile):
        return pltpu.make_async_copy(zeros, tile_at(out_ref, tile, col_blocks, size), zero_sem.at[tile])

    count = list_tiles(order_ref, live_ref, row_blocks, col_blocks)

    def fetch(at):
        slot = at % DEPTH
        return pltpu.make_async_copy(
            tile_at(cov_ref, live_ref[at], col_blocks, size), held.at[slot], in_sem.at[slot]
        )

    def put(at):
        slot = at % DEPTH
        return pltpu.make_async_copy(
            made.at[slot], tile_at(out_ref, live_ref[at], col_blocks, size), out_sem.at[slot]
        )

    for at in range(DEPTH - 1):

        @pl.when(at < count)
        def _():
            fetch(at).start()

    list_tiles(order_ref, live_ref, row_blocks, col_blocks, lambda tile: blank(tile).start())
    for block in range(col_blocks):
        weighted[block, 0], weighted[block, 1] = halves(product(inverse_ref[...], cols_ref[block], (1, 0)))

    def step(at, carry):
        tile = live_ref[at]
        row, col = tile // col_blocks, tile % col_blocks
        slot = at % DEPTH

        @pl.when(at + DEPTH - 1 < count)
        def _():
            fetch(at + DEPTH - 1).start()

        @pl.when(at >= DEPTH)
        def _():
            put(at - DEPTH).wait()

        fetch(at).wait()
        made[slot] = held[slot] - dot3(halves(rows_ref[row]), (weighted[col, 0], weighted[col, 1]))
        put(at).start()
        return carry

    lax.fori_loop(0, count, step, 0)
    lax.fori_loop(jnp.maximum(count - DEPTH, 0), count, lambda at, carry: (put(at).wait(), carry)[1], 0)
    list_tiles(order_ref, live_ref, row_blocks, col_blocks, lambda tile: blank(tile).wait())


def update(block_order, cross_rows, cross_cols, inverted, cov_tiles):
    row_blocks, size, count_obs = cross_rows.shape
    col_blocks = cross_cols.shape[0]
    tiles = row_blocks * col_blocks
    return pl.pallas_call(
        update_kernel,
        out_shape=jax.ShapeDtypeStruct(cov_tiles.shape, f32),
        in_specs=[SMEM, VMEM, VMEM, VMEM, ANY],
        out_specs=ANY,
        scratch_shapes=[
            pltpu.SMEM((tiles,), i32),
            pltpu.VMEM((DEPTH, size, size), f32),
            pltpu.VMEM((DEPTH, size, size), f32),
            pltpu.VMEM((size, size), f32),
            pltpu.VMEM((col_blocks, 2, count_obs, size), bf16),
            pltpu.SemaphoreType.DMA((DEPTH,)),
            pltpu.SemaphoreType.DMA((DEPTH,)),
            pltpu.SemaphoreType.DMA((tiles,)),
        ],
        cost_estimate=pl.CostEstimate(
            flops=3 * tiles * size * size * count_obs, bytes_accessed=6 * tiles * size * size, transcendentals=0
        ),
        name="update",
    )(block_order, cross_rows, cross_cols, inverted, cov_tiles)


def swept(matrix, work):
    size = matrix.shape[0]
    work[...] = matrix
    lanes = lax.broadcasted_iota(jnp.int32, (1, size), 1)
    rows = lax.broadcasted_iota(jnp.int32, (size, 1), 0)

    def step(pivot, carry):
        held = work[...]
        row = work[pl.ds(pivot, 1), :]
        at_lane = lanes == pivot
        at_row = rows == pivot
        column = jnp.sum(jnp.where(at_lane, held, 0.0), axis=1, keepdims=True)
        share = 1.0 / jnp.sum(jnp.where(at_lane, row, 0.0), axis=1, keepdims=True)
        kept = jnp.where(at_lane | at_row, 0.0, held)
        left = jnp.where(at_row, -1.0, column)
        right = jnp.where(at_lane, -1.0, row)
        work[...] = kept - left * (right * share)
        return carry

    quarter = size // 4
    for turn in range(4):
        lax.fori_loop(turn * quarter, (turn + 1) * quarter, step, 0)
        yield
    return -work[...]


def inverse_of(matrix, work):
    size = matrix.shape[0]
    if size <= 128:
        return (yield from swept(matrix, work))
    half = size // 2
    upper, corner, lower = matrix[:half, :half], matrix[half:, :half], matrix[half:, half:]
    upper_inverse = yield from inverse_of(upper, work)
    weight = product(corner, upper_inverse, (1, 0))
    lower_inverse = yield from inverse_of(lower - product(weight, corner, (1, 1)), work)
    below = -product(lower_inverse, weight, (1, 0))
    above = upper_inverse - product(weight, below, (0, 0))
    return jnp.concatenate(
        (jnp.concatenate((above, below.T), axis=1), jnp.concatenate((below, lower_inverse), axis=1)), axis=0
    )


def inverse_steps(matrix_ref, inverse_ref, work):
    size = matrix_ref.shape[-1]
    inverse_ref[...] = yield from inverse_of(matrix_ref[...].reshape(size, size), work)


def inverse_kernel(matrix_ref, inverse_ref, work):
    for _ in inverse_steps(matrix_ref, inverse_ref, work):
        pass


def pivot_size(size):
    return size if size <= 128 else pivot_size(size // 2)


def inverse(matrix):
    size = matrix.shape[0]
    part = pivot_size(size)
    return pl.pallas_call(
        inverse_kernel,
        out_shape=jax.ShapeDtypeStruct(matrix.shape, jnp.float32),
        in_specs=[VMEM],
        out_specs=VMEM,
        scratch_shapes=[pltpu.VMEM((part, part), jnp.float32)],
        cost_estimate=pl.CostEstimate(flops=400_000_000, bytes_accessed=8 * size * size, transcendentals=0),
        name="inverse",
    )(matrix)


def pack(stations, obs_values, obs_error):
    values = obs_values[0]
    count, size = values.shape
    return jnp.concatenate(
        (
            values,
            stations[0].astype(f32)[:, None],
            obs_error[0][:, None],
            jnp.zeros((count, 126), f32),
        ),
        axis=1,
    )


def exchange_plain(row_part, col_part, gram_part):
    tr_size, tc_size = lax.axis_size("tr"), lax.axis_size("tc")
    row_blocks, size, count_obs = row_part.shape
    col_blocks = col_part.shape[0]
    row_part = row_part.reshape(row_blocks * size, count_obs)
    col_part = col_part.transpose(0, 2, 1).reshape(col_blocks * size, count_obs)
    innovation = lax.psum(gram_part, ("tr", "tc"))
    count = tr_size * tc_size
    to_rows = [((q % tr_size) * tc_size + q // tr_size, q) for q in range(count)]
    to_cols = [(there, here) for here, there in to_rows]
    col_chunk = lax.psum_scatter(col_part, "tr", scatter_dimension=0, tiled=True)
    row_chunk = lax.psum_scatter(row_part, "tc", scatter_dimension=0, tiled=True)
    chunk = row_chunk + lax.ppermute(col_chunk, ("tr", "tc"), to_rows)
    cross_rows = lax.all_gather(chunk, "tc", axis=0, tiled=True)
    cross_cols = lax.all_gather(lax.ppermute(chunk, ("tr", "tc"), to_cols), "tr", axis=0, tiled=True)
    return (
        cross_rows.reshape(row_blocks, size, count_obs),
        cross_cols.reshape(col_blocks, size, count_obs).transpose(0, 2, 1),
        inverse(innovation),
    )


class Sems:
    def __init__(self):
        self.count = 0

    def take(self, number=1):
        self.count += number
        return self.count - number


def share_kernel(mine_ref, all_ref, send, recv, core_send, core_recv):
    row, col = lax.axis_index("tr"), lax.axis_index("tc")
    chips = all_ref.shape[0] // 2
    chip, core = col // 2, col % 2

    def copy(source, block, step):
        return pltpu.make_async_remote_copy(
            source, all_ref.at[block], send.at[step], recv.at[step],
            device_id=(row, 2 * lax.rem(chip + step, chips) + core), device_id_type=pl.DeviceIdType.MESH,
        )

    def beside(source, block, step):
        return pltpu.make_async_remote_copy(
            source, all_ref.at[block], core_send.at[step], core_recv.at[step],
            device_id=(row, 2 * chip + 1 - core), device_id_type=pl.DeviceIdType.MESH,
        )

    sent = [copy(mine_ref, col, step) for step in range(1, chips)]
    sent.append(beside(mine_ref, col, 0))
    for one in sent:
        one.start()
    all_ref[col] = mine_ref[...]
    for step in range(1, chips):
        block = 2 * lax.rem(chip + chips - step, chips) + core
        copy(mine_ref, block, step).wait_recv()
        sent.append(beside(all_ref.at[block], block, step))
        sent[-1].start()
    for step in range(chips):
        beside(mine_ref, 2 * lax.rem(chip + chips - step, chips) + 1 - core, step).wait_recv()
    for one in sent:
        one.wait_send()


def share(packed):
    many = lax.axis_size("tc")
    full = pl.pallas_call(
        share_kernel,
        out_shape=jax.ShapeDtypeStruct((many, *packed.shape), f32),
        in_specs=[VMEM],
        out_specs=VMEM,
        scratch_shapes=[pltpu.SemaphoreType.DMA((many // 2,))] * 4,
        compiler_params=pltpu.CompilerParams(has_side_effects=True),
        name="share",
    )(packed)
    return full.reshape(many * packed.shape[0], packed.shape[1])


def exchange_kernel(
    count_bits, row_ref, col_ref, gram_ref, rows_out, cols_out, inverse_out,
    gram_out, work, send, recv, from_core, sums, landed, upward, downward, rows_here, cols_here, total, relay,
    gram_work, gram_core, gram_bits, gram_line,
):
    sems = Sems()
    line = lax.axis_size("tr")
    z, j = lax.axis_index("tr"), lax.axis_index("tc")
    chip, core = j // 2, j % 2
    parts = count_bits
    width = rows_here.shape[1]
    pending = []
    beside = (z, 2 * chip + 1 - core)

    def copy(source, target, sem, device=beside):
        return pltpu.make_async_remote_copy(
            source, target, send.at[sem], recv.at[sem], device_id=device, device_id_type=pl.DeviceIdType.MESH
        )

    def begin(source, target, device):
        made = copy(source, target, sems.take(), device)
        made.start()
        pending.append(made)
        return made

    def bit(number):
        return chip // 2**number % 2

    def across(number):
        return z, 2 * (chip + (1 - 2 * bit(number)) * 2**number) + core

    def mixed(value, plane):
        return sum(
            (value // 2**number + plane // 2 ** (count_bits - 1 - number)) % 2 * 2**number
            for number in range(count_bits)
        )

    def plane_of(value, chunk):
        return sum(
            (value // 2**number + chunk // 2**number) % 2 * 2 ** (count_bits - 1 - number)
            for number in range(count_bits)
        )

    up, down = sems.take(line), sems.take(line)

    def line_begin(step):
        chunk, other = line - step, step - 1

        @pl.when(z == 0)
        def _():
            copy(col_ref.at[chunk], upward.at[chunk], up + chunk, (z + 1, j)).start()

        @pl.when(z == line - 1)
        def _():
            copy(col_ref.at[other], downward.at[other], down + other, (z - 1, j)).start()

    def line_round(step):
        chunk, other = z + line - 1 - step, z - line + 1 + step

        @pl.when((z > 0) & (chunk < line))
        def _():
            copy(upward.at[chunk], upward.at[chunk], up + chunk).wait_recv()
            upward[chunk] += col_ref[chunk]
            copy(upward.at[chunk], upward.at[chunk], up + chunk, (z + 1, j)).start()

        @pl.when((z < line - 1) & (other >= 0))
        def _():
            copy(downward.at[other], downward.at[other], down + other).wait_recv()
            downward[other] += col_ref[other]
            copy(downward.at[other], downward.at[other], down + other, (z - 1, j)).start()

    def line_end():
        total[...] = col_ref[z]

        @pl.when(z > 0)
        def _():
            copy(upward.at[z], upward.at[z], up + z).wait_recv()
            total[...] += upward[z]

        @pl.when(z < line - 1)
        def _():
            copy(downward.at[z], downward.at[z], down + z).wait_recv()
            total[...] += downward[z]

    def line_sent():
        for step in range(1, line):
            chunk, other = line - step, step - 1

            @pl.when(z < chunk)
            def _():
                copy(upward.at[chunk], upward.at[chunk], up + chunk).wait_send()

            @pl.when(z > other)
            def _():
                copy(downward.at[other], downward.at[other], down + other).wait_send()

    def chosen(part, step, flip):
        order = [(part + turn) % count_bits for turn in range(count_bits)]
        free = order[step + 1:]
        picks = []
        for pick in range(2 ** len(free)):
            where = 0
            for turn, number in enumerate(order):
                if number in free:
                    value = pick // 2 ** free.index(number) % 2
                elif turn == step and flip:
                    value = 1 - bit(number)
                else:
                    value = bit(number)
                where = where + value * 2**number
            picks.append(where)
        return order[step], picks

    step_base = [0]
    for step in range(count_bits):
        step_base.append(step_base[-1] + parts * 2 ** (count_bits - 1 - step))

    def plane_send(step):
        made = []
        for part in range(parts):
            number, picks = chosen(part, step, True)
            for slot, pick in enumerate(picks):
                at = step_base[step] + part * len(picks) + slot
                made.append(begin(sums.at[pick, part], landed.at[at], across(number)))
        return made

    def plane_add(step, made):
        for one in made:
            one.wait_recv()
        for part in range(parts):
            _, picks = chosen(part, step, False)
            for slot, pick in enumerate(picks):
                sums[pick, part] += landed[step_base[step] + part * len(picks) + slot]

    line_begin(1)
    held = 2**count_bits
    half = begin(gram_ref.at[pl.ds((1 - core) * held, held)], gram_core, beside)
    core_sum = begin(row_ref.at[1 - core], from_core, beside)
    half.wait_recv()
    gram_work[pl.ds(core * held, held)] = gram_ref[pl.ds(core * held, held)] + gram_core[...]
    for number in reversed(range(count_bits)):
        size = 2**number
        start = core * held + chip // (2 * size) * (2 * size)
        keep, give = start + bit(number) * size, start + (1 - bit(number)) * size
        begin(gram_work.at[pl.ds(give, size)], gram_bits.at[pl.ds(size, size)], across(number)).wait_recv()
        gram_work[pl.ds(keep, size)] += gram_bits[pl.ds(size, size)]
    mine = core * held + chip
    gram_line[z] = gram_work[mine]
    base = sems.take(line)
    for step in range(1, line):
        copy(gram_work.at[mine], gram_line.at[z], base + step, (lax.rem(z + step, line), j)).start()
    for step in range(2, line):
        line_begin(step)

    core_sum.wait_recv()
    for owner in range(line):
        chunk = mixed(owner, z)
        sums[owner] = row_ref[core, chunk] + from_core[chunk]
    made = plane_send(0)

    def gram_back():
        for step in range(1, line):
            copy(gram_work.at[mine], gram_line.at[lax.rem(z + line - step, line)], base + step).wait()
        gram_out[mine] = sum(gram_line[step] for step in range(line))
        for number in range(count_bits):
            size = 2**number
            spot = gram_out.at[pl.ds(core * held + chip // size * size, size)]
            sent = begin(spot, spot, across(number))
            yield
            sent.wait_recv()
        spot = gram_out.at[pl.ds(core * held, held)]
        sent = begin(spot, spot, beside)
        yield
        sent.wait_recv()

    gram_turns = gram_back()
    for step in range(1, line - 1):
        line_round(step)
        next(gram_turns, None)
        if step < count_bits:
            plane_add(step - 1, made)
            made = plane_send(step)
            next(gram_turns, None)
    for _ in gram_turns:
        pass
    for step in range(max(line - 1, 1), count_bits):
        plane_add(step - 1, made)
        made = plane_send(step)
    plane_add(count_bits - 1, made)
    inverse_turns = inverse_steps(gram_out, inverse_out, work)

    def fill(number):
        for _ in range(number):
            next(inverse_turns, None)

    to_cols, first_leg, second_leg = sems.take(), sems.take(2), sems.take(2)
    owned = mixed(chip, z)
    apart = (owned != z) | (z != chip)
    column = (owned, 2 * z + core)
    via = mixed(z, chip)
    beyond = plane_of(chip, z)

    @pl.when(apart)
    def _():
        copy(sums.at[chip], rows_here, to_cols, column).start()

    @pl.when(jnp.logical_not(apart))
    def _():
        rows_here[...] = sums[chip]

    fill(1)
    line_end()

    def piece(ref, number):
        size = total.shape[0] // 2
        return ref.at[pl.ds(number * size, size)]

    def leg_one(number):
        return copy(piece(total, number), piece(relay, number), first_leg + number, (z, 2 * via + core))

    def leg_two(number):
        return copy(piece(relay, number), piece(cols_here, number), second_leg + number, (beyond, j))

    @pl.when(via != chip)
    def _():
        leg_one(0).start()
        leg_one(1).start()

    @pl.when(via == chip)
    def _():
        relay[...] = total[...]

    @pl.when(apart)
    def _():
        copy(sums.at[chip], rows_here, to_cols, column).wait()

    for part in range(parts):
        lanes = slice(part * width, (part + 1) * width)
        cols_out[z, :, lanes] = total[:, lanes] + rows_here[part].T
    around, back = sems.take(line), sems.take(line)

    def line_spread(step):
        chunk, other = z - (step - 1), z + (step - 1)

        @pl.when(chunk >= 0)
        def _():
            if step > 1:
                copy(cols_out.at[chunk], cols_out.at[chunk], around + chunk).wait_recv()

            @pl.when(z < line - 1)
            def _():
                copy(cols_out.at[chunk], cols_out.at[chunk], around + chunk, (z + 1, j)).start()

        @pl.when(other < line)
        def _():
            if step > 1:
                copy(cols_out.at[other], cols_out.at[other], back + other).wait_recv()

            @pl.when(z > 0)
            def _():
                copy(cols_out.at[other], cols_out.at[other], back + other, (z - 1, j)).start()

    def line_spread_sent():
        for step in range(1, line + 1):
            chunk, other = z - (step - 1), z + (step - 1)

            @pl.when((chunk >= 0) & (z < line - 1))
            def _():
                copy(cols_out.at[chunk], cols_out.at[chunk], around + chunk).wait_send()

            @pl.when((other < line) & (z > 0))
            def _():
                copy(cols_out.at[other], cols_out.at[other], back + other).wait_send()

    line_spread(1)
    for number in range(2):

        @pl.when(via != chip)
        def _():
            leg_one(number).wait()

        @pl.when(beyond != z)
        def _():
            leg_two(number).start()

    @pl.when(beyond == z)
    def _():
        cols_here[...] = relay[...]

    fill(3)

    @pl.when(beyond != z)
    def _():
        leg_two(0).wait()
        leg_two(1).wait()

    for part in range(parts):
        lanes = slice(part * width, (part + 1) * width)
        rows_out[core, owned, part] = sums[chip, part] + cols_here[:, lanes].T

    def spots(turn, flip):
        for part in range(parts):
            number, picks = chosen(part, count_bits - 1 - turn, flip)
            for pick in picks:
                yield number, rows_out.at[core, mixed(pick, z), part]

    beside_copies = [begin(rows_out.at[core, owned], rows_out.at[core, owned], beside)]
    for turn in range(max(line - 1, count_bits)):
        if turn < count_bits:
            made = [begin(spot, spot, across(number)) for number, spot in spots(turn, False)]
        if turn == count_bits:
            fill(64)
        if turn + 2 <= line:
            line_spread(turn + 2)
        if turn < count_bits:
            fill(2)
            for one in made:
                one.wait_recv()
            beside_copies += [begin(spot, spot, beside) for _, spot in spots(turn, True)]
    fill(64)
    for one in beside_copies:
        one.wait_recv()
    line_spread_sent()
    line_sent()
    for one in pending:
        one.wait_send()


def exchange(row_part, col_part, gram_part):
    line, many = lax.axis_size("tr"), lax.axis_size("tc")
    count_bits = line.bit_length() - 1
    row_blocks, size, count_obs = row_part.shape
    parts, width = count_bits, size // count_bits
    seg = count_obs // many
    rows = (2, line, parts, width, count_obs)
    cols = col_part.shape
    gram = (many, seg, count_obs)
    landings = sum(parts * 2 ** (count_bits - 1 - step) for step in range(count_bits))
    part = pivot_size(count_obs)
    cross_rows, cross_cols, inverted = pl.pallas_call(
        functools.partial(exchange_kernel, count_bits),
        out_shape=tuple(jax.ShapeDtypeStruct(shape, f32) for shape in (rows, cols, gram_part.shape)),
        in_specs=[VMEM] * 3,
        out_specs=(VMEM,) * 3,
        scratch_shapes=[
            pltpu.VMEM(gram, f32),
            pltpu.VMEM((part, part), f32),
            pltpu.SemaphoreType.DMA((96,)),
            pltpu.SemaphoreType.DMA((96,)),
            pltpu.VMEM(rows[1:], f32),
            pltpu.VMEM(rows[1:], f32),
            pltpu.VMEM((landings, width, count_obs), f32),
            pltpu.VMEM(cols, f32),
            pltpu.VMEM(cols, f32),
            pltpu.VMEM(rows[2:], f32),
            pltpu.VMEM(cols[1:], f32),
            pltpu.VMEM(cols[1:], f32),
            pltpu.VMEM(cols[1:], f32),
            pltpu.VMEM(gram, f32),
            pltpu.VMEM((many // 2, seg, count_obs), f32),
            pltpu.VMEM((many // 2, seg, count_obs), f32),
            pltpu.VMEM((line, seg, count_obs), f32),
        ],
        compiler_params=pltpu.CompilerParams(has_side_effects=True),
        name="exchange",
    )(row_part.reshape(rows), col_part, gram_part.reshape(gram))
    return cross_rows.reshape(row_part.shape), cross_cols, inverted


def body(cov_tiles, block_order, stations, obs_values, obs_error):
    size = obs_values.shape[2]
    line, many = lax.axis_size("tr"), lax.axis_size("tc")
    packed = share(pack(stations, obs_values, obs_error))
    row_part, col_part, gram_part = forward(block_order, packed, cov_tiles, size)
    square = many == 2 * line and line & (line - 1) == 0 and line > 1
    whole_tiles = row_part.shape[0] == many and col_part.shape[0] == line
    spread = exchange if square and whole_tiles else exchange_plain
    cross_rows, cross_cols, inverted = spread(row_part, col_part, gram_part)
    return update(block_order, cross_rows, cross_cols, inverted, cov_tiles)


def solution(mesh):
    in_specs = (P("tr", "tc"), P(), P(None, "tc"), P(None, "tc", None), P(None, "tc"))
    out_specs = P("tr", "tc")
    return jax.shard_map(body, mesh=mesh, in_specs=in_specs, out_specs=out_specs, check_vma=False)
```

```python
import functools

import jax
import jax.numpy as jnp
from jax import lax
from jax.experimental import pallas as pl
from jax.experimental.pallas import tpu as pltpu
from jax.sharding import PartitionSpec as P

exact = lax.Precision.HIGHEST
bf16, f32, i32 = jnp.bfloat16, jnp.float32, jnp.int32
DEPTH = 4
ANY = pl.BlockSpec(memory_space=pl.ANY)
VMEM = pl.BlockSpec(memory_space=pltpu.VMEM)
SMEM = pl.BlockSpec(memory_space=pltpu.SMEM)


def product(former, latter, over, precision=exact):
    return lax.dot_general(
        former,
        latter,
        (((over[0],), (over[1],)), ((), ())),
        precision=precision,
        preferred_element_type=jnp.float32,
    )


def halves(array):
    high = array.astype(bf16)
    return high, (array - high.astype(f32)).astype(bf16)


def dot(former, latter):
    return jnp.dot(former, latter, preferred_element_type=f32)


def dot3(former, latter):
    return dot(former[0], latter[0]) + dot(former[0], latter[1]) + dot(former[1], latter[0])


def list_tiles(order_ref, live_ref, row_blocks, col_blocks, when_dead=None):
    row_first = lax.axis_index("tr") * row_blocks
    col_first = lax.axis_index("tc") * col_blocks

    def step(tile, count):
        row, col = tile // col_blocks, tile % col_blocks
        p, q = row_first + row, col_first + col
        live = (order_ref[p] > order_ref[q]) | (p == q)

        @pl.when(live)
        def _():
            live_ref[count] = tile

        if when_dead is not None:

            @pl.when(jnp.logical_not(live))
            def _():
                when_dead(tile)

        return count + live.astype(i32)

    return lax.fori_loop(0, row_blocks * col_blocks, step, jnp.int32(0))


def tile_at(ref, tile, col_blocks, size):
    row, col = tile // col_blocks, tile % col_blocks
    return ref.at[
        pl.ds(pl.multiple_of(row * size, size), size), pl.ds(pl.multiple_of(col * size, size), size)
    ]


def sorted_by_position(packed, size, order_ref):
    count = packed.shape[0]
    codes = packed[:, size:].T[0:1, :].astype(i32)
    places_across = sum(jnp.where(codes == order_ref[place], place, 0) for place in range(order_ref.shape[0]))
    places = jnp.broadcast_to(places_across.astype(f32), (128, count)).T[:, 0:1].astype(i32)
    down = lax.broadcasted_iota(i32, (count, count), 0)
    across = lax.broadcasted_iota(i32, (count, count), 1)
    earlier = (places < places_across) | ((places == places_across) & (down < across))
    rank = jnp.sum(jnp.where(earlier, 1.0, 0.0), axis=0, keepdims=True).astype(i32)
    return product(jnp.where(down == rank, 1.0, 0.0), packed, (1, 0)), places_across


def reach(count, groups):
    return tuple(min(count, (count * (group + 1) // groups + count // 8 + 7) // 8 * 8) for group in range(groups))


def forward_kernel(
    order_ref, packed_ref, cov_ref, rows_ref, cols_ref, gram_ref, fits_ref,
    live_ref, used_rows, used_cols, held, sem, for_rows, for_cols,
):
    row_blocks, size, count_obs = rows_ref.shape
    col_blocks = cols_ref.shape[0]
    windows, span = for_rows.shape[1], for_rows.shape[2] // 2
    row_first = lax.axis_index("tr") * row_blocks
    col_first = lax.axis_index("tc") * col_blocks
    count = list_tiles(order_ref, live_ref, row_blocks, col_blocks)

    def fetch(at):
        slot = at % DEPTH
        return pltpu.make_async_copy(
            tile_at(cov_ref, live_ref[at], col_blocks, size), held.at[slot], sem.at[slot]
        )

    for at in range(DEPTH - 1):

        @pl.when(at < count)
        def _():
            fetch(at).start()

    packed, places = sorted_by_position(packed_ref[...], size, order_ref)
    groups = lax.axis_size("tr")
    limits = reach(count_obs, groups)
    fits = jnp.int32(1)
    for group in range(groups - 1):
        before = jnp.sum(jnp.where(places < (group + 1) * row_blocks, 1, 0))
        fits = fits * ((before <= limits[group]) & (count_obs - before <= limits[groups - 2 - group])).astype(i32)
    fits_ref[0] = fits
    values = packed[:, :size]
    extras = packed[:, size:]
    codes_down = extras[:, 0:1].astype(i32)
    flipped = extras.T
    codes_across = flipped[0:1, :].astype(i32)
    errors_across = flipped[1:2, :]
    values_t = values.T
    for window in range(windows):
        here = slice(window * span, (window + 1) * span)
        for block in range(row_blocks):
            match = codes_down[here] == order_ref[row_first + block]
            high, low = halves(jnp.where(match, values[here], 0.0))
            for_rows[block, window] = jnp.concatenate((high, low), axis=0)
            same = codes_across[:, here] == order_ref[row_first + block]
            used_rows[block * windows + window] = jnp.sum(jnp.where(same, 1, 0))
        for block in range(col_blocks):
            match = codes_across[:, here] == order_ref[col_first + block]
            high, low = halves(jnp.where(match, values_t[:, here], 0.0))
            for_cols[block, window] = jnp.concatenate((high, low), axis=1)
            used_cols[block * windows + window] = jnp.sum(jnp.where(match, 1, 0))
    rows_ref[...] = jnp.zeros_like(rows_ref)
    cols_ref[...] = jnp.zeros_like(cols_ref)
    gram_ref[...] = jnp.zeros_like(gram_ref)

    def times_cols(parts, block, window):
        both = dot(parts[0], for_cols[block, window]) + dot(parts[1], for_cols[block, window])
        return both[:, :span] + both[:, span:]

    def rows_times(parts, block, window):
        both = dot(for_rows[block, window], parts[0])
        return both[:span] + both[span:] + dot(for_rows[block, window, :span], parts[1])

    def step(at, carry):
        tile = live_ref[at]
        row, col = tile // col_blocks, tile % col_blocks
        slot = at % DEPTH

        @pl.when(at + DEPTH - 1 < count)
        def _():
            fetch(at + DEPTH - 1).start()

        fetch(at).wait()
        strict = row_first + row != col_first + col
        for window in range(windows):
            here = slice(window * span, (window + 1) * span)

            @pl.when(used_cols[col * windows + window] > 0)
            def _():
                rows_ref[row, :, here] += times_cols(halves(held[slot]), col, window)

            @pl.when(strict & (used_rows[row * windows + window] > 0))
            def _():
                cols_ref[col, here] += rows_times(halves(held[slot]), row, window)

        return carry

    lax.fori_loop(0, count, step, 0)

    def add_col(block, carry):
        for window in range(windows):
            here = slice(window * span, (window + 1) * span)

            @pl.when(used_cols[block * windows + window] > 0)
            def _():
                gram_ref[:, here] += times_cols(halves(cols_ref[block]), block, window)

        return carry

    lax.fori_loop(0, col_blocks, add_col, 0)
    first = (lax.axis_index("tr") == 0) & (lax.axis_index("tc") == 0)
    across = lax.broadcasted_iota(i32, (count_obs, count_obs), 1)
    down = lax.broadcasted_iota(i32, (count_obs, count_obs), 0)
    gram_ref[...] = gram_ref[...].T + jnp.where((across == down) & first, errors_across, 0.0)

    def add_row(block, carry):
        for window in range(windows):
            here = slice(window * span, (window + 1) * span)

            @pl.when(used_rows[block * windows + window] > 0)
            def _():
                gram_ref[here] += rows_times(halves(rows_ref[block]), block, window)

        return carry

    lax.fori_loop(0, row_blocks, add_row, 0)


def forward(block_order, packed, cov_tiles, size):
    count_obs = packed.shape[0]
    row_blocks, col_blocks = cov_tiles.shape[0] // size, cov_tiles.shape[1] // size
    tiles = row_blocks * col_blocks
    span = pivot_size(count_obs)
    windows = count_obs // span
    return pl.pallas_call(
        forward_kernel,
        out_shape=(
            jax.ShapeDtypeStruct((row_blocks, size, count_obs), f32),
            jax.ShapeDtypeStruct((col_blocks, count_obs, size), f32),
            jax.ShapeDtypeStruct((count_obs, count_obs), f32),
            jax.ShapeDtypeStruct((1,), i32),
        ),
        in_specs=[SMEM, VMEM, ANY],
        out_specs=(VMEM, VMEM, VMEM, SMEM),
        scratch_shapes=[
            pltpu.SMEM((tiles,), i32),
            pltpu.SMEM((row_blocks * windows,), i32),
            pltpu.SMEM((col_blocks * windows,), i32),
            pltpu.VMEM((DEPTH, size, size), f32),
            pltpu.SemaphoreType.DMA((DEPTH,)),
            pltpu.VMEM((row_blocks, windows, 2 * span, size), bf16),
            pltpu.VMEM((col_blocks, windows, size, 2 * span), bf16),
        ],
        cost_estimate=pl.CostEstimate(
            flops=6 * tiles * size * size * count_obs, bytes_accessed=2 * tiles * size * size, transcendentals=0
        ),
        name="forward",
    )(block_order, packed, cov_tiles)


def update_kernel(
    order_ref, rows_ref, cols_ref, inverse_ref, cov_ref, out_ref,
    live_ref, held, made, zeros, weighted, in_sem, out_sem, zero_sem,
):
    row_blocks, size, _ = rows_ref.shape
    col_blocks = cols_ref.shape[0]
    tiles = row_blocks * col_blocks
    zeros[...] = jnp.zeros_like(zeros)

    def blank(tile):
        return pltpu.make_async_copy(zeros, tile_at(out_ref, tile, col_blocks, size), zero_sem.at[tile])

    count = list_tiles(order_ref, live_ref, row_blocks, col_blocks)

    def fetch(at):
        slot = at % DEPTH
        return pltpu.make_async_copy(
            tile_at(cov_ref, live_ref[at], col_blocks, size), held.at[slot], in_sem.at[slot]
        )

    def put(at):
        slot = at % DEPTH
        return pltpu.make_async_copy(
            made.at[slot], tile_at(out_ref, live_ref[at], col_blocks, size), out_sem.at[slot]
        )

    for at in range(DEPTH - 1):

        @pl.when(at < count)
        def _():
            fetch(at).start()

    list_tiles(order_ref, live_ref, row_blocks, col_blocks, lambda tile: blank(tile).start())
    for block in range(col_blocks):
        weighted[block, 0], weighted[block, 1] = halves(product(inverse_ref[...], cols_ref[block], (1, 0)))

    def step(at, carry):
        tile = live_ref[at]
        row, col = tile // col_blocks, tile % col_blocks
        slot = at % DEPTH

        @pl.when(at + DEPTH - 1 < count)
        def _():
            fetch(at + DEPTH - 1).start()

        @pl.when(at >= DEPTH)
        def _():
            put(at - DEPTH).wait()

        fetch(at).wait()
        made[slot] = held[slot] - dot3(halves(rows_ref[row]), (weighted[col, 0], weighted[col, 1]))
        put(at).start()
        return carry

    lax.fori_loop(0, count, step, 0)
    lax.fori_loop(jnp.maximum(count - DEPTH, 0), count, lambda at, carry: (put(at).wait(), carry)[1], 0)
    list_tiles(order_ref, live_ref, row_blocks, col_blocks, lambda tile: blank(tile).wait())


def update(block_order, cross_rows, cross_cols, inverted, cov_tiles):
    row_blocks, size, count_obs = cross_rows.shape
    col_blocks = cross_cols.shape[0]
    tiles = row_blocks * col_blocks
    return pl.pallas_call(
        update_kernel,
        out_shape=jax.ShapeDtypeStruct(cov_tiles.shape, f32),
        in_specs=[SMEM, VMEM, VMEM, VMEM, ANY],
        out_specs=ANY,
        scratch_shapes=[
            pltpu.SMEM((tiles,), i32),
            pltpu.VMEM((DEPTH, size, size), f32),
            pltpu.VMEM((DEPTH, size, size), f32),
            pltpu.VMEM((size, size), f32),
            pltpu.VMEM((col_blocks, 2, count_obs, size), bf16),
            pltpu.SemaphoreType.DMA((DEPTH,)),
            pltpu.SemaphoreType.DMA((DEPTH,)),
            pltpu.SemaphoreType.DMA((tiles,)),
        ],
        cost_estimate=pl.CostEstimate(
            flops=3 * tiles * size * size * count_obs, bytes_accessed=6 * tiles * size * size, transcendentals=0
        ),
        name="update",
    )(block_order, cross_rows, cross_cols, inverted, cov_tiles)


def swept(matrix, work):
    size = matrix.shape[0]
    work[...] = matrix
    lanes = lax.broadcasted_iota(jnp.int32, (1, size), 1)
    rows = lax.broadcasted_iota(jnp.int32, (size, 1), 0)

    def step(pivot, carry):
        held = work[...]
        row = work[pl.ds(pivot, 1), :]
        at_lane = lanes == pivot
        at_row = rows == pivot
        column = jnp.sum(jnp.where(at_lane, held, 0.0), axis=1, keepdims=True)
        share = 1.0 / jnp.sum(jnp.where(at_lane, row, 0.0), axis=1, keepdims=True)
        kept = jnp.where(at_lane | at_row, 0.0, held)
        left = jnp.where(at_row, -1.0, column)
        right = jnp.where(at_lane, -1.0, row)
        work[...] = kept - left * (right * share)
        return carry

    quarter = size // 4
    for turn in range(4):
        lax.fori_loop(turn * quarter, (turn + 1) * quarter, step, 0)
        yield
    return -work[...]


def inverse_of(matrix, work):
    size = matrix.shape[0]
    if size <= 128:
        return (yield from swept(matrix, work))
    half = size // 2
    upper, corner, lower = matrix[:half, :half], matrix[half:, :half], matrix[half:, half:]
    upper_inverse = yield from inverse_of(upper, work)
    weight = product(corner, upper_inverse, (1, 0))
    lower_inverse = yield from inverse_of(lower - product(weight, corner, (1, 1)), work)
    below = -product(lower_inverse, weight, (1, 0))
    above = upper_inverse - product(weight, below, (0, 0))
    return jnp.concatenate(
        (jnp.concatenate((above, below.T), axis=1), jnp.concatenate((below, lower_inverse), axis=1)), axis=0
    )


def inverse_steps(matrix_ref, inverse_ref, work):
    size = matrix_ref.shape[-1]
    inverse_ref[...] = yield from inverse_of(matrix_ref[...].reshape(size, size), work)


def inverse_kernel(matrix_ref, inverse_ref, work):
    for _ in inverse_steps(matrix_ref, inverse_ref, work):
        pass


def pivot_size(size):
    return size if size <= 128 else pivot_size(size // 2)


def inverse(matrix):
    size = matrix.shape[0]
    part = pivot_size(size)
    return pl.pallas_call(
        inverse_kernel,
        out_shape=jax.ShapeDtypeStruct(matrix.shape, jnp.float32),
        in_specs=[VMEM],
        out_specs=VMEM,
        scratch_shapes=[pltpu.VMEM((part, part), jnp.float32)],
        cost_estimate=pl.CostEstimate(flops=400_000_000, bytes_accessed=8 * size * size, transcendentals=0),
        name="inverse",
    )(matrix)


def pack(stations, obs_values, obs_error):
    values = obs_values[0]
    count, size = values.shape
    return jnp.concatenate(
        (
            values,
            stations[0].astype(f32)[:, None],
            obs_error[0][:, None],
            jnp.zeros((count, 126), f32),
        ),
        axis=1,
    )


def exchange_plain(row_part, col_part, gram_part):
    tr_size, tc_size = lax.axis_size("tr"), lax.axis_size("tc")
    row_blocks, size, count_obs = row_part.shape
    col_blocks = col_part.shape[0]
    row_part = row_part.reshape(row_blocks * size, count_obs)
    col_part = col_part.transpose(0, 2, 1).reshape(col_blocks * size, count_obs)
    innovation = lax.psum(gram_part, ("tr", "tc"))
    count = tr_size * tc_size
    to_rows = [((q % tr_size) * tc_size + q // tr_size, q) for q in range(count)]
    to_cols = [(there, here) for here, there in to_rows]
    col_chunk = lax.psum_scatter(col_part, "tr", scatter_dimension=0, tiled=True)
    row_chunk = lax.psum_scatter(row_part, "tc", scatter_dimension=0, tiled=True)
    chunk = row_chunk + lax.ppermute(col_chunk, ("tr", "tc"), to_rows)
    cross_rows = lax.all_gather(chunk, "tc", axis=0, tiled=True)
    cross_cols = lax.all_gather(lax.ppermute(chunk, ("tr", "tc"), to_cols), "tr", axis=0, tiled=True)
    return (
        cross_rows.reshape(row_blocks, size, count_obs),
        cross_cols.reshape(col_blocks, size, count_obs).transpose(0, 2, 1),
        inverse(innovation),
    )


class Sems:
    def __init__(self):
        self.count = 0

    def take(self, number=1):
        self.count += number
        return self.count - number


def share_kernel(mine_ref, all_ref, send, recv, core_send, core_recv):
    row, col = lax.axis_index("tr"), lax.axis_index("tc")
    chips = all_ref.shape[0] // 2
    chip, core = col // 2, col % 2

    def copy(source, block, step):
        return pltpu.make_async_remote_copy(
            source, all_ref.at[block], send.at[step], recv.at[step],
            device_id=(row, 2 * lax.rem(chip + step, chips) + core), device_id_type=pl.DeviceIdType.MESH,
        )

    def beside(source, block, step):
        return pltpu.make_async_remote_copy(
            source, all_ref.at[block], core_send.at[step], core_recv.at[step],
            device_id=(row, 2 * chip + 1 - core), device_id_type=pl.DeviceIdType.MESH,
        )

    sent = [copy(mine_ref, col, step) for step in range(1, chips)]
    sent.append(beside(mine_ref, col, 0))
    for one in sent:
        one.start()
    all_ref[col] = mine_ref[...]
    for step in range(1, chips):
        block = 2 * lax.rem(chip + chips - step, chips) + core
        copy(mine_ref, block, step).wait_recv()
        sent.append(beside(all_ref.at[block], block, step))
        sent[-1].start()
    for step in range(chips):
        beside(mine_ref, 2 * lax.rem(chip + chips - step, chips) + 1 - core, step).wait_recv()
    for one in sent:
        one.wait_send()


def share(packed):
    many = lax.axis_size("tc")
    full = pl.pallas_call(
        share_kernel,
        out_shape=jax.ShapeDtypeStruct((many, *packed.shape), f32),
        in_specs=[VMEM],
        out_specs=VMEM,
        scratch_shapes=[pltpu.SemaphoreType.DMA((many // 2,))] * 4,
        compiler_params=pltpu.CompilerParams(has_side_effects=True),
        name="share",
    )(packed)
    return full.reshape(many * packed.shape[0], packed.shape[1])


def exchange_kernel(
    count_bits, limits, row_ref, col_ref, gram_ref, rows_out, cols_out, inverse_out,
    gram_out, work, send, recv, from_core, sums, landed, upward, downward, rows_here, cols_here, total, relay,
    gram_work, gram_core, gram_bits, gram_line,
):
    sems = Sems()
    line = lax.axis_size("tr")
    z, j = lax.axis_index("tr"), lax.axis_index("tc")
    chip, core = j // 2, j % 2
    parts = count_bits
    width = rows_here.shape[1]
    pending = []
    beside = (z, 2 * chip + 1 - core)

    def copy(source, target, sem, device=beside):
        return pltpu.make_async_remote_copy(
            source, target, send.at[sem], recv.at[sem], device_id=device, device_id_type=pl.DeviceIdType.MESH
        )

    def begin(source, target, device):
        made = copy(source, target, sems.take(), device)
        made.start()
        pending.append(made)
        return made

    def bit(number):
        return chip // 2**number % 2

    def across(number):
        return z, 2 * (chip + (1 - 2 * bit(number)) * 2**number) + core

    def mixed(value, plane):
        return sum(
            (value // 2**number + plane // 2 ** (count_bits - 1 - number)) % 2 * 2**number
            for number in range(count_bits)
        )

    def plane_of(value, chunk):
        return sum(
            (value // 2**number + chunk // 2**number) % 2 * 2 ** (count_bits - 1 - number)
            for number in range(count_bits)
        )

    up, down = sems.take(line), sems.take(line)

    many_obs = total.shape[0]

    def up_rows(place):
        return pl.ds(0, limits[place])

    def down_rows(place):
        return pl.ds(many_obs - limits[line - 1 - place], limits[line - 1 - place])

    def up_copy(place, chunk, source):
        rows = up_rows(place)
        return copy(source.at[chunk, rows], upward.at[chunk, rows], up + chunk, (z + 1, j))

    def down_copy(place, chunk, source):
        rows = down_rows(place)
        return copy(source.at[chunk, rows], downward.at[chunk, rows], down + chunk, (z - 1, j))

    def line_begin(step):
        @pl.when(z == 0)
        def _():
            up_copy(0, line - step, col_ref).start()

        @pl.when(z == line - 1)
        def _():
            down_copy(line - 1, step - 1, col_ref).start()

    def line_round(step):
        for place in range(1, line - 1):
            chunk, other = place + line - 1 - step, place - line + 1 + step

            @pl.when(z == place)
            def _():
                if chunk < line:
                    fresh = limits[place] - limits[place - 1]
                    up_copy(place - 1, chunk, upward).wait_recv()
                    upward[chunk, up_rows(place - 1)] += col_ref[chunk, up_rows(place - 1)]
                    if fresh:
                        later = pl.ds(limits[place - 1], fresh)
                        upward[chunk, later] = col_ref[chunk, later]
                    up_copy(place, chunk, upward).start()
                if other >= 0:
                    fresh = limits[line - 1 - place] - limits[line - 2 - place]
                    down_copy(place + 1, other, downward).wait_recv()
                    downward[other, down_rows(place + 1)] += col_ref[other, down_rows(place + 1)]
                    if fresh:
                        later = pl.ds(many_obs - limits[line - 1 - place], fresh)
                        downward[other, later] = col_ref[other, later]
                    down_copy(place, other, downward).start()

    def line_end():
        total[...] = col_ref[z]
        for place in range(line):

            @pl.when(z == place)
            def _():
                if place > 0:
                    up_copy(place - 1, place, upward).wait_recv()
                    total[up_rows(place - 1)] += upward[place, up_rows(place - 1)]
                if place < line - 1:
                    down_copy(place + 1, place, downward).wait_recv()
                    total[down_rows(place + 1)] += downward[place, down_rows(place + 1)]

    def line_sent():
        for place in range(line):

            @pl.when(z == place)
            def _():
                for chunk in range(place + 1, line):
                    up_copy(place, chunk, upward).wait_send()
                for other in range(place):
                    down_copy(place, other, downward).wait_send()

    def chosen(part, step, flip):
        order = [(part + turn) % count_bits for turn in range(count_bits)]
        free = order[step + 1:]
        picks = []
        for pick in range(2 ** len(free)):
            where = 0
            for turn, number in enumerate(order):
                if number in free:
                    value = pick // 2 ** free.index(number) % 2
                elif turn == step and flip:
                    value = 1 - bit(number)
                else:
                    value = bit(number)
                where = where + value * 2**number
            picks.append(where)
        return order[step], picks

    step_base = [0]
    for step in range(count_bits):
        step_base.append(step_base[-1] + parts * 2 ** (count_bits - 1 - step))

    def plane_send(step):
        made = []
        for part in range(parts):
            number, picks = chosen(part, step, True)
            for slot, pick in enumerate(picks):
                at = step_base[step] + part * len(picks) + slot
                made.append(begin(sums.at[pick, part], landed.at[at], across(number)))
        return made

    def plane_add(step, made):
        for one in made:
            one.wait_recv()
        for part in range(parts):
            _, picks = chosen(part, step, False)
            for slot, pick in enumerate(picks):
                sums[pick, part] += landed[step_base[step] + part * len(picks) + slot]

    for step in range(1, line):
        line_begin(step)
    held = 2**count_bits
    half = begin(gram_ref.at[pl.ds((1 - core) * held, held)], gram_core, beside)
    core_sum = begin(row_ref.at[1 - core], from_core, beside)
    half.wait_recv()
    gram_work[pl.ds(core * held, held)] = gram_ref[pl.ds(core * held, held)] + gram_core[...]
    for number in reversed(range(count_bits)):
        size = 2**number
        start = core * held + chip // (2 * size) * (2 * size)
        keep, give = start + bit(number) * size, start + (1 - bit(number)) * size
        begin(gram_work.at[pl.ds(give, size)], gram_bits.at[pl.ds(size, size)], across(number)).wait_recv()
        gram_work[pl.ds(keep, size)] += gram_bits[pl.ds(size, size)]
    mine = core * held + chip
    gram_line[z] = gram_work[mine]
    base = sems.take(line)
    for step in range(1, line):
        copy(gram_work.at[mine], gram_line.at[z], base + step, (lax.rem(z + step, line), j)).start()
    core_sum.wait_recv()
    for owner in range(line):
        chunk = mixed(owner, z)
        sums[owner] = row_ref[core, chunk] + from_core[chunk]
    made = plane_send(0)

    def gram_back():
        for step in range(1, line):
            copy(gram_work.at[mine], gram_line.at[lax.rem(z + line - step, line)], base + step).wait()
        gram_out[mine] = sum(gram_line[step] for step in range(line))
        for number in range(count_bits):
            size = 2**number
            spot = gram_out.at[pl.ds(core * held + chip // size * size, size)]
            sent = begin(spot, spot, across(number))
            yield
            sent.wait_recv()
        spot = gram_out.at[pl.ds(core * held, held)]
        sent = begin(spot, spot, beside)
        yield
        sent.wait_recv()

    to_cols, first_leg, second_leg = sems.take(), sems.take(2), sems.take(2)
    owned = mixed(chip, z)
    apart = (owned != z) | (z != chip)
    column = (owned, 2 * z + core)
    via = mixed(z, chip)
    beyond = plane_of(chip, z)

    def piece(ref, number):
        size = total.shape[0] // 2
        return ref.at[pl.ds(number * size, size)]

    def leg_one(number):
        return copy(piece(total, number), piece(relay, number), first_leg + number, (z, 2 * via + core))

    def leg_two(number):
        return copy(piece(relay, number), piece(cols_here, number), second_leg + number, (beyond, j))

    gram_turns = gram_back()
    for step in range(1, line - 1):
        line_round(step)
        next(gram_turns, None)
        if step < count_bits:
            plane_add(step - 1, made)
            made = plane_send(step)
            next(gram_turns, None)
    for step in range(max(line - 1, 1), count_bits):
        plane_add(step - 1, made)
        made = plane_send(step)
    line_end()

    @pl.when(via != chip)
    def _():
        leg_one(0).start()
        leg_one(1).start()

    @pl.when(via == chip)
    def _():
        relay[...] = total[...]

    for _ in gram_turns:
        pass
    plane_add(count_bits - 1, made)
    inverse_turns = inverse_steps(gram_out, inverse_out, work)

    def fill(number):
        for _ in range(number):
            next(inverse_turns, None)

    @pl.when(apart)
    def _():
        copy(sums.at[chip], rows_here, to_cols, column).start()

    @pl.when(jnp.logical_not(apart))
    def _():
        rows_here[...] = sums[chip]

    for number in range(2):

        @pl.when(via != chip)
        def _():
            leg_one(number).wait()

        @pl.when(beyond != z)
        def _():
            leg_two(number).start()

    @pl.when(beyond == z)
    def _():
        cols_here[...] = relay[...]

    fill(2)

    @pl.when(apart)
    def _():
        copy(sums.at[chip], rows_here, to_cols, column).wait()

    for part in range(parts):
        lanes = slice(part * width, (part + 1) * width)
        cols_out[z, :, lanes] = total[:, lanes] + rows_here[part].T
    around, back = sems.take(line), sems.take(line)

    def line_spread(step):
        chunk, other = z - (step - 1), z + (step - 1)

        @pl.when(chunk >= 0)
        def _():
            if step > 1:
                copy(cols_out.at[chunk], cols_out.at[chunk], around + chunk).wait_recv()

            @pl.when(z < line - 1)
            def _():
                copy(cols_out.at[chunk], cols_out.at[chunk], around + chunk, (z + 1, j)).start()

        @pl.when(other < line)
        def _():
            if step > 1:
                copy(cols_out.at[other], cols_out.at[other], back + other).wait_recv()

            @pl.when(z > 0)
            def _():
                copy(cols_out.at[other], cols_out.at[other], back + other, (z - 1, j)).start()

    def line_spread_sent():
        for step in range(1, line + 1):
            chunk, other = z - (step - 1), z + (step - 1)

            @pl.when((chunk >= 0) & (z < line - 1))
            def _():
                copy(cols_out.at[chunk], cols_out.at[chunk], around + chunk).wait_send()

            @pl.when((other < line) & (z > 0))
            def _():
                copy(cols_out.at[other], cols_out.at[other], back + other).wait_send()

    line_spread(1)
    fill(1)

    @pl.when(beyond != z)
    def _():
        leg_two(0).wait()
        leg_two(1).wait()

    for part in range(parts):
        lanes = slice(part * width, (part + 1) * width)
        rows_out[core, owned, part] = sums[chip, part] + cols_here[:, lanes].T

    def spots(turn, flip):
        for part in range(parts):
            number, picks = chosen(part, count_bits - 1 - turn, flip)
            for pick in picks:
                yield number, rows_out.at[core, mixed(pick, z), part]

    beside_copies = [begin(rows_out.at[core, owned], rows_out.at[core, owned], beside)]
    for turn in range(max(line - 1, count_bits)):
        if turn < count_bits:
            made = [begin(spot, spot, across(number)) for number, spot in spots(turn, False)]
        if turn == count_bits:
            fill(64)
        if turn + 2 <= line:
            line_spread(turn + 2)
        if turn < count_bits:
            fill(2)
            for one in made:
                one.wait_recv()
            beside_copies += [begin(spot, spot, beside) for _, spot in spots(turn, True)]
    fill(64)
    for one in beside_copies:
        one.wait_recv()
    line_spread_sent()
    line_sent()
    for one in pending:
        one.wait_send()


def exchange(limits, row_part, col_part, gram_part):
    line, many = lax.axis_size("tr"), lax.axis_size("tc")
    count_bits = line.bit_length() - 1
    row_blocks, size, count_obs = row_part.shape
    parts, width = count_bits, size // count_bits
    seg = count_obs // many
    rows = (2, line, parts, width, count_obs)
    cols = col_part.shape
    gram = (many, seg, count_obs)
    landings = sum(parts * 2 ** (count_bits - 1 - step) for step in range(count_bits))
    part = pivot_size(count_obs)
    cross_rows, cross_cols, inverted = pl.pallas_call(
        functools.partial(exchange_kernel, count_bits, limits),
        out_shape=tuple(jax.ShapeDtypeStruct(shape, f32) for shape in (rows, cols, gram_part.shape)),
        in_specs=[VMEM] * 3,
        out_specs=(VMEM,) * 3,
        scratch_shapes=[
            pltpu.VMEM(gram, f32),
            pltpu.VMEM((part, part), f32),
            pltpu.SemaphoreType.DMA((96,)),
            pltpu.SemaphoreType.DMA((96,)),
            pltpu.VMEM(rows[1:], f32),
            pltpu.VMEM(rows[1:], f32),
            pltpu.VMEM((landings, width, count_obs), f32),
            pltpu.VMEM(cols, f32),
            pltpu.VMEM(cols, f32),
            pltpu.VMEM(rows[2:], f32),
            pltpu.VMEM(cols[1:], f32),
            pltpu.VMEM(cols[1:], f32),
            pltpu.VMEM(cols[1:], f32),
            pltpu.VMEM(gram, f32),
            pltpu.VMEM((many // 2, seg, count_obs), f32),
            pltpu.VMEM((many // 2, seg, count_obs), f32),
            pltpu.VMEM((line, seg, count_obs), f32),
        ],
        compiler_params=pltpu.CompilerParams(has_side_effects=True),
        name="exchange",
    )(row_part.reshape(rows), col_part, gram_part.reshape(gram))
    return cross_rows.reshape(row_part.shape), cross_cols, inverted


def body(cov_tiles, block_order, stations, obs_values, obs_error):
    size = obs_values.shape[2]
    line, many = lax.axis_size("tr"), lax.axis_size("tc")
    packed = share(pack(stations, obs_values, obs_error))
    row_part, col_part, gram_part, fits = forward(block_order, packed, cov_tiles, size)
    square = many == 2 * line and line & (line - 1) == 0 and line > 1
    whole_tiles = row_part.shape[0] == many and col_part.shape[0] == line
    parts = (row_part, col_part, gram_part)
    if square and whole_tiles:
        count_obs = gram_part.shape[0]
        cross_rows, cross_cols, inverted = lax.cond(
            fits[0] > 0,
            functools.partial(exchange, reach(count_obs, line)),
            functools.partial(exchange, (count_obs,) * line),
            *parts,
        )
    else:
        cross_rows, cross_cols, inverted = exchange_plain(*parts)
    return update(block_order, cross_rows, cross_cols, inverted, cov_tiles)


def solution(mesh):
    in_specs = (P("tr", "tc"), P(), P(None, "tc"), P(None, "tc", None), P(None, "tc"))
    out_specs = P("tr", "tc")
    return jax.shard_map(body, mesh=mesh, in_specs=in_specs, out_specs=out_specs, check_vma=False)
```

```python
import functools

import jax
import jax.numpy as jnp
from jax import lax
from jax.experimental import pallas as pl
from jax.experimental.pallas import tpu as pltpu
from jax.sharding import PartitionSpec as P

exact = lax.Precision.HIGHEST
bf16, f32, i32 = jnp.bfloat16, jnp.float32, jnp.int32
DEPTH = 4
ROOM = 40 * 2**20
ANY = pl.BlockSpec(memory_space=pl.ANY)
VMEM = pl.BlockSpec(memory_space=pltpu.VMEM)
SMEM = pl.BlockSpec(memory_space=pltpu.SMEM)


def product(former, latter, over, precision=exact):
    return lax.dot_general(
        former,
        latter,
        (((over[0],), (over[1],)), ((), ())),
        precision=precision,
        preferred_element_type=jnp.float32,
    )


def halves(array):
    high = array.astype(bf16)
    return high, (array - high.astype(f32)).astype(bf16)


def dot(former, latter):
    return jnp.dot(former, latter, preferred_element_type=f32)


def dot3(former, latter):
    return dot(former[0], latter[0]) + dot(former[0], latter[1]) + dot(former[1], latter[0])


def list_tiles(order_ref, live_ref, row_blocks, col_blocks, when_dead=None):
    row_first = lax.axis_index("tr") * row_blocks
    col_first = lax.axis_index("tc") * col_blocks

    def step(tile, count):
        row, col = tile // col_blocks, tile % col_blocks
        p, q = row_first + row, col_first + col
        live = (order_ref[p] > order_ref[q]) | (p == q)

        @pl.when(live)
        def _():
            live_ref[count] = tile

        if when_dead is not None:

            @pl.when(jnp.logical_not(live))
            def _():
                when_dead(tile)

        return count + live.astype(i32)

    return lax.fori_loop(0, row_blocks * col_blocks, step, jnp.int32(0))


def tile_at(ref, tile, col_blocks, size):
    row, col = tile // col_blocks, tile % col_blocks
    return ref.at[
        pl.ds(pl.multiple_of(row * size, size), size), pl.ds(pl.multiple_of(col * size, size), size)
    ]


def sorted_by_position(packed, size, order_ref):
    count = packed.shape[0]
    codes = packed[:, size:].T[0:1, :].astype(i32)
    places_across = sum(jnp.where(codes == order_ref[place], place, 0) for place in range(order_ref.shape[0]))
    places = jnp.broadcast_to(places_across.astype(f32), (128, count)).T[:, 0:1].astype(i32)
    down = lax.broadcasted_iota(i32, (count, count), 0)
    across = lax.broadcasted_iota(i32, (count, count), 1)
    earlier = (places < places_across) | ((places == places_across) & (down < across))
    rank = jnp.sum(jnp.where(earlier, 1.0, 0.0), axis=0, keepdims=True).astype(i32)
    return product(jnp.where(down == rank, 1.0, 0.0), packed, (1, 0)), places_across


def reach(count, groups):
    return tuple(min(count, (count * (group + 1) // groups + count // 8 + 7) // 8 * 8) for group in range(groups))


def forward_kernel(
    order_ref, packed_ref, cov_ref, rows_ref, cols_ref, gram_ref, fits_ref,
    live_ref, used_rows, used_cols, held, sem, for_rows, for_cols,
):
    row_blocks, size, count_obs = rows_ref.shape
    col_blocks = cols_ref.shape[0]
    windows, span = for_rows.shape[1], for_rows.shape[2] // 2
    row_first = lax.axis_index("tr") * row_blocks
    col_first = lax.axis_index("tc") * col_blocks
    count = list_tiles(order_ref, live_ref, row_blocks, col_blocks)

    def fetch(at):
        slot = at % DEPTH
        return pltpu.make_async_copy(
            tile_at(cov_ref, live_ref[at], col_blocks, size), held.at[slot], sem.at[slot]
        )

    for at in range(DEPTH - 1):

        @pl.when(at < count)
        def _():
            fetch(at).start()

    packed, places = sorted_by_position(packed_ref[...], size, order_ref)
    groups = lax.axis_size("tr")
    limits = reach(count_obs, groups)
    fits = jnp.int32(1)
    for group in range(groups - 1):
        before = jnp.sum(jnp.where(places < (group + 1) * row_blocks, 1, 0))
        fits = fits * ((before <= limits[group]) & (count_obs - before <= limits[groups - 2 - group])).astype(i32)
    fits_ref[0] = fits
    values = packed[:, :size]
    extras = packed[:, size:]
    codes_down = extras[:, 0:1].astype(i32)
    flipped = extras.T
    codes_across = flipped[0:1, :].astype(i32)
    errors_across = flipped[1:2, :]
    values_t = values.T
    for window in range(windows):
        here = slice(window * span, (window + 1) * span)
        for block in range(row_blocks):
            match = codes_down[here] == order_ref[row_first + block]
            high, low = halves(jnp.where(match, values[here], 0.0))
            for_rows[block, window] = jnp.concatenate((high, low), axis=0)
            same = codes_across[:, here] == order_ref[row_first + block]
            used_rows[block * windows + window] = jnp.sum(jnp.where(same, 1, 0))
        for block in range(col_blocks):
            match = codes_across[:, here] == order_ref[col_first + block]
            high, low = halves(jnp.where(match, values_t[:, here], 0.0))
            for_cols[block, window] = jnp.concatenate((high, low), axis=1)
            used_cols[block * windows + window] = jnp.sum(jnp.where(match, 1, 0))
    rows_ref[...] = jnp.zeros_like(rows_ref)
    cols_ref[...] = jnp.zeros_like(cols_ref)
    gram_ref[...] = jnp.zeros_like(gram_ref)

    def times_cols(parts, block, window):
        both = dot(parts[0], for_cols[block, window]) + dot(parts[1], for_cols[block, window])
        return both[:, :span] + both[:, span:]

    def rows_times(parts, block, window):
        both = dot(for_rows[block, window], parts[0])
        return both[:span] + both[span:] + dot(for_rows[block, window, :span], parts[1])

    def step(at, carry):
        tile = live_ref[at]
        row, col = tile // col_blocks, tile % col_blocks
        slot = at % DEPTH

        @pl.when(at + DEPTH - 1 < count)
        def _():
            fetch(at + DEPTH - 1).start()

        fetch(at).wait()
        strict = row_first + row != col_first + col
        for window in range(windows):
            here = slice(window * span, (window + 1) * span)

            @pl.when(used_cols[col * windows + window] > 0)
            def _():
                rows_ref[row, :, here] += times_cols(halves(held[slot]), col, window)

            @pl.when(strict & (used_rows[row * windows + window] > 0))
            def _():
                cols_ref[col, here] += rows_times(halves(held[slot]), row, window)

        return carry

    lax.fori_loop(0, count, step, 0)

    def add_col(block, carry):
        for window in range(windows):
            here = slice(window * span, (window + 1) * span)

            @pl.when(used_cols[block * windows + window] > 0)
            def _():
                gram_ref[:, here] += times_cols(halves(cols_ref[block]), block, window)

        return carry

    lax.fori_loop(0, col_blocks, add_col, 0)
    first = (lax.axis_index("tr") == 0) & (lax.axis_index("tc") == 0)
    across = lax.broadcasted_iota(i32, (count_obs, count_obs), 1)
    down = lax.broadcasted_iota(i32, (count_obs, count_obs), 0)
    gram_ref[...] = gram_ref[...].T + jnp.where((across == down) & first, errors_across, 0.0)

    def add_row(block, carry):
        for window in range(windows):
            here = slice(window * span, (window + 1) * span)

            @pl.when(used_rows[block * windows + window] > 0)
            def _():
                gram_ref[here] += rows_times(halves(rows_ref[block]), block, window)

        return carry

    lax.fori_loop(0, row_blocks, add_row, 0)


def forward(block_order, packed, cov_tiles, size):
    count_obs = packed.shape[0]
    row_blocks, col_blocks = cov_tiles.shape[0] // size, cov_tiles.shape[1] // size
    tiles = row_blocks * col_blocks
    span = pivot_size(count_obs)
    windows = count_obs // span
    return pl.pallas_call(
        forward_kernel,
        out_shape=(
            jax.ShapeDtypeStruct((row_blocks, size, count_obs), f32),
            jax.ShapeDtypeStruct((col_blocks, count_obs, size), f32),
            jax.ShapeDtypeStruct((count_obs, count_obs), f32),
            jax.ShapeDtypeStruct((1,), i32),
        ),
        in_specs=[SMEM, VMEM, ANY],
        out_specs=(VMEM, VMEM, VMEM, SMEM),
        scratch_shapes=[
            pltpu.SMEM((tiles,), i32),
            pltpu.SMEM((row_blocks * windows,), i32),
            pltpu.SMEM((col_blocks * windows,), i32),
            pltpu.VMEM((DEPTH, size, size), f32),
            pltpu.SemaphoreType.DMA((DEPTH,)),
            pltpu.VMEM((row_blocks, windows, 2 * span, size), bf16),
            pltpu.VMEM((col_blocks, windows, size, 2 * span), bf16),
        ],
        cost_estimate=pl.CostEstimate(
            flops=6 * tiles * size * size * count_obs, bytes_accessed=2 * tiles * size * size, transcendentals=0
        ),
        compiler_params=pltpu.CompilerParams(vmem_limit_bytes=ROOM),
        name="forward",
    )(block_order, packed, cov_tiles)


def update_kernel(
    order_ref, rows_ref, cols_ref, inverse_ref, cov_ref, out_ref,
    live_ref, held, made, zeros, weighted, in_sem, out_sem, zero_sem,
):
    row_blocks, size, _ = rows_ref.shape
    col_blocks = cols_ref.shape[0]
    tiles = row_blocks * col_blocks
    zeros[...] = jnp.zeros_like(zeros)

    def blank(tile):
        return pltpu.make_async_copy(zeros, tile_at(out_ref, tile, col_blocks, size), zero_sem.at[tile])

    count = list_tiles(order_ref, live_ref, row_blocks, col_blocks)

    def fetch(at):
        slot = at % DEPTH
        return pltpu.make_async_copy(
            tile_at(cov_ref, live_ref[at], col_blocks, size), held.at[slot], in_sem.at[slot]
        )

    def put(at):
        slot = at % DEPTH
        return pltpu.make_async_copy(
            made.at[slot], tile_at(out_ref, live_ref[at], col_blocks, size), out_sem.at[slot]
        )

    for at in range(DEPTH - 1):

        @pl.when(at < count)
        def _():
            fetch(at).start()

    list_tiles(order_ref, live_ref, row_blocks, col_blocks, lambda tile: blank(tile).start())
    for block in range(col_blocks):
        weighted[block, 0], weighted[block, 1] = halves(product(inverse_ref[...], cols_ref[block], (1, 0)))

    def step(at, carry):
        tile = live_ref[at]
        row, col = tile // col_blocks, tile % col_blocks
        slot = at % DEPTH

        @pl.when(at + DEPTH - 1 < count)
        def _():
            fetch(at + DEPTH - 1).start()

        @pl.when(at >= DEPTH)
        def _():
            put(at - DEPTH).wait()

        fetch(at).wait()
        made[slot] = held[slot] - dot3(halves(rows_ref[row]), (weighted[col, 0], weighted[col, 1]))
        put(at).start()
        return carry

    lax.fori_loop(0, count, step, 0)
    lax.fori_loop(jnp.maximum(count - DEPTH, 0), count, lambda at, carry: (put(at).wait(), carry)[1], 0)
    list_tiles(order_ref, live_ref, row_blocks, col_blocks, lambda tile: blank(tile).wait())


def update(block_order, cross_rows, cross_cols, inverted, cov_tiles):
    row_blocks, size, count_obs = cross_rows.shape
    col_blocks = cross_cols.shape[0]
    tiles = row_blocks * col_blocks
    return pl.pallas_call(
        update_kernel,
        out_shape=jax.ShapeDtypeStruct(cov_tiles.shape, f32),
        in_specs=[SMEM, VMEM, VMEM, VMEM, ANY],
        out_specs=ANY,
        scratch_shapes=[
            pltpu.SMEM((tiles,), i32),
            pltpu.VMEM((DEPTH, size, size), f32),
            pltpu.VMEM((DEPTH, size, size), f32),
            pltpu.VMEM((size, size), f32),
            pltpu.VMEM((col_blocks, 2, count_obs, size), bf16),
            pltpu.SemaphoreType.DMA((DEPTH,)),
            pltpu.SemaphoreType.DMA((DEPTH,)),
            pltpu.SemaphoreType.DMA((tiles,)),
        ],
        cost_estimate=pl.CostEstimate(
            flops=3 * tiles * size * size * count_obs, bytes_accessed=6 * tiles * size * size, transcendentals=0
        ),
        compiler_params=pltpu.CompilerParams(vmem_limit_bytes=ROOM),
        name="update",
    )(block_order, cross_rows, cross_cols, inverted, cov_tiles)


def swept(matrix, work):
    size = matrix.shape[0]
    work[...] = matrix
    lanes = lax.broadcasted_iota(jnp.int32, (1, size), 1)
    rows = lax.broadcasted_iota(jnp.int32, (size, 1), 0)

    def step(pivot, carry):
        held = work[...]
        row = work[pl.ds(pivot, 1), :]
        at_lane = lanes == pivot
        at_row = rows == pivot
        column = jnp.sum(jnp.where(at_lane, held, 0.0), axis=1, keepdims=True)
        share = 1.0 / jnp.sum(jnp.where(at_lane, row, 0.0), axis=1, keepdims=True)
        kept = jnp.where(at_lane | at_row, 0.0, held)
        left = jnp.where(at_row, -1.0, column)
        right = jnp.where(at_lane, -1.0, row)
        work[...] = kept - left * (right * share)
        return carry

    quarter = size // 4
    for turn in range(4):
        lax.fori_loop(turn * quarter, (turn + 1) * quarter, step, 0)
        yield
    return -work[...]


def inverse_of(matrix, work):
    size = matrix.shape[0]
    if size <= 128:
        return (yield from swept(matrix, work))
    half = size // 2
    upper, corner, lower = matrix[:half, :half], matrix[half:, :half], matrix[half:, half:]
    upper_inverse = yield from inverse_of(upper, work)
    weight = product(corner, upper_inverse, (1, 0))
    lower_inverse = yield from inverse_of(lower - product(weight, corner, (1, 1)), work)
    below = -product(lower_inverse, weight, (1, 0))
    above = upper_inverse - product(weight, below, (0, 0))
    return jnp.concatenate(
        (jnp.concatenate((above, below.T), axis=1), jnp.concatenate((below, lower_inverse), axis=1)), axis=0
    )


def inverse_steps(matrix_ref, inverse_ref, work):
    size = matrix_ref.shape[-1]
    inverse_ref[...] = yield from inverse_of(matrix_ref[...].reshape(size, size), work)


def inverse_kernel(matrix_ref, inverse_ref, work):
    for _ in inverse_steps(matrix_ref, inverse_ref, work):
        pass


def pivot_size(size):
    return size if size <= 128 else pivot_size(size // 2)


def inverse(matrix):
    size = matrix.shape[0]
    part = pivot_size(size)
    return pl.pallas_call(
        inverse_kernel,
        out_shape=jax.ShapeDtypeStruct(matrix.shape, jnp.float32),
        in_specs=[VMEM],
        out_specs=VMEM,
        scratch_shapes=[pltpu.VMEM((part, part), jnp.float32)],
        cost_estimate=pl.CostEstimate(flops=400_000_000, bytes_accessed=8 * size * size, transcendentals=0),
        name="inverse",
    )(matrix)


def exchange_plain(row_part, col_part, gram_part):
    tr_size, tc_size = lax.axis_size("tr"), lax.axis_size("tc")
    row_blocks, size, count_obs = row_part.shape
    col_blocks = col_part.shape[0]
    row_part = row_part.reshape(row_blocks * size, count_obs)
    col_part = col_part.transpose(0, 2, 1).reshape(col_blocks * size, count_obs)
    innovation = lax.psum(gram_part, ("tr", "tc"))
    count = tr_size * tc_size
    to_rows = [((q % tr_size) * tc_size + q // tr_size, q) for q in range(count)]
    to_cols = [(there, here) for here, there in to_rows]
    col_chunk = lax.psum_scatter(col_part, "tr", scatter_dimension=0, tiled=True)
    row_chunk = lax.psum_scatter(row_part, "tc", scatter_dimension=0, tiled=True)
    chunk = row_chunk + lax.ppermute(col_chunk, ("tr", "tc"), to_rows)
    cross_rows = lax.all_gather(chunk, "tc", axis=0, tiled=True)
    cross_cols = lax.all_gather(lax.ppermute(chunk, ("tr", "tc"), to_cols), "tr", axis=0, tiled=True)
    return (
        cross_rows.reshape(row_blocks, size, count_obs),
        cross_cols.reshape(col_blocks, size, count_obs).transpose(0, 2, 1),
        inverse(innovation),
    )


class Sems:
    def __init__(self):
        self.count = 0

    def take(self, number=1):
        self.count += number
        return self.count - number


def share_kernel(stations_ref, values_ref, errors_ref, all_ref, mine_ref, send, recv, core_send, core_recv):
    row, col = lax.axis_index("tr"), lax.axis_index("tc")
    chips = all_ref.shape[0] // 2
    chip, core = col // 2, col % 2

    def copy(source, block, step):
        return pltpu.make_async_remote_copy(
            source, all_ref.at[block], send.at[step], recv.at[step],
            device_id=(row, 2 * lax.rem(chip + step, chips) + core), device_id_type=pl.DeviceIdType.MESH,
        )

    def beside(source, block, step):
        return pltpu.make_async_remote_copy(
            source, all_ref.at[block], core_send.at[step], core_recv.at[step],
            device_id=(row, 2 * chip + 1 - core), device_id_type=pl.DeviceIdType.MESH,
        )

    number, size = values_ref.shape[1:]
    equal = lax.broadcasted_iota(i32, (number, number), 0) == lax.broadcasted_iota(i32, (number, number), 1)

    def upright(across):
        return jnp.sum(jnp.where(equal, across, 0.0), axis=1, keepdims=True)

    lanes = lax.broadcasted_iota(i32, (number, mine_ref.shape[1] - size), 1)
    stations, errors = upright(stations_ref[...].astype(f32)), upright(errors_ref[...])
    mine_ref[:, :size] = values_ref[0]
    mine_ref[:, size:] = jnp.where(lanes == 0, stations, jnp.where(lanes == 1, errors, 0.0))
    sent = [copy(mine_ref, col, step) for step in range(1, chips)]
    sent.append(beside(mine_ref, col, 0))
    for one in sent:
        one.start()
    all_ref[col] = mine_ref[...]
    for step in range(1, chips):
        block = 2 * lax.rem(chip + chips - step, chips) + core
        copy(mine_ref, block, step).wait_recv()
        sent.append(beside(all_ref.at[block], block, step))
        sent[-1].start()
    for step in range(chips):
        beside(mine_ref, 2 * lax.rem(chip + chips - step, chips) + 1 - core, step).wait_recv()
    for one in sent:
        one.wait_send()


def share(stations, obs_values, obs_error):
    many = lax.axis_size("tc")
    _, number, size = obs_values.shape
    packed = (number, size + 128)
    full = pl.pallas_call(
        share_kernel,
        out_shape=jax.ShapeDtypeStruct((many, *packed), f32),
        in_specs=[VMEM] * 3,
        out_specs=VMEM,
        scratch_shapes=[pltpu.VMEM(packed, f32)] + [pltpu.SemaphoreType.DMA((many // 2,))] * 4,
        compiler_params=pltpu.CompilerParams(has_side_effects=True, vmem_limit_bytes=8 * 2**20),
        name="share",
    )(stations, obs_values, obs_error)
    return full.reshape(many * number, size + 128)


def exchange_kernel(
    count_bits, limits, row_ref, col_ref, gram_ref, rows_out, cols_out, inverse_out,
    gram_out, work, send, recv, from_core, sums, landed, upward, downward, rows_here, cols_here, total, relay,
    gram_work, gram_core, gram_bits, gram_line,
):
    sems = Sems()
    line = lax.axis_size("tr")
    z, j = lax.axis_index("tr"), lax.axis_index("tc")
    chip, core = j // 2, j % 2
    parts = count_bits
    width = rows_here.shape[1]
    pending = []
    beside = (z, 2 * chip + 1 - core)

    def copy(source, target, sem, device=beside):
        return pltpu.make_async_remote_copy(
            source, target, send.at[sem], recv.at[sem], device_id=device, device_id_type=pl.DeviceIdType.MESH
        )

    def begin(source, target, device):
        made = copy(source, target, sems.take(), device)
        made.start()
        pending.append(made)
        return made

    def bit(number):
        return chip // 2**number % 2

    def across(number):
        return z, 2 * (chip + (1 - 2 * bit(number)) * 2**number) + core

    def mixed(value, plane):
        return sum(
            (value // 2**number + plane // 2 ** (count_bits - 1 - number)) % 2 * 2**number
            for number in range(count_bits)
        )

    def plane_of(value, chunk):
        return sum(
            (value // 2**number + chunk // 2**number) % 2 * 2 ** (count_bits - 1 - number)
            for number in range(count_bits)
        )

    up, down = sems.take(line), sems.take(line)

    many_obs = total.shape[0]

    def up_rows(place):
        return pl.ds(0, limits[place])

    def down_rows(place):
        return pl.ds(many_obs - limits[line - 1 - place], limits[line - 1 - place])

    def up_copy(place, chunk, source):
        rows = up_rows(place)
        return copy(source.at[chunk, rows], upward.at[chunk, rows], up + chunk, (z + 1, j))

    def down_copy(place, chunk, source):
        rows = down_rows(place)
        return copy(source.at[chunk, rows], downward.at[chunk, rows], down + chunk, (z - 1, j))

    def line_begin(step):
        @pl.when(z == 0)
        def _():
            up_copy(0, line - step, col_ref).start()

        @pl.when(z == line - 1)
        def _():
            down_copy(line - 1, step - 1, col_ref).start()

    def line_round(step):
        for place in range(1, line - 1):
            chunk, other = place + line - 1 - step, place - line + 1 + step

            @pl.when(z == place)
            def _():
                if chunk < line:
                    fresh = limits[place] - limits[place - 1]
                    up_copy(place - 1, chunk, upward).wait_recv()
                    upward[chunk, up_rows(place - 1)] += col_ref[chunk, up_rows(place - 1)]
                    if fresh:
                        later = pl.ds(limits[place - 1], fresh)
                        upward[chunk, later] = col_ref[chunk, later]
                    up_copy(place, chunk, upward).start()
                if other >= 0:
                    fresh = limits[line - 1 - place] - limits[line - 2 - place]
                    down_copy(place + 1, other, downward).wait_recv()
                    downward[other, down_rows(place + 1)] += col_ref[other, down_rows(place + 1)]
                    if fresh:
                        later = pl.ds(many_obs - limits[line - 1 - place], fresh)
                        downward[other, later] = col_ref[other, later]
                    down_copy(place, other, downward).start()

    def line_end():
        total[...] = col_ref[z]
        for place in range(line):

            @pl.when(z == place)
            def _():
                if place > 0:
                    up_copy(place - 1, place, upward).wait_recv()
                    total[up_rows(place - 1)] += upward[place, up_rows(place - 1)]
                if place < line - 1:
                    down_copy(place + 1, place, downward).wait_recv()
                    total[down_rows(place + 1)] += downward[place, down_rows(place + 1)]

    def line_sent():
        for place in range(line):

            @pl.when(z == place)
            def _():
                for chunk in range(place + 1, line):
                    up_copy(place, chunk, upward).wait_send()
                for other in range(place):
                    down_copy(place, other, downward).wait_send()

    def chosen(part, step, flip):
        order = [(part + turn) % count_bits for turn in range(count_bits)]
        free = order[step + 1:]
        picks = []
        for pick in range(2 ** len(free)):
            where = 0
            for turn, number in enumerate(order):
                if number in free:
                    value = pick // 2 ** free.index(number) % 2
                elif turn == step and flip:
                    value = 1 - bit(number)
                else:
                    value = bit(number)
                where = where + value * 2**number
            picks.append(where)
        return order[step], picks

    step_base = [0]
    for step in range(count_bits):
        step_base.append(step_base[-1] + parts * 2 ** (count_bits - 1 - step))

    def plane_send(step):
        made = []
        for part in range(parts):
            number, picks = chosen(part, step, True)
            for slot, pick in enumerate(picks):
                at = step_base[step] + part * len(picks) + slot
                made.append(begin(sums.at[pick, part], landed.at[at], across(number)))
        return made

    def plane_add(step, made):
        for one in made:
            one.wait_recv()
        for part in range(parts):
            _, picks = chosen(part, step, False)
            for slot, pick in enumerate(picks):
                sums[pick, part] += landed[step_base[step] + part * len(picks) + slot]

    for step in range(1, line):
        line_begin(step)
    held = 2**count_bits
    half = begin(gram_ref.at[pl.ds((1 - core) * held, held)], gram_core, beside)
    core_sum = begin(row_ref.at[1 - core], from_core, beside)
    half.wait_recv()
    gram_work[pl.ds(core * held, held)] = gram_ref[pl.ds(core * held, held)] + gram_core[...]
    for number in reversed(range(count_bits)):
        size = 2**number
        start = core * held + chip // (2 * size) * (2 * size)
        keep, give = start + bit(number) * size, start + (1 - bit(number)) * size
        begin(gram_work.at[pl.ds(give, size)], gram_bits.at[pl.ds(size, size)], across(number)).wait_recv()
        gram_work[pl.ds(keep, size)] += gram_bits[pl.ds(size, size)]
    mine = core * held + chip
    gram_line[z] = gram_work[mine]
    base = sems.take(line)
    for step in range(1, line):
        copy(gram_work.at[mine], gram_line.at[z], base + step, (lax.rem(z + step, line), j)).start()
    core_sum.wait_recv()
    for owner in range(line):
        chunk = mixed(owner, z)
        sums[owner] = row_ref[core, chunk] + from_core[chunk]
    made = plane_send(0)

    def gram_back():
        for step in range(1, line):
            copy(gram_work.at[mine], gram_line.at[lax.rem(z + line - step, line)], base + step).wait()
        gram_out[mine] = sum(gram_line[step] for step in range(line))
        for number in range(count_bits):
            size = 2**number
            spot = gram_out.at[pl.ds(core * held + chip // size * size, size)]
            sent = begin(spot, spot, across(number))
            yield
            sent.wait_recv()
        spot = gram_out.at[pl.ds(core * held, held)]
        sent = begin(spot, spot, beside)
        yield
        sent.wait_recv()

    to_cols, first_leg, second_leg = sems.take(), sems.take(2), sems.take(2)
    owned = mixed(chip, z)
    apart = (owned != z) | (z != chip)
    column = (owned, 2 * z + core)
    via = mixed(z, chip)
    beyond = plane_of(chip, z)

    def piece(ref, number):
        size = total.shape[0] // 2
        return ref.at[pl.ds(number * size, size)]

    def leg_one(number):
        return copy(piece(total, number), piece(relay, number), first_leg + number, (z, 2 * via + core))

    def leg_two(number):
        return copy(piece(relay, number), piece(cols_here, number), second_leg + number, (beyond, j))

    gram_turns = gram_back()
    for step in range(1, line - 1):
        line_round(step)
        next(gram_turns, None)
        if step < count_bits:
            plane_add(step - 1, made)
            made = plane_send(step)
            next(gram_turns, None)
    for step in range(max(line - 1, 1), count_bits):
        plane_add(step - 1, made)
        made = plane_send(step)
    line_end()

    @pl.when(via != chip)
    def _():
        leg_one(0).start()
        leg_one(1).start()

    @pl.when(via == chip)
    def _():
        relay[...] = total[...]

    for _ in gram_turns:
        pass
    plane_add(count_bits - 1, made)
    inverse_turns = inverse_steps(gram_out, inverse_out, work)

    def fill(number):
        for _ in range(number):
            next(inverse_turns, None)

    @pl.when(apart)
    def _():
        copy(sums.at[chip], rows_here, to_cols, column).start()

    @pl.when(jnp.logical_not(apart))
    def _():
        rows_here[...] = sums[chip]

    for number in range(2):

        @pl.when(via != chip)
        def _():
            leg_one(number).wait()

        @pl.when(beyond != z)
        def _():
            leg_two(number).start()

    @pl.when(beyond == z)
    def _():
        cols_here[...] = relay[...]

    fill(2)

    @pl.when(apart)
    def _():
        copy(sums.at[chip], rows_here, to_cols, column).wait()

    for part in range(parts):
        lanes = slice(part * width, (part + 1) * width)
        cols_out[z, :, lanes] = total[:, lanes] + rows_here[part].T
    around, back = sems.take(line), sems.take(line)

    def line_spread(step):
        chunk, other = z - (step - 1), z + (step - 1)

        @pl.when(chunk >= 0)
        def _():
            if step > 1:
                copy(cols_out.at[chunk], cols_out.at[chunk], around + chunk).wait_recv()

            @pl.when(z < line - 1)
            def _():
                copy(cols_out.at[chunk], cols_out.at[chunk], around + chunk, (z + 1, j)).start()

        @pl.when(other < line)
        def _():
            if step > 1:
                copy(cols_out.at[other], cols_out.at[other], back + other).wait_recv()

            @pl.when(z > 0)
            def _():
                copy(cols_out.at[other], cols_out.at[other], back + other, (z - 1, j)).start()

    def line_spread_sent():
        for step in range(1, line + 1):
            chunk, other = z - (step - 1), z + (step - 1)

            @pl.when((chunk >= 0) & (z < line - 1))
            def _():
                copy(cols_out.at[chunk], cols_out.at[chunk], around + chunk).wait_send()

            @pl.when((other < line) & (z > 0))
            def _():
                copy(cols_out.at[other], cols_out.at[other], back + other).wait_send()

    line_spread(1)
    fill(1)

    @pl.when(beyond != z)
    def _():
        leg_two(0).wait()
        leg_two(1).wait()

    for part in range(parts):
        lanes = slice(part * width, (part + 1) * width)
        rows_out[core, owned, part] = sums[chip, part] + cols_here[:, lanes].T

    def spots(turn, flip):
        for part in range(parts):
            number, picks = chosen(part, count_bits - 1 - turn, flip)
            for pick in picks:
                yield number, rows_out.at[core, mixed(pick, z), part]

    beside_copies = [begin(rows_out.at[core, owned], rows_out.at[core, owned], beside)]
    for turn in range(max(line - 1, count_bits)):
        if turn < count_bits:
            made = [begin(spot, spot, across(number)) for number, spot in spots(turn, False)]
        if turn == count_bits:
            fill(64)
        if turn + 2 <= line:
            line_spread(turn + 2)
        if turn < count_bits:
            fill(2)
            for one in made:
                one.wait_recv()
            beside_copies += [begin(spot, spot, beside) for _, spot in spots(turn, True)]
    fill(64)
    for one in beside_copies:
        one.wait_recv()
    line_spread_sent()
    line_sent()
    for one in pending:
        one.wait_send()


def exchange(limits, row_part, col_part, gram_part):
    line, many = lax.axis_size("tr"), lax.axis_size("tc")
    count_bits = line.bit_length() - 1
    row_blocks, size, count_obs = row_part.shape
    parts, width = count_bits, size // count_bits
    seg = count_obs // many
    rows = (2, line, parts, width, count_obs)
    cols = col_part.shape
    gram = (many, seg, count_obs)
    landings = sum(parts * 2 ** (count_bits - 1 - step) for step in range(count_bits))
    part = pivot_size(count_obs)
    cross_rows, cross_cols, inverted = pl.pallas_call(
        functools.partial(exchange_kernel, count_bits, limits),
        out_shape=tuple(jax.ShapeDtypeStruct(shape, f32) for shape in (rows, cols, gram_part.shape)),
        in_specs=[VMEM] * 3,
        out_specs=(VMEM,) * 3,
        scratch_shapes=[
            pltpu.VMEM(gram, f32),
            pltpu.VMEM((part, part), f32),
            pltpu.SemaphoreType.DMA((96,)),
            pltpu.SemaphoreType.DMA((96,)),
            pltpu.VMEM(rows[1:], f32),
            pltpu.VMEM(rows[1:], f32),
            pltpu.VMEM((landings, width, count_obs), f32),
            pltpu.VMEM(cols, f32),
            pltpu.VMEM(cols, f32),
            pltpu.VMEM(rows[2:], f32),
            pltpu.VMEM(cols[1:], f32),
            pltpu.VMEM(cols[1:], f32),
            pltpu.VMEM(cols[1:], f32),
            pltpu.VMEM(gram, f32),
            pltpu.VMEM((many // 2, seg, count_obs), f32),
            pltpu.VMEM((many // 2, seg, count_obs), f32),
            pltpu.VMEM((line, seg, count_obs), f32),
        ],
        compiler_params=pltpu.CompilerParams(has_side_effects=True, vmem_limit_bytes=ROOM),
        name="exchange",
    )(row_part.reshape(rows), col_part, gram_part.reshape(gram))
    return cross_rows.reshape(row_part.shape), cross_cols, inverted


def body(cov_tiles, block_order, stations, obs_values, obs_error):
    size = obs_values.shape[2]
    line, many = lax.axis_size("tr"), lax.axis_size("tc")
    packed = share(stations, obs_values, obs_error)
    row_part, col_part, gram_part, fits = forward(block_order, packed, cov_tiles, size)
    square = many == 2 * line and line & (line - 1) == 0 and line > 1
    whole_tiles = row_part.shape[0] == many and col_part.shape[0] == line
    parts = (row_part, col_part, gram_part)
    if square and whole_tiles:
        count_obs = gram_part.shape[0]
        cross_rows, cross_cols, inverted = lax.cond(
            fits[0] > 0,
            functools.partial(exchange, reach(count_obs, line)),
            functools.partial(exchange, (count_obs,) * line),
            *parts,
        )
    else:
        cross_rows, cross_cols, inverted = exchange_plain(*parts)
    return update(block_order, cross_rows, cross_cols, inverted, cov_tiles)


def solution(mesh):
    in_specs = (P("tr", "tc"), P(), P(None, "tc"), P(None, "tc", None), P(None, "tc"))
    out_specs = P("tr", "tc")
    return jax.shard_map(body, mesh=mesh, in_specs=in_specs, out_specs=out_specs, check_vma=False)
```

```python
import functools

import jax
import jax.numpy as jnp
from jax import lax
from jax.experimental import pallas as pl
from jax.experimental.pallas import tpu as pltpu
from jax.sharding import PartitionSpec as P

exact = lax.Precision.HIGHEST
bf16, f32, i32 = jnp.bfloat16, jnp.float32, jnp.int32
DEPTH = 4
ROOM = 40 * 2**20
ANY = pl.BlockSpec(memory_space=pl.ANY)
VMEM = pl.BlockSpec(memory_space=pltpu.VMEM)
SMEM = pl.BlockSpec(memory_space=pltpu.SMEM)


def product(former, latter, over, precision=exact):
    return lax.dot_general(
        former,
        latter,
        (((over[0],), (over[1],)), ((), ())),
        precision=precision,
        preferred_element_type=jnp.float32,
    )


def halves(array):
    high = array.astype(bf16)
    return high, (array - high.astype(f32)).astype(bf16)


def dot(former, latter):
    return jnp.dot(former, latter, preferred_element_type=f32)


def dot3(former, latter):
    return dot(former[0], latter[0]) + dot(former[0], latter[1]) + dot(former[1], latter[0])


def list_tiles(order_ref, live_ref, row_blocks, col_blocks, when_dead=None):
    row_first = lax.axis_index("tr") * row_blocks
    col_first = lax.axis_index("tc") * col_blocks

    def step(tile, count):
        row, col = tile // col_blocks, tile % col_blocks
        p, q = row_first + row, col_first + col
        live = (order_ref[p] > order_ref[q]) | (p == q)

        @pl.when(live)
        def _():
            live_ref[count] = tile

        if when_dead is not None:

            @pl.when(jnp.logical_not(live))
            def _():
                when_dead(tile)

        return count + live.astype(i32)

    return lax.fori_loop(0, row_blocks * col_blocks, step, jnp.int32(0))


def tile_at(ref, tile, col_blocks, size):
    row, col = tile // col_blocks, tile % col_blocks
    return ref.at[
        pl.ds(pl.multiple_of(row * size, size), size), pl.ds(pl.multiple_of(col * size, size), size)
    ]


def sorted_by_position(packed, size, order_ref):
    count = packed.shape[0]
    codes = packed[:, size:].T[0:1, :].astype(i32)
    places_across = sum(jnp.where(codes == order_ref[place], place, 0) for place in range(order_ref.shape[0]))
    places = jnp.broadcast_to(places_across.astype(f32), (128, count)).T[:, 0:1].astype(i32)
    down = lax.broadcasted_iota(i32, (count, count), 0)
    across = lax.broadcasted_iota(i32, (count, count), 1)
    earlier = (places < places_across) | ((places == places_across) & (down < across))
    rank = jnp.sum(jnp.where(earlier, 1.0, 0.0), axis=0, keepdims=True).astype(i32)
    return product(jnp.where(down == rank, 1.0, 0.0), packed, (1, 0)), places_across


def reach(count, groups):
    return tuple(min(count, (count * (group + 1) // groups + count // 8 + 7) // 8 * 8) for group in range(groups))


def forward_kernel(
    order_ref, packed_ref, cov_ref, rows_ref, cols_ref, gram_ref, fits_ref,
    live_ref, used_rows, used_cols, held, sem, for_rows, for_cols,
):
    row_blocks, size, count_obs = rows_ref.shape
    col_blocks = cols_ref.shape[0]
    windows, span = for_rows.shape[1], for_rows.shape[2] // 2
    row_first = lax.axis_index("tr") * row_blocks
    col_first = lax.axis_index("tc") * col_blocks
    count = list_tiles(order_ref, live_ref, row_blocks, col_blocks)

    def fetch(at):
        slot = at % DEPTH
        return pltpu.make_async_copy(
            tile_at(cov_ref, live_ref[at], col_blocks, size), held.at[slot], sem.at[slot]
        )

    for at in range(DEPTH - 1):

        @pl.when(at < count)
        def _():
            fetch(at).start()

    packed, places = sorted_by_position(packed_ref[...], size, order_ref)
    groups = lax.axis_size("tr")
    limits = reach(count_obs, groups)
    fits = jnp.int32(1)
    for group in range(groups - 1):
        before = jnp.sum(jnp.where(places < (group + 1) * row_blocks, 1, 0))
        fits = fits * ((before <= limits[group]) & (count_obs - before <= limits[groups - 2 - group])).astype(i32)
    fits_ref[0] = fits
    values = packed[:, :size]
    extras = packed[:, size:]
    codes_down = extras[:, 0:1].astype(i32)
    flipped = extras.T
    codes_across = flipped[0:1, :].astype(i32)
    errors_across = flipped[1:2, :]
    values_t = values.T
    for window in range(windows):
        here = slice(window * span, (window + 1) * span)
        for block in range(row_blocks):
            match = codes_down[here] == order_ref[row_first + block]
            high, low = halves(jnp.where(match, values[here], 0.0))
            for_rows[block, window] = jnp.concatenate((high, low), axis=0)
            same = codes_across[:, here] == order_ref[row_first + block]
            used_rows[block * windows + window] = jnp.sum(jnp.where(same, 1, 0))
        for block in range(col_blocks):
            match = codes_across[:, here] == order_ref[col_first + block]
            high, low = halves(jnp.where(match, values_t[:, here], 0.0))
            for_cols[block, window] = jnp.concatenate((high, low), axis=1)
            used_cols[block * windows + window] = jnp.sum(jnp.where(match, 1, 0))
    rows_ref[...] = jnp.zeros_like(rows_ref)
    cols_ref[...] = jnp.zeros_like(cols_ref)
    gram_ref[...] = jnp.zeros_like(gram_ref)

    def times_cols(parts, block, window):
        both = dot(parts[0], for_cols[block, window]) + dot(parts[1], for_cols[block, window])
        return both[:, :span] + both[:, span:]

    def rows_times(parts, block, window):
        both = dot(for_rows[block, window], parts[0])
        return both[:span] + both[span:] + dot(for_rows[block, window, :span], parts[1])

    def step(at, carry):
        tile = live_ref[at]
        row, col = tile // col_blocks, tile % col_blocks
        slot = at % DEPTH

        @pl.when(at + DEPTH - 1 < count)
        def _():
            fetch(at + DEPTH - 1).start()

        fetch(at).wait()
        strict = row_first + row != col_first + col
        for window in range(windows):
            here = slice(window * span, (window + 1) * span)

            @pl.when(used_cols[col * windows + window] > 0)
            def _():
                rows_ref[row, :, here] += times_cols(halves(held[slot]), col, window)

            @pl.when(strict & (used_rows[row * windows + window] > 0))
            def _():
                cols_ref[col, here] += rows_times(halves(held[slot]), row, window)

        return carry

    lax.fori_loop(0, count, step, 0)

    def add_col(block, carry):
        for window in range(windows):
            here = slice(window * span, (window + 1) * span)

            @pl.when(used_cols[block * windows + window] > 0)
            def _():
                gram_ref[:, here] += times_cols(halves(cols_ref[block]), block, window)

        return carry

    lax.fori_loop(0, col_blocks, add_col, 0)
    first = (lax.axis_index("tr") == 0) & (lax.axis_index("tc") == 0)
    across = lax.broadcasted_iota(i32, (count_obs, count_obs), 1)
    down = lax.broadcasted_iota(i32, (count_obs, count_obs), 0)
    gram_ref[...] = gram_ref[...].T + jnp.where((across == down) & first, errors_across, 0.0)

    def add_row(block, carry):
        for window in range(windows):
            here = slice(window * span, (window + 1) * span)

            @pl.when(used_rows[block * windows + window] > 0)
            def _():
                gram_ref[here] += rows_times(halves(rows_ref[block]), block, window)

        return carry

    lax.fori_loop(0, row_blocks, add_row, 0)


def forward(block_order, packed, cov_tiles, size):
    count_obs = packed.shape[0]
    row_blocks, col_blocks = cov_tiles.shape[0] // size, cov_tiles.shape[1] // size
    tiles = row_blocks * col_blocks
    span = pivot_size(count_obs)
    windows = count_obs // span
    return pl.pallas_call(
        forward_kernel,
        out_shape=(
            jax.ShapeDtypeStruct((row_blocks, size, count_obs), f32),
            jax.ShapeDtypeStruct((col_blocks, count_obs, size), f32),
            jax.ShapeDtypeStruct((count_obs, count_obs), f32),
            jax.ShapeDtypeStruct((1,), i32),
        ),
        in_specs=[SMEM, VMEM, ANY],
        out_specs=(VMEM, VMEM, VMEM, SMEM),
        scratch_shapes=[
            pltpu.SMEM((tiles,), i32),
            pltpu.SMEM((row_blocks * windows,), i32),
            pltpu.SMEM((col_blocks * windows,), i32),
            pltpu.VMEM((DEPTH, size, size), f32),
            pltpu.SemaphoreType.DMA((DEPTH,)),
            pltpu.VMEM((row_blocks, windows, 2 * span, size), bf16),
            pltpu.VMEM((col_blocks, windows, size, 2 * span), bf16),
        ],
        cost_estimate=pl.CostEstimate(
            flops=6 * tiles * size * size * count_obs, bytes_accessed=2 * tiles * size * size, transcendentals=0
        ),
        compiler_params=pltpu.CompilerParams(vmem_limit_bytes=ROOM),
        name="forward",
    )(block_order, packed, cov_tiles)


def update_kernel(
    order_ref, rows_ref, cols_ref, inverse_ref, cov_ref, out_ref,
    live_ref, held, made, zeros, weighted, in_sem, out_sem, zero_sem,
):
    row_blocks, size, _ = rows_ref.shape
    col_blocks = cols_ref.shape[0]
    tiles = row_blocks * col_blocks
    zeros[...] = jnp.zeros_like(zeros)

    def blank(tile):
        return pltpu.make_async_copy(zeros, tile_at(out_ref, tile, col_blocks, size), zero_sem.at[tile])

    count = list_tiles(order_ref, live_ref, row_blocks, col_blocks)

    def fetch(at):
        slot = at % DEPTH
        return pltpu.make_async_copy(
            tile_at(cov_ref, live_ref[at], col_blocks, size), held.at[slot], in_sem.at[slot]
        )

    def put(at):
        slot = at % DEPTH
        return pltpu.make_async_copy(
            made.at[slot], tile_at(out_ref, live_ref[at], col_blocks, size), out_sem.at[slot]
        )

    for at in range(DEPTH - 1):

        @pl.when(at < count)
        def _():
            fetch(at).start()

    list_tiles(order_ref, live_ref, row_blocks, col_blocks, lambda tile: blank(tile).start())
    for block in range(col_blocks):
        weighted[block, 0], weighted[block, 1] = halves(product(inverse_ref[...], cols_ref[block], (1, 0)))

    def step(at, carry):
        tile = live_ref[at]
        row, col = tile // col_blocks, tile % col_blocks
        slot = at % DEPTH

        @pl.when(at + DEPTH - 1 < count)
        def _():
            fetch(at + DEPTH - 1).start()

        @pl.when(at >= DEPTH)
        def _():
            put(at - DEPTH).wait()

        fetch(at).wait()
        made[slot] = held[slot] - dot3(halves(rows_ref[row]), (weighted[col, 0], weighted[col, 1]))
        put(at).start()
        return carry

    lax.fori_loop(0, count, step, 0)
    lax.fori_loop(jnp.maximum(count - DEPTH, 0), count, lambda at, carry: (put(at).wait(), carry)[1], 0)
    list_tiles(order_ref, live_ref, row_blocks, col_blocks, lambda tile: blank(tile).wait())


def update(block_order, cross_rows, cross_cols, inverted, cov_tiles):
    row_blocks, size, count_obs = cross_rows.shape
    col_blocks = cross_cols.shape[0]
    tiles = row_blocks * col_blocks
    return pl.pallas_call(
        update_kernel,
        out_shape=jax.ShapeDtypeStruct(cov_tiles.shape, f32),
        in_specs=[SMEM, VMEM, VMEM, VMEM, ANY],
        out_specs=ANY,
        scratch_shapes=[
            pltpu.SMEM((tiles,), i32),
            pltpu.VMEM((DEPTH, size, size), f32),
            pltpu.VMEM((DEPTH, size, size), f32),
            pltpu.VMEM((size, size), f32),
            pltpu.VMEM((col_blocks, 2, count_obs, size), bf16),
            pltpu.SemaphoreType.DMA((DEPTH,)),
            pltpu.SemaphoreType.DMA((DEPTH,)),
            pltpu.SemaphoreType.DMA((tiles,)),
        ],
        cost_estimate=pl.CostEstimate(
            flops=3 * tiles * size * size * count_obs, bytes_accessed=6 * tiles * size * size, transcendentals=0
        ),
        compiler_params=pltpu.CompilerParams(vmem_limit_bytes=ROOM),
        name="update",
    )(block_order, cross_rows, cross_cols, inverted, cov_tiles)


def swept(matrix, work):
    size = matrix.shape[0]
    work[...] = matrix
    lanes = lax.broadcasted_iota(jnp.int32, (1, size), 1)
    rows = lax.broadcasted_iota(jnp.int32, (size, 1), 0)

    def step(pivot, carry):
        held = work[...]
        row = work[pl.ds(pivot, 1), :]
        at_lane = lanes == pivot
        at_row = rows == pivot
        column = jnp.sum(jnp.where(at_lane, held, 0.0), axis=1, keepdims=True)
        share = 1.0 / jnp.sum(jnp.where(at_lane, row, 0.0), axis=1, keepdims=True)
        kept = jnp.where(at_lane | at_row, 0.0, held)
        left = jnp.where(at_row, -1.0, column)
        right = jnp.where(at_lane, -1.0, row)
        work[...] = kept - left * (right * share)
        return carry

    quarter = size // 4
    for turn in range(4):
        lax.fori_loop(turn * quarter, (turn + 1) * quarter, step, 0)
        yield
    return -work[...]


def inverse_of(matrix, work):
    size = matrix.shape[0]
    if size <= 128:
        return (yield from swept(matrix, work))
    half = size // 2
    upper, corner, lower = matrix[:half, :half], matrix[half:, :half], matrix[half:, half:]
    upper_inverse = yield from inverse_of(upper, work)
    weight = product(corner, upper_inverse, (1, 0))
    lower_inverse = yield from inverse_of(lower - product(weight, corner, (1, 1)), work)
    below = -product(lower_inverse, weight, (1, 0))
    above = upper_inverse - product(weight, below, (0, 0))
    return jnp.concatenate(
        (jnp.concatenate((above, below.T), axis=1), jnp.concatenate((below, lower_inverse), axis=1)), axis=0
    )


def inverse_steps(matrix_ref, inverse_ref, work):
    size = matrix_ref.shape[-1]
    inverse_ref[...] = yield from inverse_of(matrix_ref[...].reshape(size, size), work)


def inverse_kernel(matrix_ref, inverse_ref, work):
    for _ in inverse_steps(matrix_ref, inverse_ref, work):
        pass


def pivot_size(size):
    return size if size <= 128 else pivot_size(size // 2)


def inverse(matrix):
    size = matrix.shape[0]
    part = pivot_size(size)
    return pl.pallas_call(
        inverse_kernel,
        out_shape=jax.ShapeDtypeStruct(matrix.shape, jnp.float32),
        in_specs=[VMEM],
        out_specs=VMEM,
        scratch_shapes=[pltpu.VMEM((part, part), jnp.float32)],
        cost_estimate=pl.CostEstimate(flops=400_000_000, bytes_accessed=8 * size * size, transcendentals=0),
        name="inverse",
    )(matrix)


def exchange_plain(row_part, col_part, gram_part):
    tr_size, tc_size = lax.axis_size("tr"), lax.axis_size("tc")
    row_blocks, size, count_obs = row_part.shape
    col_blocks = col_part.shape[0]
    row_part = row_part.reshape(row_blocks * size, count_obs)
    col_part = col_part.transpose(0, 2, 1).reshape(col_blocks * size, count_obs)
    innovation = lax.psum(gram_part, ("tr", "tc"))
    count = tr_size * tc_size
    to_rows = [((q % tr_size) * tc_size + q // tr_size, q) for q in range(count)]
    to_cols = [(there, here) for here, there in to_rows]
    col_chunk = lax.psum_scatter(col_part, "tr", scatter_dimension=0, tiled=True)
    row_chunk = lax.psum_scatter(row_part, "tc", scatter_dimension=0, tiled=True)
    chunk = row_chunk + lax.ppermute(col_chunk, ("tr", "tc"), to_rows)
    cross_rows = lax.all_gather(chunk, "tc", axis=0, tiled=True)
    cross_cols = lax.all_gather(lax.ppermute(chunk, ("tr", "tc"), to_cols), "tr", axis=0, tiled=True)
    return (
        cross_rows.reshape(row_blocks, size, count_obs),
        cross_cols.reshape(col_blocks, size, count_obs).transpose(0, 2, 1),
        inverse(innovation),
    )


class Sems:
    def __init__(self):
        self.count = 0

    def take(self, number=1):
        self.count += number
        return self.count - number


def share_kernel(stations_ref, values_ref, errors_ref, all_ref, mine_ref, send, recv, core_send, core_recv):
    row, col = lax.axis_index("tr"), lax.axis_index("tc")
    chips = all_ref.shape[0] // 2
    chip, core = col // 2, col % 2

    def copy(source, block, step):
        return pltpu.make_async_remote_copy(
            source, all_ref.at[block], send.at[step], recv.at[step],
            device_id=(row, 2 * lax.rem(chip + step, chips) + core), device_id_type=pl.DeviceIdType.MESH,
        )

    def beside(source, block, step):
        return pltpu.make_async_remote_copy(
            source, all_ref.at[block], core_send.at[step], core_recv.at[step],
            device_id=(row, 2 * chip + 1 - core), device_id_type=pl.DeviceIdType.MESH,
        )

    number, size = values_ref.shape[1:]
    equal = lax.broadcasted_iota(i32, (number, number), 0) == lax.broadcasted_iota(i32, (number, number), 1)

    def upright(across):
        return jnp.sum(jnp.where(equal, across, 0.0), axis=1, keepdims=True)

    lanes = lax.broadcasted_iota(i32, (number, mine_ref.shape[1] - size), 1)
    stations, errors = upright(stations_ref[...].astype(f32)), upright(errors_ref[...])
    mine_ref[:, :size] = values_ref[0]
    mine_ref[:, size:] = jnp.where(lanes == 0, stations, jnp.where(lanes == 1, errors, 0.0))
    sent = [copy(mine_ref, col, step) for step in range(1, chips)]
    sent.append(beside(mine_ref, col, 0))
    for one in sent:
        one.start()
    all_ref[col] = mine_ref[...]
    for step in range(1, chips):
        block = 2 * lax.rem(chip + chips - step, chips) + core
        copy(mine_ref, block, step).wait_recv()
        sent.append(beside(all_ref.at[block], block, step))
        sent[-1].start()
    for step in range(chips):
        beside(mine_ref, 2 * lax.rem(chip + chips - step, chips) + 1 - core, step).wait_recv()
    for one in sent:
        one.wait_send()


def share(stations, obs_values, obs_error):
    many = lax.axis_size("tc")
    _, number, size = obs_values.shape
    packed = (number, size + 128)
    full = pl.pallas_call(
        share_kernel,
        out_shape=jax.ShapeDtypeStruct((many, *packed), f32),
        in_specs=[VMEM] * 3,
        out_specs=VMEM,
        scratch_shapes=[pltpu.VMEM(packed, f32)] + [pltpu.SemaphoreType.DMA((many // 2,))] * 4,
        compiler_params=pltpu.CompilerParams(has_side_effects=True, vmem_limit_bytes=8 * 2**20),
        name="share",
    )(stations, obs_values, obs_error)
    return full.reshape(many * number, size + 128)


def exchange_kernel(
    count_bits, limits, row_ref, col_ref, gram_ref, rows_out, cols_out, inverse_out,
    gram_out, work, send, recv, from_core, sums, landed, upward, downward, rows_here, cols_here, total, relay,
    gram_work, gram_core, gram_bits, gram_line,
):
    sems = Sems()
    line = lax.axis_size("tr")
    z, j = lax.axis_index("tr"), lax.axis_index("tc")
    chip, core = j // 2, j % 2
    parts = count_bits
    width = rows_here.shape[1]
    pending = []
    beside = (z, 2 * chip + 1 - core)

    def copy(source, target, sem, device=beside):
        return pltpu.make_async_remote_copy(
            source, target, send.at[sem], recv.at[sem], device_id=device, device_id_type=pl.DeviceIdType.MESH
        )

    def begin(source, target, device):
        made = copy(source, target, sems.take(), device)
        made.start()
        pending.append(made)
        return made

    def bit(number):
        return chip // 2**number % 2

    def across(number):
        return z, 2 * (chip + (1 - 2 * bit(number)) * 2**number) + core

    def mixed(value, plane):
        return sum(
            (value // 2**number + plane // 2 ** (count_bits - 1 - number)) % 2 * 2**number
            for number in range(count_bits)
        )

    def plane_of(value, chunk):
        return sum(
            (value // 2**number + chunk // 2**number) % 2 * 2 ** (count_bits - 1 - number)
            for number in range(count_bits)
        )

    up, down = sems.take(line), sems.take(line)

    many_obs = total.shape[0]

    def up_rows(place):
        return pl.ds(0, limits[place])

    def down_rows(place):
        return pl.ds(many_obs - limits[line - 1 - place], limits[line - 1 - place])

    def up_copy(place, chunk, source):
        rows = up_rows(place)
        return copy(source.at[chunk, rows], upward.at[chunk, rows], up + chunk, (z + 1, j))

    def down_copy(place, chunk, source):
        rows = down_rows(place)
        return copy(source.at[chunk, rows], downward.at[chunk, rows], down + chunk, (z - 1, j))

    def line_begin(step):
        @pl.when(z == 0)
        def _():
            up_copy(0, line - step, col_ref).start()

        @pl.when(z == line - 1)
        def _():
            down_copy(line - 1, step - 1, col_ref).start()

    def line_round(step):
        for place in range(1, line - 1):
            chunk, other = place + line - 1 - step, place - line + 1 + step

            @pl.when(z == place)
            def _():
                if chunk < line:
                    fresh = limits[place] - limits[place - 1]
                    up_copy(place - 1, chunk, upward).wait_recv()
                    upward[chunk, up_rows(place - 1)] += col_ref[chunk, up_rows(place - 1)]
                    if fresh:
                        later = pl.ds(limits[place - 1], fresh)
                        upward[chunk, later] = col_ref[chunk, later]
                    up_copy(place, chunk, upward).start()
                if other >= 0:
                    fresh = limits[line - 1 - place] - limits[line - 2 - place]
                    down_copy(place + 1, other, downward).wait_recv()
                    downward[other, down_rows(place + 1)] += col_ref[other, down_rows(place + 1)]
                    if fresh:
                        later = pl.ds(many_obs - limits[line - 1 - place], fresh)
                        downward[other, later] = col_ref[other, later]
                    down_copy(place, other, downward).start()

    def line_end():
        total[...] = col_ref[z]
        for place in range(line):

            @pl.when(z == place)
            def _():
                if place > 0:
                    up_copy(place - 1, place, upward).wait_recv()
                    total[up_rows(place - 1)] += upward[place, up_rows(place - 1)]
                if place < line - 1:
                    down_copy(place + 1, place, downward).wait_recv()
                    total[down_rows(place + 1)] += downward[place, down_rows(place + 1)]

    def line_sent():
        for place in range(line):

            @pl.when(z == place)
            def _():
                for chunk in range(place + 1, line):
                    up_copy(place, chunk, upward).wait_send()
                for other in range(place):
                    down_copy(place, other, downward).wait_send()

    def chosen(part, step, flip):
        order = [(part + turn) % count_bits for turn in range(count_bits)]
        free = order[step + 1:]
        picks = []
        for pick in range(2 ** len(free)):
            where = 0
            for turn, number in enumerate(order):
                if number in free:
                    value = pick // 2 ** free.index(number) % 2
                elif turn == step and flip:
                    value = 1 - bit(number)
                else:
                    value = bit(number)
                where = where + value * 2**number
            picks.append(where)
        return order[step], picks

    step_base = [0]
    for step in range(count_bits):
        step_base.append(step_base[-1] + parts * 2 ** (count_bits - 1 - step))

    def plane_send(step):
        made = []
        for part in range(parts):
            number, picks = chosen(part, step, True)
            for slot, pick in enumerate(picks):
                at = step_base[step] + part * len(picks) + slot
                made.append(begin(sums.at[pick, part], landed.at[at], across(number)))
        return made

    def plane_add(step, made):
        for one in made:
            one.wait_recv()
        for part in range(parts):
            _, picks = chosen(part, step, False)
            for slot, pick in enumerate(picks):
                sums[pick, part] += landed[step_base[step] + part * len(picks) + slot]

    for step in range(1, line):
        line_begin(step)
    held = 2**count_bits
    half = begin(gram_ref.at[pl.ds((1 - core) * held, held)], gram_core, beside)
    core_sum = begin(row_ref.at[1 - core], from_core, beside)
    half.wait_recv()
    gram_work[pl.ds(core * held, held)] = gram_ref[pl.ds(core * held, held)] + gram_core[...]
    for number in reversed(range(count_bits)):
        size = 2**number
        start = core * held + chip // (2 * size) * (2 * size)
        keep, give = start + bit(number) * size, start + (1 - bit(number)) * size
        begin(gram_work.at[pl.ds(give, size)], gram_bits.at[pl.ds(size, size)], across(number)).wait_recv()
        gram_work[pl.ds(keep, size)] += gram_bits[pl.ds(size, size)]
    mine = core * held + chip
    gram_line[z] = gram_work[mine]
    base = sems.take(line)
    for step in range(1, line):
        copy(gram_work.at[mine], gram_line.at[z], base + step, (lax.rem(z + step, line), j)).start()
    core_sum.wait_recv()
    for owner in range(line):
        chunk = mixed(owner, z)
        sums[owner] = row_ref[core, chunk] + from_core[chunk]
    made = plane_send(0)

    def gram_back():
        for step in range(1, line):
            copy(gram_work.at[mine], gram_line.at[lax.rem(z + line - step, line)], base + step).wait()
        gram_out[mine] = sum(gram_line[step] for step in range(line))
        for number in range(count_bits):
            size = 2**number
            spot = gram_out.at[pl.ds(core * held + chip // size * size, size)]
            sent = begin(spot, spot, across(number))
            yield
            sent.wait_recv()
        spot = gram_out.at[pl.ds(core * held, held)]
        sent = begin(spot, spot, beside)
        yield
        sent.wait_recv()

    to_cols, first_leg, second_leg = sems.take(), sems.take(2), sems.take(2)
    owned = mixed(chip, z)
    apart = (owned != z) | (z != chip)
    column = (owned, 2 * z + core)
    via = mixed(z, chip)
    beyond = plane_of(chip, z)

    def piece(ref, number):
        size = total.shape[0] // 2
        return ref.at[pl.ds(number * size, size)]

    def leg_one(number):
        return copy(piece(total, number), piece(relay, number), first_leg + number, (z, 2 * via + core))

    def leg_two(number):
        return copy(piece(relay, number), piece(cols_here, number), second_leg + number, (beyond, j))

    gram_turns = gram_back()
    for step in range(1, line - 1):
        line_round(step)
        next(gram_turns, None)
        if step < count_bits:
            plane_add(step - 1, made)
            made = plane_send(step)
            next(gram_turns, None)
    for step in range(max(line - 1, 1), count_bits):
        plane_add(step - 1, made)
        made = plane_send(step)
    line_end()

    @pl.when(via != chip)
    def _():
        leg_one(0).start()
        leg_one(1).start()

    @pl.when(via == chip)
    def _():
        relay[...] = total[...]

    for _ in gram_turns:
        pass
    plane_add(count_bits - 1, made)
    inverse_turns = inverse_steps(gram_out, inverse_out, work)

    def fill(number):
        for _ in range(number):
            next(inverse_turns, None)

    @pl.when(apart)
    def _():
        copy(sums.at[chip], rows_here, to_cols, column).start()

    @pl.when(jnp.logical_not(apart))
    def _():
        rows_here[...] = sums[chip]

    for number in range(2):

        @pl.when(via != chip)
        def _():
            leg_one(number).wait()

        @pl.when(beyond != z)
        def _():
            leg_two(number).start()

    @pl.when(beyond == z)
    def _():
        cols_here[...] = relay[...]

    fill(1)

    @pl.when(apart)
    def _():
        copy(sums.at[chip], rows_here, to_cols, column).wait()

    for part in range(parts):
        lanes = slice(part * width, (part + 1) * width)
        cols_out[z, :, lanes] = total[:, lanes] + rows_here[part].T
    around, back = sems.take(line), sems.take(line)

    def line_spread(step):
        chunk, other = z - (step - 1), z + (step - 1)

        @pl.when(chunk >= 0)
        def _():
            if step > 1:
                copy(cols_out.at[chunk], cols_out.at[chunk], around + chunk).wait_recv()

            @pl.when(z < line - 1)
            def _():
                copy(cols_out.at[chunk], cols_out.at[chunk], around + chunk, (z + 1, j)).start()

        @pl.when(other < line)
        def _():
            if step > 1:
                copy(cols_out.at[other], cols_out.at[other], back + other).wait_recv()

            @pl.when(z > 0)
            def _():
                copy(cols_out.at[other], cols_out.at[other], back + other, (z - 1, j)).start()

    def line_spread_sent():
        for step in range(1, line + 1):
            chunk, other = z - (step - 1), z + (step - 1)

            @pl.when((chunk >= 0) & (z < line - 1))
            def _():
                copy(cols_out.at[chunk], cols_out.at[chunk], around + chunk).wait_send()

            @pl.when((other < line) & (z > 0))
            def _():
                copy(cols_out.at[other], cols_out.at[other], back + other).wait_send()

    line_spread(1)
    fill(2)

    @pl.when(beyond != z)
    def _():
        leg_two(0).wait()
        leg_two(1).wait()

    for part in range(parts):
        lanes = slice(part * width, (part + 1) * width)
        rows_out[core, owned, part] = sums[chip, part] + cols_here[:, lanes].T

    def spots(turn, flip):
        for part in range(parts):
            number, picks = chosen(part, count_bits - 1 - turn, flip)
            for pick in picks:
                yield number, rows_out.at[core, mixed(pick, z), part]

    beside_copies = [begin(rows_out.at[core, owned], rows_out.at[core, owned], beside)]
    for turn in range(max(line - 1, count_bits)):
        if turn < count_bits:
            made = [begin(spot, spot, across(number)) for number, spot in spots(turn, False)]
        if turn == count_bits:
            fill(64)
        if turn + 2 <= line:
            line_spread(turn + 2)
        if turn < count_bits:
            fill(2)
            for one in made:
                one.wait_recv()
            beside_copies += [begin(spot, spot, beside) for _, spot in spots(turn, True)]
    fill(64)
    for one in beside_copies:
        one.wait_recv()
    line_spread_sent()
    line_sent()
    for one in pending:
        one.wait_send()


def exchange(limits, row_part, col_part, gram_part):
    line, many = lax.axis_size("tr"), lax.axis_size("tc")
    count_bits = line.bit_length() - 1
    row_blocks, size, count_obs = row_part.shape
    parts, width = count_bits, size // count_bits
    seg = count_obs // many
    rows = (2, line, parts, width, count_obs)
    cols = col_part.shape
    gram = (many, seg, count_obs)
    landings = sum(parts * 2 ** (count_bits - 1 - step) for step in range(count_bits))
    part = pivot_size(count_obs)
    cross_rows, cross_cols, inverted = pl.pallas_call(
        functools.partial(exchange_kernel, count_bits, limits),
        out_shape=tuple(jax.ShapeDtypeStruct(shape, f32) for shape in (rows, cols, gram_part.shape)),
        in_specs=[VMEM] * 3,
        out_specs=(VMEM,) * 3,
        scratch_shapes=[
            pltpu.VMEM(gram, f32),
            pltpu.VMEM((part, part), f32),
            pltpu.SemaphoreType.DMA((96,)),
            pltpu.SemaphoreType.DMA((96,)),
            pltpu.VMEM(rows[1:], f32),
            pltpu.VMEM(rows[1:], f32),
            pltpu.VMEM((landings, width, count_obs), f32),
            pltpu.VMEM(cols, f32),
            pltpu.VMEM(cols, f32),
            pltpu.VMEM(rows[2:], f32),
            pltpu.VMEM(cols[1:], f32),
            pltpu.VMEM(cols[1:], f32),
            pltpu.VMEM(cols[1:], f32),
            pltpu.VMEM(gram, f32),
            pltpu.VMEM((many // 2, seg, count_obs), f32),
            pltpu.VMEM((many // 2, seg, count_obs), f32),
            pltpu.VMEM((line, seg, count_obs), f32),
        ],
        compiler_params=pltpu.CompilerParams(has_side_effects=True, vmem_limit_bytes=ROOM),
        name="exchange",
    )(row_part.reshape(rows), col_part, gram_part.reshape(gram))
    return cross_rows.reshape(row_part.shape), cross_cols, inverted


def body(cov_tiles, block_order, stations, obs_values, obs_error):
    size = obs_values.shape[2]
    line, many = lax.axis_size("tr"), lax.axis_size("tc")
    packed = share(stations, obs_values, obs_error)
    row_part, col_part, gram_part, fits = forward(block_order, packed, cov_tiles, size)
    square = many == 2 * line and line & (line - 1) == 0 and line > 1
    whole_tiles = row_part.shape[0] == many and col_part.shape[0] == line
    parts = (row_part, col_part, gram_part)
    if square and whole_tiles:
        count_obs = gram_part.shape[0]
        cross_rows, cross_cols, inverted = lax.cond(
            fits[0] > 0,
            functools.partial(exchange, reach(count_obs, line)),
            functools.partial(exchange, (count_obs,) * line),
            *parts,
        )
    else:
        cross_rows, cross_cols, inverted = exchange_plain(*parts)
    return update(block_order, cross_rows, cross_cols, inverted, cov_tiles)


def solution(mesh):
    in_specs = (P("tr", "tc"), P(), P(None, "tc"), P(None, "tc", None), P(None, "tc"))
    out_specs = P("tr", "tc")
    return jax.shard_map(body, mesh=mesh, in_specs=in_specs, out_specs=out_specs, check_vma=False)
```

```python
import functools

import jax
import jax.numpy as jnp
from jax import lax
from jax.experimental import pallas as pl
from jax.experimental.pallas import tpu as pltpu
from jax.sharding import PartitionSpec as P

exact = lax.Precision.HIGHEST
bf16, f32, i32 = jnp.bfloat16, jnp.float32, jnp.int32
DEPTH = 4
ROOM = 40 * 2**20
ANY = pl.BlockSpec(memory_space=pl.ANY)
VMEM = pl.BlockSpec(memory_space=pltpu.VMEM)
SMEM = pl.BlockSpec(memory_space=pltpu.SMEM)


def product(former, latter, over, precision=exact):
    return lax.dot_general(
        former,
        latter,
        (((over[0],), (over[1],)), ((), ())),
        precision=precision,
        preferred_element_type=jnp.float32,
    )


def halves(array):
    high = array.astype(bf16)
    return high, (array - high.astype(f32)).astype(bf16)


def dot(former, latter):
    return jnp.dot(former, latter, preferred_element_type=f32)


def dot3(former, latter):
    return dot(former[0], latter[0]) + dot(former[0], latter[1]) + dot(former[1], latter[0])


def list_tiles(order_ref, live_ref, row_blocks, col_blocks, when_dead=None):
    row_first = lax.axis_index("tr") * row_blocks
    col_first = lax.axis_index("tc") * col_blocks

    def step(tile, count):
        row, col = tile // col_blocks, tile % col_blocks
        p, q = row_first + row, col_first + col
        live = (order_ref[p] > order_ref[q]) | (p == q)

        @pl.when(live)
        def _():
            live_ref[count] = tile

        if when_dead is not None:

            @pl.when(jnp.logical_not(live))
            def _():
                when_dead(tile)

        return count + live.astype(i32)

    return lax.fori_loop(0, row_blocks * col_blocks, step, jnp.int32(0))


def tile_at(ref, tile, col_blocks, size):
    row, col = tile // col_blocks, tile % col_blocks
    return ref.at[
        pl.ds(pl.multiple_of(row * size, size), size), pl.ds(pl.multiple_of(col * size, size), size)
    ]


def sorted_by_position(packed, size, order_ref):
    count = packed.shape[0]
    codes = packed[:, size:].T[0:1, :].astype(i32)
    places_across = sum(jnp.where(codes == order_ref[place], place, 0) for place in range(order_ref.shape[0]))
    places = jnp.broadcast_to(places_across.astype(f32), (128, count)).T[:, 0:1].astype(i32)
    down = lax.broadcasted_iota(i32, (count, count), 0)
    across = lax.broadcasted_iota(i32, (count, count), 1)
    earlier = (places < places_across) | ((places == places_across) & (down < across))
    rank = jnp.sum(jnp.where(earlier, 1.0, 0.0), axis=0, keepdims=True).astype(i32)
    return product(jnp.where(down == rank, 1.0, 0.0), packed, (1, 0)), places_across


def reach(count, groups):
    return tuple(min(count, (count * (group + 1) // groups + count // 8 + 7) // 8 * 8) for group in range(groups))


def forward_kernel(
    order_ref, packed_ref, cov_ref, rows_ref, cols_ref, gram_ref, fits_ref,
    live_ref, used_rows, used_cols, held, sem, for_rows, for_cols,
):
    row_blocks, size, count_obs = rows_ref.shape
    col_blocks = cols_ref.shape[0]
    windows, span = for_rows.shape[1], for_rows.shape[2] // 2
    row_first = lax.axis_index("tr") * row_blocks
    col_first = lax.axis_index("tc") * col_blocks
    count = list_tiles(order_ref, live_ref, row_blocks, col_blocks)

    def fetch(at):
        slot = at % DEPTH
        return pltpu.make_async_copy(
            tile_at(cov_ref, live_ref[at], col_blocks, size), held.at[slot], sem.at[slot]
        )

    for at in range(DEPTH - 1):

        @pl.when(at < count)
        def _():
            fetch(at).start()

    packed, places = sorted_by_position(packed_ref[...], size, order_ref)
    groups = lax.axis_size("tr")
    limits = reach(count_obs, groups)
    fits = jnp.int32(1)
    for group in range(groups - 1):
        before = jnp.sum(jnp.where(places < (group + 1) * row_blocks, 1, 0))
        fits = fits * ((before <= limits[group]) & (count_obs - before <= limits[groups - 2 - group])).astype(i32)
    fits_ref[0] = fits
    values = packed[:, :size]
    extras = packed[:, size:]
    codes_down = extras[:, 0:1].astype(i32)
    flipped = extras.T
    codes_across = flipped[0:1, :].astype(i32)
    errors_across = flipped[1:2, :]
    values_t = values.T
    for window in range(windows):
        here = slice(window * span, (window + 1) * span)
        for block in range(row_blocks):
            match = codes_down[here] == order_ref[row_first + block]
            high, low = halves(jnp.where(match, values[here], 0.0))
            for_rows[block, window] = jnp.concatenate((high, low), axis=0)
            same = codes_across[:, here] == order_ref[row_first + block]
            used_rows[block * windows + window] = jnp.sum(jnp.where(same, 1, 0))
        for block in range(col_blocks):
            match = codes_across[:, here] == order_ref[col_first + block]
            high, low = halves(jnp.where(match, values_t[:, here], 0.0))
            for_cols[block, window] = jnp.concatenate((high, low), axis=1)
            used_cols[block * windows + window] = jnp.sum(jnp.where(match, 1, 0))
    rows_ref[...] = jnp.zeros_like(rows_ref)
    cols_ref[...] = jnp.zeros_like(cols_ref)
    gram_ref[...] = jnp.zeros_like(gram_ref)

    def times_cols(parts, block, window):
        both = dot(parts[0], for_cols[block, window]) + dot(parts[1], for_cols[block, window])
        return both[:, :span] + both[:, span:]

    def rows_times(parts, block, window):
        both = dot(for_rows[block, window], parts[0])
        return both[:span] + both[span:] + dot(for_rows[block, window, :span], parts[1])

    def step(at, carry):
        tile = live_ref[at]
        row, col = tile // col_blocks, tile % col_blocks
        slot = at % DEPTH

        @pl.when(at + DEPTH - 1 < count)
        def _():
            fetch(at + DEPTH - 1).start()

        fetch(at).wait()
        strict = row_first + row != col_first + col
        for window in range(windows):
            here = slice(window * span, (window + 1) * span)

            @pl.when(used_cols[col * windows + window] > 0)
            def _():
                rows_ref[row, :, here] += times_cols(halves(held[slot]), col, window)

            @pl.when(strict & (used_rows[row * windows + window] > 0))
            def _():
                cols_ref[col, here] += rows_times(halves(held[slot]), row, window)

        return carry

    lax.fori_loop(0, count, step, 0)

    def add_col(block, carry):
        for window in range(windows):
            here = slice(window * span, (window + 1) * span)

            @pl.when(used_cols[block * windows + window] > 0)
            def _():
                gram_ref[:, here] += times_cols(halves(cols_ref[block]), block, window)

        return carry

    lax.fori_loop(0, col_blocks, add_col, 0)
    first = (lax.axis_index("tr") == 0) & (lax.axis_index("tc") == 0)
    across = lax.broadcasted_iota(i32, (count_obs, count_obs), 1)
    down = lax.broadcasted_iota(i32, (count_obs, count_obs), 0)
    gram_ref[...] = gram_ref[...].T + jnp.where((across == down) & first, errors_across, 0.0)

    def add_row(block, carry):
        for window in range(windows):
            here = slice(window * span, (window + 1) * span)

            @pl.when(used_rows[block * windows + window] > 0)
            def _():
                gram_ref[here] += rows_times(halves(rows_ref[block]), block, window)

        return carry

    lax.fori_loop(0, row_blocks, add_row, 0)


def forward(block_order, packed, cov_tiles, size):
    count_obs = packed.shape[0]
    row_blocks, col_blocks = cov_tiles.shape[0] // size, cov_tiles.shape[1] // size
    tiles = row_blocks * col_blocks
    span = pivot_size(count_obs)
    windows = count_obs // span
    return pl.pallas_call(
        forward_kernel,
        out_shape=(
            jax.ShapeDtypeStruct((row_blocks, size, count_obs), f32),
            jax.ShapeDtypeStruct((col_blocks, count_obs, size), f32),
            jax.ShapeDtypeStruct((count_obs, count_obs), f32),
            jax.ShapeDtypeStruct((1,), i32),
        ),
        in_specs=[SMEM, VMEM, ANY],
        out_specs=(VMEM, VMEM, VMEM, SMEM),
        scratch_shapes=[
            pltpu.SMEM((tiles,), i32),
            pltpu.SMEM((row_blocks * windows,), i32),
            pltpu.SMEM((col_blocks * windows,), i32),
            pltpu.VMEM((DEPTH, size, size), f32),
            pltpu.SemaphoreType.DMA((DEPTH,)),
            pltpu.VMEM((row_blocks, windows, 2 * span, size), bf16),
            pltpu.VMEM((col_blocks, windows, size, 2 * span), bf16),
        ],
        cost_estimate=pl.CostEstimate(
            flops=6 * tiles * size * size * count_obs, bytes_accessed=2 * tiles * size * size, transcendentals=0
        ),
        compiler_params=pltpu.CompilerParams(vmem_limit_bytes=ROOM),
        name="forward",
    )(block_order, packed, cov_tiles)


def update_kernel(
    order_ref, rows_ref, cols_ref, inverse_ref, cov_ref, out_ref,
    live_ref, held, made, zeros, weighted, in_sem, out_sem, zero_sem,
):
    row_blocks, size, _ = rows_ref.shape
    col_blocks = cols_ref.shape[0]
    tiles = row_blocks * col_blocks
    zeros[...] = jnp.zeros_like(zeros)

    def blank(tile):
        return pltpu.make_async_copy(zeros, tile_at(out_ref, tile, col_blocks, size), zero_sem.at[tile])

    count = list_tiles(order_ref, live_ref, row_blocks, col_blocks)

    def fetch(at):
        slot = at % DEPTH
        return pltpu.make_async_copy(
            tile_at(cov_ref, live_ref[at], col_blocks, size), held.at[slot], in_sem.at[slot]
        )

    def put(at):
        slot = at % DEPTH
        return pltpu.make_async_copy(
            made.at[slot], tile_at(out_ref, live_ref[at], col_blocks, size), out_sem.at[slot]
        )

    for at in range(DEPTH - 1):

        @pl.when(at < count)
        def _():
            fetch(at).start()

    list_tiles(order_ref, live_ref, row_blocks, col_blocks, lambda tile: blank(tile).start())
    for block in range(col_blocks):
        weighted[block, 0], weighted[block, 1] = halves(product(inverse_ref[...], cols_ref[block], (1, 0)))

    def step(at, carry):
        tile = live_ref[at]
        row, col = tile // col_blocks, tile % col_blocks
        slot = at % DEPTH

        @pl.when(at + DEPTH - 1 < count)
        def _():
            fetch(at + DEPTH - 1).start()

        @pl.when(at >= DEPTH)
        def _():
            put(at - DEPTH).wait()

        fetch(at).wait()
        made[slot] = held[slot] - dot3(halves(rows_ref[row]), (weighted[col, 0], weighted[col, 1]))
        put(at).start()
        return carry

    lax.fori_loop(0, count, step, 0)
    lax.fori_loop(jnp.maximum(count - DEPTH, 0), count, lambda at, carry: (put(at).wait(), carry)[1], 0)
    list_tiles(order_ref, live_ref, row_blocks, col_blocks, lambda tile: blank(tile).wait())


def update(block_order, cross_rows, cross_cols, inverted, cov_tiles):
    row_blocks, size, count_obs = cross_rows.shape
    col_blocks = cross_cols.shape[0]
    tiles = row_blocks * col_blocks
    return pl.pallas_call(
        update_kernel,
        out_shape=jax.ShapeDtypeStruct(cov_tiles.shape, f32),
        in_specs=[SMEM, VMEM, VMEM, VMEM, ANY],
        out_specs=ANY,
        scratch_shapes=[
            pltpu.SMEM((tiles,), i32),
            pltpu.VMEM((DEPTH, size, size), f32),
            pltpu.VMEM((DEPTH, size, size), f32),
            pltpu.VMEM((size, size), f32),
            pltpu.VMEM((col_blocks, 2, count_obs, size), bf16),
            pltpu.SemaphoreType.DMA((DEPTH,)),
            pltpu.SemaphoreType.DMA((DEPTH,)),
            pltpu.SemaphoreType.DMA((tiles,)),
        ],
        cost_estimate=pl.CostEstimate(
            flops=3 * tiles * size * size * count_obs, bytes_accessed=6 * tiles * size * size, transcendentals=0
        ),
        compiler_params=pltpu.CompilerParams(vmem_limit_bytes=ROOM),
        name="update",
    )(block_order, cross_rows, cross_cols, inverted, cov_tiles)


def swept(matrix, work):
    size = matrix.shape[0]
    work[...] = matrix
    lanes = lax.broadcasted_iota(jnp.int32, (1, size), 1)
    rows = lax.broadcasted_iota(jnp.int32, (size, 1), 0)

    def step(pivot, carry):
        held = work[...]
        row = work[pl.ds(pivot, 1), :]
        at_lane = lanes == pivot
        at_row = rows == pivot
        column = jnp.sum(jnp.where(at_lane, held, 0.0), axis=1, keepdims=True)
        share = 1.0 / jnp.sum(jnp.where(at_lane, row, 0.0), axis=1, keepdims=True)
        kept = jnp.where(at_lane | at_row, 0.0, held)
        left = jnp.where(at_row, -1.0, column)
        right = jnp.where(at_lane, -1.0, row)
        work[...] = kept - left * (right * share)
        return carry

    quarter = size // 4
    for turn in range(4):
        lax.fori_loop(turn * quarter, (turn + 1) * quarter, step, 0)
        yield
    return -work[...]


def inverse_of(matrix, work):
    size = matrix.shape[0]
    if size <= 128:
        return (yield from swept(matrix, work))
    half = size // 2
    upper, corner, lower = matrix[:half, :half], matrix[half:, :half], matrix[half:, half:]
    upper_inverse = yield from inverse_of(upper, work)
    weight = product(corner, upper_inverse, (1, 0))
    lower_inverse = yield from inverse_of(lower - product(weight, corner, (1, 1)), work)
    below = -product(lower_inverse, weight, (1, 0))
    above = upper_inverse - product(weight, below, (0, 0))
    return jnp.concatenate(
        (jnp.concatenate((above, below.T), axis=1), jnp.concatenate((below, lower_inverse), axis=1)), axis=0
    )


def inverse_steps(matrix_ref, inverse_ref, work):
    size = matrix_ref.shape[-1]
    inverse_ref[...] = yield from inverse_of(matrix_ref[...].reshape(size, size), work)


def inverse_kernel(matrix_ref, inverse_ref, work):
    for _ in inverse_steps(matrix_ref, inverse_ref, work):
        pass


def pivot_size(size):
    return size if size <= 128 else pivot_size(size // 2)


def inverse(matrix):
    size = matrix.shape[0]
    part = pivot_size(size)
    return pl.pallas_call(
        inverse_kernel,
        out_shape=jax.ShapeDtypeStruct(matrix.shape, jnp.float32),
        in_specs=[VMEM],
        out_specs=VMEM,
        scratch_shapes=[pltpu.VMEM((part, part), jnp.float32)],
        cost_estimate=pl.CostEstimate(flops=400_000_000, bytes_accessed=8 * size * size, transcendentals=0),
        name="inverse",
    )(matrix)


def exchange_plain(row_part, col_part, gram_part):
    tr_size, tc_size = lax.axis_size("tr"), lax.axis_size("tc")
    row_blocks, size, count_obs = row_part.shape
    col_blocks = col_part.shape[0]
    row_part = row_part.reshape(row_blocks * size, count_obs)
    col_part = col_part.transpose(0, 2, 1).reshape(col_blocks * size, count_obs)
    innovation = lax.psum(gram_part, ("tr", "tc"))
    count = tr_size * tc_size
    to_rows = [((q % tr_size) * tc_size + q // tr_size, q) for q in range(count)]
    to_cols = [(there, here) for here, there in to_rows]
    col_chunk = lax.psum_scatter(col_part, "tr", scatter_dimension=0, tiled=True)
    row_chunk = lax.psum_scatter(row_part, "tc", scatter_dimension=0, tiled=True)
    chunk = row_chunk + lax.ppermute(col_chunk, ("tr", "tc"), to_rows)
    cross_rows = lax.all_gather(chunk, "tc", axis=0, tiled=True)
    cross_cols = lax.all_gather(lax.ppermute(chunk, ("tr", "tc"), to_cols), "tr", axis=0, tiled=True)
    return (
        cross_rows.reshape(row_blocks, size, count_obs),
        cross_cols.reshape(col_blocks, size, count_obs).transpose(0, 2, 1),
        inverse(innovation),
    )


class Sems:
    def __init__(self):
        self.count = 0

    def take(self, number=1):
        self.count += number
        return self.count - number


def share_kernel(stations_ref, values_ref, errors_ref, all_ref, mine_ref, send, recv, core_send, core_recv):
    row, col = lax.axis_index("tr"), lax.axis_index("tc")
    chips = all_ref.shape[0] // 2
    chip, core = col // 2, col % 2

    def copy(source, block, step):
        return pltpu.make_async_remote_copy(
            source, all_ref.at[block], send.at[step], recv.at[step],
            device_id=(row, 2 * lax.rem(chip + step, chips) + core), device_id_type=pl.DeviceIdType.MESH,
        )

    def beside(source, block, step):
        return pltpu.make_async_remote_copy(
            source, all_ref.at[block], core_send.at[step], core_recv.at[step],
            device_id=(row, 2 * chip + 1 - core), device_id_type=pl.DeviceIdType.MESH,
        )

    number, size = values_ref.shape[1:]
    equal = lax.broadcasted_iota(i32, (number, number), 0) == lax.broadcasted_iota(i32, (number, number), 1)

    def upright(across):
        return jnp.sum(jnp.where(equal, across, 0.0), axis=1, keepdims=True)

    lanes = lax.broadcasted_iota(i32, (number, mine_ref.shape[1] - size), 1)
    stations, errors = upright(stations_ref[...].astype(f32)), upright(errors_ref[...])
    mine_ref[:, :size] = values_ref[0]
    mine_ref[:, size:] = jnp.where(lanes == 0, stations, jnp.where(lanes == 1, errors, 0.0))
    sent = [copy(mine_ref, col, step) for step in range(1, chips)]
    sent.append(beside(mine_ref, col, 0))
    for one in sent:
        one.start()
    all_ref[col] = mine_ref[...]
    for step in range(1, chips):
        block = 2 * lax.rem(chip + chips - step, chips) + core
        copy(mine_ref, block, step).wait_recv()
        sent.append(beside(all_ref.at[block], block, step))
        sent[-1].start()
    for step in range(chips):
        beside(mine_ref, 2 * lax.rem(chip + chips - step, chips) + 1 - core, step).wait_recv()
    for one in sent:
        one.wait_send()


def share(stations, obs_values, obs_error):
    many = lax.axis_size("tc")
    _, number, size = obs_values.shape
    packed = (number, size + 128)
    full = pl.pallas_call(
        share_kernel,
        out_shape=jax.ShapeDtypeStruct((many, *packed), f32),
        in_specs=[VMEM] * 3,
        out_specs=VMEM,
        scratch_shapes=[pltpu.VMEM(packed, f32)] + [pltpu.SemaphoreType.DMA((many // 2,))] * 4,
        compiler_params=pltpu.CompilerParams(has_side_effects=True, vmem_limit_bytes=8 * 2**20),
        name="share",
    )(stations, obs_values, obs_error)
    return full.reshape(many * number, size + 128)


def exchange_kernel(
    count_bits, limits, row_ref, col_ref, gram_ref, rows_out, cols_out, inverse_out,
    gram_out, work, send, recv, from_core, sums, landed, upward, downward, rows_here, cols_here, total, relay,
    gram_work, gram_core, gram_bits, gram_line,
):
    sems = Sems()
    line = lax.axis_size("tr")
    z, j = lax.axis_index("tr"), lax.axis_index("tc")
    chip, core = j // 2, j % 2
    parts = count_bits
    width = rows_here.shape[1]
    pending = []
    beside = (z, 2 * chip + 1 - core)

    def copy(source, target, sem, device=beside):
        return pltpu.make_async_remote_copy(
            source, target, send.at[sem], recv.at[sem], device_id=device, device_id_type=pl.DeviceIdType.MESH
        )

    def begin(source, target, device):
        made = copy(source, target, sems.take(), device)
        made.start()
        pending.append(made)
        return made

    def bit(number):
        return chip // 2**number % 2

    def across(number):
        return z, 2 * (chip + (1 - 2 * bit(number)) * 2**number) + core

    def mixed(value, plane):
        return sum(
            (value // 2**number + plane // 2 ** (count_bits - 1 - number)) % 2 * 2**number
            for number in range(count_bits)
        )

    def plane_of(value, chunk):
        return sum(
            (value // 2**number + chunk // 2**number) % 2 * 2 ** (count_bits - 1 - number)
            for number in range(count_bits)
        )

    up, down = sems.take(line), sems.take(line)

    many_obs = total.shape[0]

    def up_rows(place):
        return pl.ds(0, limits[place])

    def down_rows(place):
        return pl.ds(many_obs - limits[line - 1 - place], limits[line - 1 - place])

    def up_copy(place, chunk, source):
        rows = up_rows(place)
        return copy(source.at[chunk, rows], upward.at[chunk, rows], up + chunk, (z + 1, j))

    def down_copy(place, chunk, source):
        rows = down_rows(place)
        return copy(source.at[chunk, rows], downward.at[chunk, rows], down + chunk, (z - 1, j))

    def line_begin(step):
        @pl.when(z == 0)
        def _():
            up_copy(0, line - step, col_ref).start()

        @pl.when(z == line - 1)
        def _():
            down_copy(line - 1, step - 1, col_ref).start()

    def line_round(step):
        for place in range(1, line - 1):
            chunk, other = place + line - 1 - step, place - line + 1 + step

            @pl.when(z == place)
            def _():
                if chunk < line:
                    fresh = limits[place] - limits[place - 1]
                    up_copy(place - 1, chunk, upward).wait_recv()
                    upward[chunk, up_rows(place - 1)] += col_ref[chunk, up_rows(place - 1)]
                    if fresh:
                        later = pl.ds(limits[place - 1], fresh)
                        upward[chunk, later] = col_ref[chunk, later]
                    up_copy(place, chunk, upward).start()
                if other >= 0:
                    fresh = limits[line - 1 - place] - limits[line - 2 - place]
                    down_copy(place + 1, other, downward).wait_recv()
                    downward[other, down_rows(place + 1)] += col_ref[other, down_rows(place + 1)]
                    if fresh:
                        later = pl.ds(many_obs - limits[line - 1 - place], fresh)
                        downward[other, later] = col_ref[other, later]
                    down_copy(place, other, downward).start()

    def line_end():
        total[...] = col_ref[z]
        for place in range(line):

            @pl.when(z == place)
            def _():
                if place > 0:
                    up_copy(place - 1, place, upward).wait_recv()
                    total[up_rows(place - 1)] += upward[place, up_rows(place - 1)]
                if place < line - 1:
                    down_copy(place + 1, place, downward).wait_recv()
                    total[down_rows(place + 1)] += downward[place, down_rows(place + 1)]

    def line_sent():
        for place in range(line):

            @pl.when(z == place)
            def _():
                for chunk in range(place + 1, line):
                    up_copy(place, chunk, upward).wait_send()
                for other in range(place):
                    down_copy(place, other, downward).wait_send()

    def chosen(part, step, flip):
        order = [(part + turn) % count_bits for turn in range(count_bits)]
        free = order[step + 1:]
        picks = []
        for pick in range(2 ** len(free)):
            where = 0
            for turn, number in enumerate(order):
                if number in free:
                    value = pick // 2 ** free.index(number) % 2
                elif turn == step and flip:
                    value = 1 - bit(number)
                else:
                    value = bit(number)
                where = where + value * 2**number
            picks.append(where)
        return order[step], picks

    step_base = [0]
    for step in range(count_bits):
        step_base.append(step_base[-1] + parts * 2 ** (count_bits - 1 - step))

    def plane_send(step):
        made = []
        for part in range(parts):
            number, picks = chosen(part, step, True)
            for slot, pick in enumerate(picks):
                at = step_base[step] + part * len(picks) + slot
                made.append(begin(sums.at[pick, part], landed.at[at], across(number)))
        return made

    def plane_add(step, made):
        for one in made:
            one.wait_recv()
        for part in range(parts):
            _, picks = chosen(part, step, False)
            for slot, pick in enumerate(picks):
                sums[pick, part] += landed[step_base[step] + part * len(picks) + slot]

    for step in range(1, line):
        line_begin(step)
    held = 2**count_bits
    half = begin(gram_ref.at[pl.ds((1 - core) * held, held)], gram_core, beside)
    core_sum = begin(row_ref.at[1 - core], from_core, beside)
    half.wait_recv()
    gram_work[pl.ds(core * held, held)] = gram_ref[pl.ds(core * held, held)] + gram_core[...]
    for number in reversed(range(count_bits)):
        size = 2**number
        start = core * held + chip // (2 * size) * (2 * size)
        keep, give = start + bit(number) * size, start + (1 - bit(number)) * size
        begin(gram_work.at[pl.ds(give, size)], gram_bits.at[pl.ds(size, size)], across(number)).wait_recv()
        gram_work[pl.ds(keep, size)] += gram_bits[pl.ds(size, size)]
    mine = core * held + chip
    gram_line[z] = gram_work[mine]
    base = sems.take(line)
    for step in range(1, line):
        copy(gram_work.at[mine], gram_line.at[z], base + step, (lax.rem(z + step, line), j)).start()
    core_sum.wait_recv()
    for owner in range(line):
        chunk = mixed(owner, z)
        sums[owner] = row_ref[core, chunk] + from_core[chunk]
    made = plane_send(0)

    def gram_back():
        for step in range(1, line):
            copy(gram_work.at[mine], gram_line.at[lax.rem(z + line - step, line)], base + step).wait()
        gram_out[mine] = sum(gram_line[step] for step in range(line))
        for number in range(count_bits):
            size = 2**number
            spot = gram_out.at[pl.ds(core * held + chip // size * size, size)]
            sent = begin(spot, spot, across(number))
            yield
            sent.wait_recv()
        spot = gram_out.at[pl.ds(core * held, held)]
        sent = begin(spot, spot, beside)
        yield
        sent.wait_recv()

    to_cols, first_leg, second_leg = sems.take(), sems.take(2), sems.take(2)
    owned = mixed(chip, z)
    apart = (owned != z) | (z != chip)
    column = (owned, 2 * z + core)
    via = mixed(z, chip)
    beyond = plane_of(chip, z)

    def piece(ref, number):
        size = total.shape[0] // 2
        return ref.at[pl.ds(number * size, size)]

    def leg_one(number):
        return copy(piece(total, number), piece(relay, number), first_leg + number, (z, 2 * via + core))

    def leg_two(number):
        return copy(piece(relay, number), piece(cols_here, number), second_leg + number, (beyond, j))

    gram_turns = gram_back()
    for step in range(1, line - 1):
        line_round(step)
        next(gram_turns, None)
        if step < count_bits:
            plane_add(step - 1, made)
            made = plane_send(step)
            next(gram_turns, None)
    for step in range(max(line - 1, 1), count_bits):
        plane_add(step - 1, made)
        made = plane_send(step)
    line_end()

    @pl.when(via != chip)
    def _():
        leg_one(0).start()
        leg_one(1).start()

    @pl.when(via == chip)
    def _():
        relay[...] = total[...]

    for _ in gram_turns:
        pass
    plane_add(count_bits - 1, made)
    inverse_turns = inverse_steps(gram_out, inverse_out, work)

    def fill(number):
        for _ in range(number):
            next(inverse_turns, None)

    @pl.when(apart)
    def _():
        copy(sums.at[chip], rows_here, to_cols, column).start()

    @pl.when(jnp.logical_not(apart))
    def _():
        rows_here[...] = sums[chip]

    for number in range(2):

        @pl.when(via != chip)
        def _():
            leg_one(number).wait()

        @pl.when(beyond != z)
        def _():
            leg_two(number).start()

    @pl.when(beyond == z)
    def _():
        cols_here[...] = relay[...]

    @pl.when(apart)
    def _():
        copy(sums.at[chip], rows_here, to_cols, column).wait()

    for part in range(parts):
        lanes = slice(part * width, (part + 1) * width)
        cols_out[z, :, lanes] = total[:, lanes] + rows_here[part].T
    around, back = sems.take(line), sems.take(line)

    def line_spread(step):
        chunk, other = z - (step - 1), z + (step - 1)

        @pl.when(chunk >= 0)
        def _():
            if step > 1:
                copy(cols_out.at[chunk], cols_out.at[chunk], around + chunk).wait_recv()

            @pl.when(z < line - 1)
            def _():
                copy(cols_out.at[chunk], cols_out.at[chunk], around + chunk, (z + 1, j)).start()

        @pl.when(other < line)
        def _():
            if step > 1:
                copy(cols_out.at[other], cols_out.at[other], back + other).wait_recv()

            @pl.when(z > 0)
            def _():
                copy(cols_out.at[other], cols_out.at[other], back + other, (z - 1, j)).start()

    def line_spread_sent():
        for step in range(1, line + 1):
            chunk, other = z - (step - 1), z + (step - 1)

            @pl.when((chunk >= 0) & (z < line - 1))
            def _():
                copy(cols_out.at[chunk], cols_out.at[chunk], around + chunk).wait_send()

            @pl.when((other < line) & (z > 0))
            def _():
                copy(cols_out.at[other], cols_out.at[other], back + other).wait_send()

    line_spread(1)
    fill(3)

    @pl.when(beyond != z)
    def _():
        leg_two(0).wait()
        leg_two(1).wait()

    for part in range(parts):
        lanes = slice(part * width, (part + 1) * width)
        rows_out[core, owned, part] = sums[chip, part] + cols_here[:, lanes].T

    def spots(turn, flip):
        for part in range(parts):
            number, picks = chosen(part, count_bits - 1 - turn, flip)
            for pick in picks:
                yield number, rows_out.at[core, mixed(pick, z), part]

    beside_copies = [begin(rows_out.at[core, owned], rows_out.at[core, owned], beside)]
    for turn in range(max(line - 1, count_bits)):
        if turn < count_bits:
            made = [begin(spot, spot, across(number)) for number, spot in spots(turn, False)]
        if turn == count_bits:
            fill(64)
        if turn + 2 <= line:
            line_spread(turn + 2)
        if turn < count_bits:
            fill(2)
            for one in made:
                one.wait_recv()
            beside_copies += [begin(spot, spot, beside) for _, spot in spots(turn, True)]
    fill(64)
    for one in beside_copies:
        one.wait_recv()
    line_spread_sent()
    line_sent()
    for one in pending:
        one.wait_send()


def exchange(limits, row_part, col_part, gram_part):
    line, many = lax.axis_size("tr"), lax.axis_size("tc")
    count_bits = line.bit_length() - 1
    row_blocks, size, count_obs = row_part.shape
    parts, width = count_bits, size // count_bits
    seg = count_obs // many
    rows = (2, line, parts, width, count_obs)
    cols = col_part.shape
    gram = (many, seg, count_obs)
    landings = sum(parts * 2 ** (count_bits - 1 - step) for step in range(count_bits))
    part = pivot_size(count_obs)
    cross_rows, cross_cols, inverted = pl.pallas_call(
        functools.partial(exchange_kernel, count_bits, limits),
        out_shape=tuple(jax.ShapeDtypeStruct(shape, f32) for shape in (rows, cols, gram_part.shape)),
        in_specs=[VMEM] * 3,
        out_specs=(VMEM,) * 3,
        scratch_shapes=[
            pltpu.VMEM(gram, f32),
            pltpu.VMEM((part, part), f32),
            pltpu.SemaphoreType.DMA((96,)),
            pltpu.SemaphoreType.DMA((96,)),
            pltpu.VMEM(rows[1:], f32),
            pltpu.VMEM(rows[1:], f32),
            pltpu.VMEM((landings, width, count_obs), f32),
            pltpu.VMEM(cols, f32),
            pltpu.VMEM(cols, f32),
            pltpu.VMEM(rows[2:], f32),
            pltpu.VMEM(cols[1:], f32),
            pltpu.VMEM(cols[1:], f32),
            pltpu.VMEM(cols[1:], f32),
            pltpu.VMEM(gram, f32),
            pltpu.VMEM((many // 2, seg, count_obs), f32),
            pltpu.VMEM((many // 2, seg, count_obs), f32),
            pltpu.VMEM((line, seg, count_obs), f32),
        ],
        compiler_params=pltpu.CompilerParams(has_side_effects=True, vmem_limit_bytes=ROOM),
        name="exchange",
    )(row_part.reshape(rows), col_part, gram_part.reshape(gram))
    return cross_rows.reshape(row_part.shape), cross_cols, inverted


def body(cov_tiles, block_order, stations, obs_values, obs_error):
    size = obs_values.shape[2]
    line, many = lax.axis_size("tr"), lax.axis_size("tc")
    packed = share(stations, obs_values, obs_error)
    row_part, col_part, gram_part, fits = forward(block_order, packed, cov_tiles, size)
    square = many == 2 * line and line & (line - 1) == 0 and line > 1
    whole_tiles = row_part.shape[0] == many and col_part.shape[0] == line
    parts = (row_part, col_part, gram_part)
    if square and whole_tiles:
        count_obs = gram_part.shape[0]
        cross_rows, cross_cols, inverted = lax.cond(
            fits[0] > 0,
            functools.partial(exchange, reach(count_obs, line)),
            functools.partial(exchange, (count_obs,) * line),
            *parts,
        )
    else:
        cross_rows, cross_cols, inverted = exchange_plain(*parts)
    return update(block_order, cross_rows, cross_cols, inverted, cov_tiles)


def solution(mesh):
    in_specs = (P("tr", "tc"), P(), P(None, "tc"), P(None, "tc", None), P(None, "tc"))
    out_specs = P("tr", "tc")
    return jax.shard_map(body, mesh=mesh, in_specs=in_specs, out_specs=out_specs, check_vma=False)
```
